256 devices in a mesh: dp: 8 (over x, z_lo), owner: 32 (over y, z_hi, core).
Axes of the slice: x: 4, y: 4, z: 8 (z_hi: 4, z_lo: 2; z = z_hi * 2 + z_lo), core: 2. Of those that a mesh axis runs over, the one named last changes fastest.
Arguments:
- partial_grads: bfloat16 [8, 48, 1024, 1024], P('dp', None, 'owner'), may hold values from -2.09375 to 2.09375
- owner_map: int32 [48], replicated, may hold values from 0 to 31, as said below
- left_stats: float32 [32, 3, 1024, 1024], P('owner', None, 'dp'), may hold values from -1.8 to 1.8
- right_stats: float32 [32, 3, 1024, 1024], P('owner', None, 'dp'), may hold values from -1.8 to 1.8
- left_roots: bfloat16 [32, 3, 1024, 1024], P('owner', None, 'dp'), as said below
- right_roots: bfloat16 [32, 3, 1024, 1024], P('owner', None, 'dp'), as said below
Outputs:
- direction: bfloat16 [48, 1024, 1024], P(None, ('dp', 'owner'))
- new_left_stats: float32 [32, 3, 1024, 1024], P('owner', None, 'dp')
- new_right_stats: float32 [32, 3, 1024, 1024], P('owner', None, 'dp')
The draws below stay inside these ranges and needn't reach their ends.
Inputs may be any that keep to these rules, and one draw needn't show every extreme that they name: `owner_map`: no owner index holds more than 3 blocks, and some owner holds exactly 3. `left_roots`: each block is dense and not symmetric; its diagonal entries are of order one and its off-diagonal entries are small. `right_roots`: each block is dense and not symmetric; its diagonal entries are of order one and its off-diagonal entries are small.
All inputs are finite; a program needn't handle non-finite values.
Results may differ from the reference program's by a relative error of at most 0.017.
Values may be sent and summed in bfloat16 or wider, within the bound.
A program may use at most 128 MiB of HBM per device.

```python
import jax
import jax.numpy as jnp
from jax import lax

D_MODEL = 2560
D_IN = 10576
D_INNER = 5120
TILE = 1024
TILES = 48
OWNERS = 32
SLOTS = 3
N_DP = 8


def draw_owner_map(key, part):
    first, second = jax.random.split(jax.random.fold_in(key, 7))
    total = OWNERS * SLOTS
    ranks = jax.random.permutation(first, total).astype(jnp.int32)
    chosen = jax.random.randint(second, (), 0, OWNERS, dtype=jnp.int32)
    ids = jnp.arange(total, dtype=jnp.int32)
    keyed = jnp.where(ids // SLOTS == chosen, -1 - ids % SLOTS, ranks)
    order = jnp.argsort(keyed, stable=True).astype(jnp.int32)
    return (order[:TILES] // SLOTS).astype(jnp.int32)


def draw_root(key):
    first, second = jax.random.split(key)
    shape = (OWNERS, SLOTS, TILE, TILE)
    diag = jax.random.uniform(first, (OWNERS, SLOTS, TILE), jnp.float32, 0.5, 1.5)
    off = jax.random.normal(second, shape, jnp.float32) * (0.4 / TILE ** 0.5)
    eye = jnp.eye(TILE, dtype=jnp.float32)
    return off + diag[..., None] * eye


def draw_left_roots(key, part):
    return draw_root(jax.random.fold_in(key, 11)).astype(jnp.bfloat16)


def draw_right_roots(key, part):
    return draw_root(jax.random.fold_in(key, 13)).astype(jnp.bfloat16)


def shard_levels(own_key, shape, shards, least, high):
    level = 1.0
    for position, shards_of in shards:
        draws = jax.random.uniform(jax.random.fold_in(jax.random.fold_in(own_key, 6), position), (shards_of,), jnp.float32, least / len(shards), high / len(shards))
        level = level * jnp.repeat(jnp.exp(draws), shape[position] // shards_of).reshape((-1,) + (1,) * (len(shape) - 1 - position))
    return level


def centred(key, shape, deviation, limit, shards=(), kind=jnp.bfloat16):
    values = deviation * jax.random.normal(key, shape, jnp.float32)
    if shards:
        values = values * shard_levels(key, shape, shards, -0.22, 0.18)
    return jnp.clip(values, -limit, limit).astype(kind)


def setup_inputs(seed: int = 0) -> dict:
    key_of = jax.random.split(jax.random.key(seed), 7)
    partial_grads = centred(key_of[0], (N_DP, TILES, TILE, TILE), 0.35, 2.09375, ((0, 8), (2, 32)))
    owner_map = draw_owner_map(jax.random.fold_in(key_of[6], 71), 0)
    left_stats = centred(key_of[2], (OWNERS, SLOTS, TILE, TILE), 0.3, 1.8, ((0, 32), (2, 8)), jnp.float32)
    right_stats = centred(key_of[3], (OWNERS, SLOTS, TILE, TILE), 0.3, 1.8, ((0, 32), (2, 8)), jnp.float32)
    left_roots = draw_left_roots(jax.random.fold_in(key_of[6], 71), 0)
    right_roots = draw_right_roots(jax.random.fold_in(key_of[6], 71), 0)
    return {"partial_grads": partial_grads, "owner_map": owner_map, "left_stats": left_stats, "right_stats": right_stats, "left_roots": left_roots, "right_roots": right_roots}


stat_decay = 0.999


def extents(count):
    index = jnp.arange(count, dtype=jnp.int32)
    in_cols = -(-D_IN // TILE)
    out_cols = -(-D_MODEL // TILE)
    in_count = (-(-D_MODEL // TILE)) * in_cols
    is_in = index < in_count
    other = jnp.maximum(index - in_count, 0)
    rows = jnp.where(is_in, jnp.minimum(TILE, D_MODEL - (index // in_cols) * TILE), jnp.minimum(TILE, D_INNER - (other // out_cols) * TILE))
    cols = jnp.where(is_in, jnp.minimum(TILE, D_IN - (index % in_cols) * TILE), jnp.minimum(TILE, D_MODEL - (other % out_cols) * TILE))
    return rows.astype(jnp.int32), cols.astype(jnp.int32)


def reference(partial_grads, owner_map, left_stats, right_stats, left_roots, right_roots):
    rows, cols = extents(TILES)
    line = jnp.arange(TILE, dtype=jnp.int32)
    mask = (line[None, :, None] < rows[:, None, None]) & (line[None, None, :] < cols[:, None, None])
    total = jnp.zeros(partial_grads.shape[1:], jnp.float32)
    for source in range(N_DP):
        total = total + partial_grads[source].astype(jnp.float32)
    grads = jnp.where(mask, total, jnp.float32(0.0)).astype(jnp.bfloat16)
    ids = jnp.arange(TILES, dtype=jnp.int32)
    same = (owner_map[:, None] == owner_map[None, :]) & (ids[None, :] < ids[:, None])
    slot = jnp.sum(same.astype(jnp.int32), axis=1).astype(jnp.int32)

    def per_tile(index):
        grad = grads[index]
        owner = owner_map[index]
        place = slot[index]
        left_new = stat_decay * left_stats[owner, place] + (1.0 - stat_decay) * jnp.dot(grad, grad.T, preferred_element_type=jnp.float32)
        right_new = stat_decay * right_stats[owner, place] + (1.0 - stat_decay) * jnp.dot(grad.T, grad, preferred_element_type=jnp.float32)
        left_part = jnp.dot(left_roots[owner, place], grad, preferred_element_type=jnp.float32).astype(jnp.bfloat16)
        result = jnp.dot(left_part, right_roots[owner, place], preferred_element_type=jnp.float32)
        result = jnp.where(mask[index], result, jnp.float32(0.0)).astype(jnp.bfloat16)
        return left_new, right_new, result

    left_all, right_all, direction = lax.map(per_tile, ids)
    new_left = (stat_decay * left_stats).at[owner_map, slot].set(left_all)
    new_right = (stat_decay * right_stats).at[owner_map, slot].set(right_all)
    return (direction, new_left, new_right)
```

```python
import jax
import jax.numpy as jnp
from jax import lax
from jax.experimental import pallas as pl
from jax.experimental.pallas import tpu as pltpu
from jax.sharding import Mesh
from jax.sharding import PartitionSpec as P

D_MODEL = 2560
D_IN = 10576
D_INNER = 5120
TILE = 1024
TILES = 48
OWNERS = 32
SLOTS = 3
PIECE = 32
LANES = 128
COLS = 128
HALF = 512
CHUNKS = 4
PER = TILES // CHUNKS
OWNER = ("owner_0", "owner_1", "owner_2")
DP = ("dp_0", "dp_1")
DP_OWNER = ("dp_0", "dp_1", "owner_0", "owner_1", "owner_2")
MESH = pl.DeviceIdType.MESH
F32 = jnp.float32
BF16 = jnp.bfloat16

stat_decay = 0.999


def extent(t):
    in_cols = -(-D_IN // TILE)
    out_cols = -(-D_MODEL // TILE)
    in_count = -(-D_MODEL // TILE) * in_cols
    other = jnp.maximum(t - in_count, 0)
    is_in = t < in_count
    rows = jnp.where(
        is_in,
        jnp.minimum(TILE, D_MODEL - t // in_cols * TILE),
        jnp.minimum(TILE, D_INNER - other // out_cols * TILE),
    )
    cols = jnp.where(
        is_in,
        jnp.minimum(TILE, D_IN - t % in_cols * TILE),
        jnp.minimum(TILE, D_MODEL - other % out_cols * TILE),
    )
    return rows, cols


class Ids:
    def __init__(self):
        self.n = 0

    def __call__(self, *shape):
        size = 1
        for s in shape:
            size *= s
        base = self.n
        self.n += size

        def at(*index):
            flat = 0
            for i, s in zip(index, shape):
                flat = flat * s + i
            return base + flat

        return at


IDS = Ids()
FAR = IDS(CHUNKS, 2)
NEAR = IDS(CHUNKS, 2)
CHAIN = IDS(CHUNKS, 2)
ZZ = IDS(CHUNKS)
RZ = IDS(SLOTS)
RN = IDS(SLOTS, 2)
RF = IDS(SLOTS, 2)
LZ = IDS(SLOTS)
A2A = IDS(SLOTS)
GZ = IDS(SLOTS)
GN = IDS(SLOTS, 2, 2)
GF = IDS(SLOTS, 2)
RET = IDS(SLOTS)
N_SEMS = IDS.n
LOC = Ids()
L_PG = LOC(CHUNKS)
L_R = LOC(SLOTS)
L_L = LOC(SLOTS)
L_LS = LOC(1)
L_RS = LOC(1)
L_NL = LOC(SLOTS)
L_NR = LOC(SLOTS)
N_LOC = LOC.n


def kernel(
    tile_s,
    place_s,
    pg_h,
    l_h,
    r_h,
    ls_h,
    rs_h,
    dir_o,
    nl_h,
    nr_h,
    pg,
    far,
    chs,
    near,
    ch,
    hs,
    zrecv,
    shares,
    staged,
    gf,
    rf,
    lp,
    ls,
    rs,
    nl,
    nr,
    gt,
    tp,
    obuf,
    ostage,
    ret,
    send,
    recv,
    local,
):
    x = lax.axis_index("dp_0")
    zl = lax.axis_index("dp_1")
    y = lax.axis_index("owner_0")
    zh = lax.axis_index("owner_1")
    co = lax.axis_index("owner_2")
    me = (y * 4 + zh) * 2 + co
    d = x * 2 + zl
    xp = (x + 1) % 4
    xm = (x + 3) % 4
    x2 = (x + 2) % 4
    zo = 1 - zl
    here = zl * 32 + me
    to_xp = {"dp_0": xp}
    to_xm = {"dp_0": xm}
    to_z = {"dp_1": zo}

    def owner_device(i):
        return {"owner_0": i // 8, "owner_1": (i // 2) % 4, "owner_2": i % 2}

    def any_device(i):
        return {
            "dp_1": i // 32,
            "owner_0": (i // 8) % 4,
            "owner_1": (i // 2) % 4,
            "owner_2": i % 2,
        }

    sent = []

    def start(src, dst, sem, device):
        copy = pltpu.make_async_remote_copy(
            src_ref=src,
            dst_ref=dst,
            send_sem=send.at[sem],
            recv_sem=recv.at[sem],
            device_id=device,
            device_id_type=MESH,
        )
        copy.start()
        sent.append(copy)

    def arrived(dst, sem):
        pltpu.make_async_remote_copy(
            src_ref=dst,
            dst_ref=dst,
            send_sem=send.at[sem],
            recv_sem=recv.at[sem],
            device_id=to_xp,
            device_id_type=MESH,
        ).wait_recv()

    def lanes(block, width=COLS):
        return pl.ds(pl.multiple_of(block * width, width), width)

    def chunk(k):
        return pl.ds(k * PER, PER)

    pg_in = [
        pltpu.make_async_copy(pg_h.at[chunk(k)], pg.at[chunk(k)], local.at[L_PG(k)])
        for k in range(CHUNKS)
    ]
    for copy in pg_in:
        copy.start()
    own_rows = pl.ds(pl.multiple_of(d * LANES, LANES), LANES)
    pair_rows = pl.ds(pl.multiple_of(zl * LANES, LANES), LANES)
    r_in = [
        pltpu.make_async_copy(
            r_h.at[s, :, lanes(zl, HALF)], rf.at[s, own_rows, :], local.at[L_R(s)]
        )
        for s in range(SLOTS)
    ]
    l_in = [
        pltpu.make_async_copy(l_h.at[s], lp.at[s, pair_rows, :], local.at[L_L(s)])
        for s in range(SLOTS)
    ]
    ls_in = pltpu.make_async_copy(ls_h, ls, local.at[L_LS(0)])
    rs_in = pltpu.make_async_copy(rs_h, rs, local.at[L_RS(0)])
    for copy in (*r_in, *l_in, ls_in, rs_in):
        copy.start()

    barrier = pltpu.get_barrier_semaphore()
    pl.semaphore_signal(barrier, inc=1, device_id=to_xp, device_id_type=MESH)
    pl.semaphore_signal(barrier, inc=1, device_id=to_xm, device_id_type=MESH)

    def greet(k, carry):
        pl.semaphore_signal(
            barrier, inc=1, device_id=any_device((here + k) % 64), device_id_type=MESH
        )
        return carry

    lax.fori_loop(1, 64, greet, 0)
    pl.semaphore_wait(barrier, 65)

    def send_near(k):
        start(pg.at[chunk(k), :, lanes(xp)], near.at[0, chunk(k)], NEAR(k, 0), to_xp)
        start(pg.at[chunk(k), :, lanes(4 + xm)], near.at[1, chunk(k)], NEAR(k, 1), to_xm)

    for k in range(CHUNKS):
        pg_in[k].wait()
        start(pg.at[chunk(k), :, lanes(x2)], far.at[0, chunk(k)], FAR(k, 0), to_xm)
        start(pg.at[chunk(k), :, lanes(4 + x2)], far.at[1, chunk(k)], FAR(k, 1), to_xp)
    send_near(0)

    for s in range(SLOTS):
        r_in[s].wait()
        start(r_h.at[s, :, lanes(zo, HALF)], rf.at[s, own_rows, :], RZ(s), to_z)
    start(l_h.at[0], lp.at[0, pair_rows, :], LZ(0), to_z)

    def per_tile(k, step, unroll=2):
        def one(i, carry):
            step(k * PER + i)
            return carry

        lax.fori_loop(0, PER, one, 0, unroll=unroll)

    for k in range(CHUNKS):
        arrived(far.at[0, chunk(k)], FAR(k, 0))
        arrived(far.at[1, chunk(k)], FAR(k, 1))

        def add_chain(t):
            chs[0, t] = (
                far[0, t].astype(F32) + pg[t, :, lanes(xm)].astype(F32)
            ).astype(BF16)
            chs[1, t] = (
                far[1, t].astype(F32) + pg[t, :, lanes(4 + xp)].astype(F32)
            ).astype(BF16)

        per_tile(k, add_chain)
        if k + 1 < CHUNKS:
            send_near(k + 1)
        start(chs.at[0, chunk(k)], ch.at[0, chunk(k)], CHAIN(k, 0), to_xm)
        start(chs.at[1, chunk(k)], ch.at[1, chunk(k)], CHAIN(k, 1), to_xp)

    def total(half, t):
        return (
            pg[t, :, lanes(half * 4 + x)].astype(F32)
            + near[half, t].astype(F32)
            + ch[half, t].astype(F32)
        )

    for k in range(CHUNKS):
        for side in range(2):
            arrived(near.at[side, chunk(k)], NEAR(k, side))
            arrived(ch.at[side, chunk(k)], CHAIN(k, side))

        def other_half(t):
            hs[t] = total(zo, t).astype(BF16)

        per_tile(k, other_half)
        start(hs.at[chunk(k)], zrecv.at[chunk(k)], ZZ(k), to_z)

    def quad(chip, part, rows):
        return pl.ds(pl.multiple_of(chip * 256 + part, LANES), rows)

    for s in range(SLOTS):
        arrived(rf.at[s, own_rows, :], RZ(s))
        block = rf.at[s, quad(x, 0, 256), :]
        start(block, block, RN(s, 0), to_xp)
        start(block, block, RN(s, 1), to_xm)

    my_block = zl * 4 + x
    other_block = zo * 4 + x
    row_of = lax.broadcasted_iota(jnp.int32, (PIECE, COLS), 0) + me * PIECE
    col_of = lax.broadcasted_iota(jnp.int32, (PIECE, COLS), 1) + my_block * COLS
    for k in range(CHUNKS):
        arrived(zrecv.at[chunk(k)], ZZ(k))

        def share(t):
            rows, cols = extent(t)
            value = total(zl, t) + zrecv[t].astype(F32)
            shares[t] = jnp.where((row_of < rows) & (col_of < cols), value, 0.0).astype(BF16)

        per_tile(k, share)
    shares[TILES] = jnp.zeros((PIECE, COLS), BF16)

    my_cols = lanes(my_block)
    my_piece = pl.ds(pl.multiple_of(me * PIECE, PIECE), PIECE)
    for s in range(SLOTS):

        def stage(o, carry):
            staged[s, o] = shares[tile_s[s * OWNERS + o]]
            return carry

        lax.fori_loop(0, OWNERS, stage, 0, unroll=4)

    def to_owners(s):
        def one(k, carry):
            o = (me + k) % OWNERS
            pltpu.make_async_remote_copy(
                src_ref=staged.at[s, o],
                dst_ref=gf.at[s, my_piece, my_cols],
                send_sem=send.at[A2A(s)],
                recv_sem=recv.at[A2A(s)],
                device_id=owner_device(o),
                device_id_type=MESH,
            ).start()
            return carry

        lax.fori_loop(1, OWNERS, one, 0)

    for s in range(SLOTS):
        to_owners(s)
    for s in range(1, SLOTS):
        start(l_h.at[s], lp.at[s, pair_rows, :], LZ(s), to_z)
    for s in range(SLOTS):
        gf[s, my_piece, my_cols] = staged[s, me]

    def g_own(s):
        arrived(staged.at[s, pl.ds(0, OWNERS - 1)], A2A(s))
        block = gf.at[s, :, my_cols]
        start(block, block, GZ(s), to_z)
        start(block, block, GN(s, 0, 0), to_xp)
        start(block, block, GN(s, 1, 0), to_xm)

    def g_pair(s):
        block = gf.at[s, :, lanes(other_block)]
        arrived(block, GZ(s))
        start(block, block, GN(s, 0, 1), to_xp)
        start(block, block, GN(s, 1, 1), to_xm)

    def g_far(s):
        block = gf.at[s, :, lanes(xm)]
        arrived(block, GN(s, 0, zl))
        start(block, block, GF(s, 0), to_xp)
        block = gf.at[s, :, lanes(4 + xp)]
        arrived(block, GN(s, 1, zo))
        start(block, block, GF(s, 1), to_xm)

    def g_done(s):
        arrived(gf.at[s, :, lanes(4 + xm)], GN(s, 0, zo))
        arrived(gf.at[s, :, lanes(xp)], GN(s, 1, zl))
        arrived(gf.at[s, :, lanes(x2)], GF(s, 0))
        arrived(gf.at[s, :, lanes(4 + x2)], GF(s, 1))

    def r_far(s):
        arrived(rf.at[s, quad(xm, 0, 256), :], RN(s, 0))
        block = rf.at[s, quad(xm, 0, LANES), :]
        start(block, block, RF(s, 0), to_xp)
        arrived(rf.at[s, quad(xp, 0, 256), :], RN(s, 1))
        block = rf.at[s, quad(xp, LANES, LANES), :]
        start(block, block, RF(s, 1), to_xm)

    def r_done(s):
        arrived(rf.at[s, quad(x2, 0, LANES), :], RF(s, 0))
        arrived(rf.at[s, quad(x2, LANES, LANES), :], RF(s, 1))
        arrived(lp.at[s, pair_rows, :], LZ(s))

    def grams(s):
        gt[...] = gf[s, :, lanes(d)].T
        grad_rows = gf[s, pl.ds(pl.multiple_of(d * LANES, LANES), LANES), :]

        def columns(n, carry):
            at = pl.ds(pl.multiple_of(n * 256, 256), 256)
            right = jnp.dot(gt[...], gf[s, :, at], preferred_element_type=F32)
            nr[s, :, at] = stat_decay * rs[s, :, at] + (1.0 - stat_decay) * right
            part = jnp.dot(lp[s], gf[s, :, at], preferred_element_type=F32)
            tp[:, at] = part.astype(BF16)
            left = lax.dot_general(
                grad_rows, gf[s, at, :], (((1,), (1,)), ((), ())), preferred_element_type=F32
            )
            nl[s, :, at] = stat_decay * ls[s, :, at] + (1.0 - stat_decay) * left
            return carry

        lax.fori_loop(0, 4, columns, 0)

    outs = []

    def stats_out(s):
        for src, dst, sem in ((nl, nl_h, L_NL(s)), (nr, nr_h, L_NR(s))):
            copy = pltpu.make_async_copy(src.at[s], dst.at[s], local.at[sem])
            copy.start()
            outs.append(copy)

    out_cols = lanes(zl, HALF)

    def direction_rows(s):
        def columns(n, carry):
            at = pl.ds(pl.multiple_of(n * 256, 256), 256)
            obuf[:, at] = jnp.dot(tp[...], rf[s, :, at], preferred_element_type=F32)
            return carry

        lax.fori_loop(0, 2, columns, 0)

        def rows(i, carry):
            value = obuf[pl.ds(pl.multiple_of(i * 8, 8), 8), :]
            ostage[s, 2 * i] = value[:4].astype(BF16)
            ostage[s, 2 * i + 1] = value[4:].astype(BF16)
            return carry

        lax.fori_loop(0, 32, rows, 0, unroll=4)
        ret[s * OWNERS + me, :, out_cols] = ostage[s, here]

        def one(k, carry):
            i = (here + k) % 64
            pltpu.make_async_remote_copy(
                src_ref=ostage.at[s, i],
                dst_ref=ret.at[s * OWNERS + me, :, out_cols],
                send_sem=send.at[RET(s)],
                recv_sem=recv.at[RET(s)],
                device_id=any_device(i),
                device_id_type=MESH,
            ).start()
            return carry

        lax.fori_loop(1, 64, one, 0)

    g_own(0)
    for s in range(SLOTS):
        r_far(s)
    g_pair(0)
    g_own(1)
    g_far(0)
    g_pair(1)
    g_own(2)
    g_far(1)
    g_pair(2)
    for s in range(SLOTS):
        l_in[s].wait()
    ls_in.wait()
    rs_in.wait()
    g_done(0)
    r_done(0)
    grams(0)
    direction_rows(0)
    g_far(2)
    stats_out(0)
    g_done(1)
    r_done(1)
    grams(1)
    direction_rows(1)
    stats_out(1)
    g_done(2)
    r_done(2)
    grams(2)
    direction_rows(2)
    stats_out(2)

    for s in range(SLOTS):
        arrived(ostage.at[s, pl.ds(0, 63)], RET(s))
    line = lax.broadcasted_iota(jnp.int32, (4, TILE), 0) + (d * LANES + me * 4)
    lane = lax.broadcasted_iota(jnp.int32, (4, TILE), 1)

    def write(t, carry):
        rows, cols = extent(t)
        value = ret[place_s[t]].astype(F32)
        dir_o[t] = jnp.where((line < rows) & (lane < cols), value, 0.0).astype(BF16)
        return carry

    lax.fori_loop(0, TILES, write, 0, unroll=4)

    for copy in outs:
        copy.wait()
    for copy in sent:
        copy.wait_send()
    for s in range(SLOTS):
        for src, sem in (
            (staged.at[s, pl.ds(0, OWNERS - 1)], A2A(s)),
            (ostage.at[s, pl.ds(0, 63)], RET(s)),
        ):
            pltpu.make_async_remote_copy(
                src_ref=src,
                dst_ref=src,
                send_sem=send.at[sem],
                recv_sem=recv.at[sem],
                device_id=to_xp,
                device_id_type=MESH,
            ).wait_send()


def body(partial_grads, owner_map, left_stats, right_stats, left_roots, right_roots):
    ids = jnp.arange(TILES, dtype=jnp.int32)
    same = (owner_map[:, None] == owner_map[None, :]) & (ids[None, :] < ids[:, None])
    slot = jnp.sum(same.astype(jnp.int32), axis=1)
    place = slot * OWNERS + owner_map
    seats = jnp.arange(SLOTS * OWNERS, dtype=jnp.int32)
    tile_of = TILES + jnp.sum(
        jnp.where(place[None, :] == seats[:, None], ids[None, :] - TILES, 0), axis=1
    )
    smem = pl.BlockSpec(memory_space=pltpu.SMEM)
    hbm = pl.BlockSpec(memory_space=pl.ANY)
    direction, new_left, new_right = pl.pallas_call(
        kernel,
        out_shape=(
            jax.ShapeDtypeStruct((TILES, 4, TILE), BF16),
            jax.ShapeDtypeStruct((SLOTS, LANES, TILE), F32),
            jax.ShapeDtypeStruct((SLOTS, LANES, TILE), F32),
        ),
        in_specs=[smem, smem, hbm, hbm, hbm, hbm, hbm],
        out_specs=(pl.BlockSpec(memory_space=pltpu.VMEM), hbm, hbm),
        scratch_shapes=[
            pltpu.VMEM((TILES, PIECE, TILE), BF16),
            pltpu.VMEM((2, TILES, PIECE, COLS), BF16),
            pltpu.VMEM((2, TILES, PIECE, COLS), BF16),
            pltpu.VMEM((2, TILES, PIECE, COLS), BF16),
            pltpu.VMEM((2, TILES, PIECE, COLS), BF16),
            pltpu.VMEM((TILES, PIECE, COLS), BF16),
            pltpu.VMEM((TILES, PIECE, COLS), BF16),
            pltpu.VMEM((TILES + 1, PIECE, COLS), BF16),
            pltpu.VMEM((SLOTS, OWNERS, PIECE, COLS), BF16),
            pltpu.VMEM((SLOTS, TILE, TILE), BF16),
            pltpu.VMEM((SLOTS, TILE, HALF), BF16),
            pltpu.VMEM((SLOTS, 256, TILE), BF16),
            pltpu.VMEM((SLOTS, LANES, TILE), F32),
            pltpu.VMEM((SLOTS, LANES, TILE), F32),
            pltpu.VMEM((SLOTS, LANES, TILE), F32),
            pltpu.VMEM((SLOTS, LANES, TILE), F32),
            pltpu.VMEM((LANES, TILE), BF16),
            pltpu.VMEM((256, TILE), BF16),
            pltpu.VMEM((256, HALF), F32),
            pltpu.VMEM((SLOTS, 64, 4, HALF), BF16),
            pltpu.VMEM((SLOTS * OWNERS, 4, TILE), BF16),
            pltpu.SemaphoreType.DMA((N_SEMS,)),
            pltpu.SemaphoreType.DMA((N_SEMS,)),
            pltpu.SemaphoreType.DMA((N_LOC,)),
        ],
        compiler_params=pltpu.CompilerParams(
            collective_id=0, has_side_effects=True, vmem_limit_bytes=60 * 1024 * 1024
        ),
    )(
        tile_of,
        place,
        partial_grads[0],
        left_roots[0],
        right_roots[0],
        left_stats[0],
        right_stats[0],
    )
    return direction, new_left[None], new_right[None]


def solution(mesh):
    torus = Mesh(
        mesh.devices.reshape(4, 2, 4, 4, 2), ("dp_0", "dp_1", "owner_0", "owner_1", "owner_2")
    )
    in_specs = (
        P(DP, None, OWNER, None),
        P(),
        P(OWNER, None, DP, None),
        P(OWNER, None, DP, None),
        P(OWNER, None, DP, None),
        P(OWNER, None, DP, None),
    )
    out_specs = (P(None, DP_OWNER, None), P(OWNER, None, DP, None), P(OWNER, None, DP, None))
    return jax.shard_map(body, mesh=torus, in_specs=in_specs, out_specs=out_specs, check_vma=False)
```

```python
import jax
import jax.numpy as jnp
from jax import lax
from jax.experimental import pallas as pl
from jax.experimental.pallas import tpu as pltpu
from jax.sharding import Mesh
from jax.sharding import PartitionSpec as P

D_MODEL = 2560
D_IN = 10576
D_INNER = 5120
TILE = 1024
TILES = 48
OWNERS = 32
SLOTS = 3
PIECE = 32
LANES = 128
COLS = 128
HALF = 512
BOUNDS = (0, 14, 28, 42, 48)
CHUNKS = len(BOUNDS) - 1
OWNER = ("owner_0", "owner_1", "owner_2")
DP = ("dp_0", "dp_1")
DP_OWNER = ("dp_0", "dp_1", "owner_0", "owner_1", "owner_2")
MESH = pl.DeviceIdType.MESH
F32 = jnp.float32
BF16 = jnp.bfloat16

stat_decay = 0.999


def extent(t):
    in_cols = -(-D_IN // TILE)
    out_cols = -(-D_MODEL // TILE)
    in_count = -(-D_MODEL // TILE) * in_cols
    other = jnp.maximum(t - in_count, 0)
    is_in = t < in_count
    rows = jnp.where(
        is_in,
        jnp.minimum(TILE, D_MODEL - t // in_cols * TILE),
        jnp.minimum(TILE, D_INNER - other // out_cols * TILE),
    )
    cols = jnp.where(
        is_in,
        jnp.minimum(TILE, D_IN - t % in_cols * TILE),
        jnp.minimum(TILE, D_MODEL - other % out_cols * TILE),
    )
    return rows, cols


class Ids:
    def __init__(self):
        self.n = 0

    def __call__(self, *shape):
        size = 1
        for s in shape:
            size *= s
        base = self.n
        self.n += size

        def at(*index):
            flat = 0
            for i, s in zip(index, shape):
                flat = flat * s + i
            return base + flat

        return at


IDS = Ids()
FAR = IDS(CHUNKS, 2)
NEAR = IDS(CHUNKS, 2)
CHAIN = IDS(CHUNKS, 2)
ZZ = IDS(CHUNKS)
RZ = IDS(SLOTS)
RN = IDS(SLOTS, 2)
RF = IDS(SLOTS, 2)
LZ = IDS(SLOTS)
A2A = IDS(SLOTS)
GZ = IDS(SLOTS)
GZ_FAR = IDS(SLOTS)
GN = IDS(SLOTS, 2)
GP = IDS(SLOTS, 2, 2)
GF = IDS(SLOTS, 2)
GPF = IDS(SLOTS, 2)
RET = IDS(SLOTS)
N_SEMS = IDS.n
LOC = Ids()
L_PG = LOC(CHUNKS)
L_R = LOC(SLOTS)
L_L = LOC(SLOTS)
L_LS = LOC(1)
L_RS = LOC(1)
L_SEAT = LOC(1)
N_LOC = LOC.n


def kernel(
    owner_s,
    pg_h,
    l_h,
    r_h,
    ls_h,
    rs_h,
    ret,
    nl,
    nr,
    pg,
    far,
    chs,
    near,
    ch,
    hs,
    zrecv,
    shares,
    staged,
    gf,
    rf,
    lp,
    ls,
    rs,
    gt,
    tp,
    obuf,
    ostage,
    tile_v,
    tile_s,
    send,
    recv,
    local,
):
    x = lax.axis_index("dp_0")
    zl = lax.axis_index("dp_1")
    y = lax.axis_index("owner_0")
    zh = lax.axis_index("owner_1")
    co = lax.axis_index("owner_2")
    me = (y * 4 + zh) * 2 + co
    d = x * 2 + zl
    xp = (x + 1) % 4
    xm = (x + 3) % 4
    x2 = (x + 2) % 4
    zo = 1 - zl
    here = zl * 32 + me
    to_xp = {"dp_0": xp}
    to_xm = {"dp_0": xm}
    to_z = {"dp_1": zo}

    def owner_device(i):
        return {"owner_0": i // 8, "owner_1": (i // 2) % 4, "owner_2": i % 2}

    def any_device(i):
        return {
            "dp_1": i // 32,
            "owner_0": (i // 8) % 4,
            "owner_1": (i // 2) % 4,
            "owner_2": i % 2,
        }

    sent = []

    def start(src, dst, sem, device):
        copy = pltpu.make_async_remote_copy(
            src_ref=src,
            dst_ref=dst,
            send_sem=send.at[sem],
            recv_sem=recv.at[sem],
            device_id=device,
            device_id_type=MESH,
        )
        copy.start()
        sent.append(copy)

    def arrived(dst, sem):
        pltpu.make_async_remote_copy(
            src_ref=dst,
            dst_ref=dst,
            send_sem=send.at[sem],
            recv_sem=recv.at[sem],
            device_id=to_xp,
            device_id_type=MESH,
        ).wait_recv()

    def lanes(block, width=COLS):
        return pl.ds(pl.multiple_of(block * width, width), width)

    def chunk(k):
        return pl.ds(BOUNDS[k], BOUNDS[k + 1] - BOUNDS[k])

    pg_in = [
        pltpu.make_async_copy(pg_h.at[chunk(k)], pg.at[chunk(k)], local.at[L_PG(k)])
        for k in range(CHUNKS)
    ]
    for copy in pg_in:
        copy.start()
    own_rows = pl.ds(pl.multiple_of(d * LANES, LANES), LANES)
    pair_rows = pl.ds(pl.multiple_of(zl * LANES, LANES), LANES)
    r_in = [
        pltpu.make_async_copy(
            r_h.at[s, :, lanes(zl, HALF)], rf.at[s, own_rows, :], local.at[L_R(s)]
        )
        for s in range(SLOTS)
    ]
    l_in = [
        pltpu.make_async_copy(l_h.at[s], lp.at[s, pair_rows, :], local.at[L_L(s)])
        for s in range(SLOTS)
    ]
    ls_in = pltpu.make_async_copy(ls_h, ls, local.at[L_LS(0)])
    rs_in = pltpu.make_async_copy(rs_h, rs, local.at[L_RS(0)])
    for copy in (*r_in, *l_in, ls_in, rs_in):
        copy.start()

    barrier = pltpu.get_barrier_semaphore()
    pl.semaphore_signal(barrier, inc=1, device_id=to_xp, device_id_type=MESH)
    pl.semaphore_signal(barrier, inc=1, device_id=to_xm, device_id_type=MESH)

    def greet(k, carry):
        pl.semaphore_signal(
            barrier, inc=1, device_id=any_device((here + k) % 64), device_id_type=MESH
        )
        return carry

    lax.fori_loop(1, 64, greet, 0)

    seat = lax.broadcasted_iota(jnp.int32, (1, LANES), 1)

    def take(t, carry):
        tile, count = carry
        mine = seat % OWNERS == owner_s[t]
        tile = jnp.where(mine & (count == seat // OWNERS), t, tile)
        return tile, count + mine.astype(jnp.int32)

    tile_v[...], _ = lax.fori_loop(
        0, TILES, take, (jnp.full((1, LANES), TILES, jnp.int32), jnp.zeros((1, LANES), jnp.int32))
    )
    seats_in = pltpu.make_async_copy(tile_v, tile_s, local.at[L_SEAT(0)])
    seats_in.start()
    pl.semaphore_wait(barrier, 65)

    def send_near(k):
        start(pg.at[chunk(k), :, lanes(xp)], near.at[0, chunk(k)], NEAR(k, 0), to_xp)
        start(pg.at[chunk(k), :, lanes(4 + xm)], near.at[1, chunk(k)], NEAR(k, 1), to_xm)

    for k in range(CHUNKS):
        pg_in[k].wait()
        start(pg.at[chunk(k), :, lanes(x2)], far.at[0, chunk(k)], FAR(k, 0), to_xm)
        start(pg.at[chunk(k), :, lanes(4 + x2)], far.at[1, chunk(k)], FAR(k, 1), to_xp)
    send_near(0)

    for s in range(SLOTS):
        r_in[s].wait()
        start(r_h.at[s, :, lanes(zo, HALF)], rf.at[s, own_rows, :], RZ(s), to_z)
    for s in range(2):
        start(l_h.at[s], lp.at[s, pair_rows, :], LZ(s), to_z)

    def per_tile(k, step):
        def one(t, carry):
            step(t)
            return carry

        lax.fori_loop(BOUNDS[k], BOUNDS[k + 1], one, 0, unroll=2)

    for k in range(CHUNKS):
        arrived(far.at[0, chunk(k)], FAR(k, 0))
        arrived(far.at[1, chunk(k)], FAR(k, 1))

        def add_chain(t):
            chs[0, t] = (
                far[0, t].astype(F32) + pg[t, :, lanes(xm)].astype(F32)
            ).astype(BF16)
            chs[1, t] = (
                far[1, t].astype(F32) + pg[t, :, lanes(4 + xp)].astype(F32)
            ).astype(BF16)

        per_tile(k, add_chain)
        if k + 1 < CHUNKS:
            send_near(k + 1)
        start(chs.at[0, chunk(k)], ch.at[0, chunk(k)], CHAIN(k, 0), to_xm)
        start(chs.at[1, chunk(k)], ch.at[1, chunk(k)], CHAIN(k, 1), to_xp)

    def quad(chip, part, rows):
        return pl.ds(pl.multiple_of(chip * 256 + part, LANES), rows)

    for s in range(SLOTS):
        arrived(rf.at[s, own_rows, :], RZ(s))
        block = rf.at[s, quad(x, 0, 256), :]
        start(block, block, RN(s, 0), to_xp)
        start(block, block, RN(s, 1), to_xm)

    def total(half, t):
        return (
            pg[t, :, lanes(half * 4 + x)].astype(F32)
            + near[half, t].astype(F32)
            + ch[half, t].astype(F32)
        )

    for k in range(CHUNKS):
        for side in range(2):
            arrived(near.at[side, chunk(k)], NEAR(k, side))
            arrived(ch.at[side, chunk(k)], CHAIN(k, side))

        def other_half(t):
            hs[t] = total(zo, t).astype(BF16)

        per_tile(k, other_half)
        start(hs.at[chunk(k)], zrecv.at[chunk(k)], ZZ(k), to_z)

    my_block = zl * 4 + x
    other_block = zo * 4 + x
    row_of = lax.broadcasted_iota(jnp.int32, (PIECE, COLS), 0) + me * PIECE
    col_of = lax.broadcasted_iota(jnp.int32, (PIECE, COLS), 1) + my_block * COLS
    for k in range(CHUNKS):
        arrived(zrecv.at[chunk(k)], ZZ(k))

        def share(t):
            rows, cols = extent(t)
            value = total(zl, t) + zrecv[t].astype(F32)
            shares[t] = jnp.where((row_of < rows) & (col_of < cols), value, 0.0).astype(BF16)

        per_tile(k, share)
    shares[TILES] = jnp.zeros((PIECE, COLS), BF16)

    my_cols = lanes(my_block)
    my_piece = pl.ds(pl.multiple_of(me * PIECE, PIECE), PIECE)
    seats_in.wait()
    for s in range(SLOTS):

        def stage(o, carry):
            staged[s, o] = shares[tile_s[0, s * OWNERS + o]]
            return carry

        lax.fori_loop(0, OWNERS, stage, 0, unroll=4)

    def to_owners(s):
        def one(k, carry):
            o = (me + k) % OWNERS
            pltpu.make_async_remote_copy(
                src_ref=staged.at[s, o],
                dst_ref=gf.at[s, my_piece, my_cols],
                send_sem=send.at[A2A(s)],
                recv_sem=recv.at[A2A(s)],
                device_id=owner_device(o),
                device_id_type=MESH,
            ).start()
            return carry

        lax.fori_loop(1, OWNERS, one, 0)

    for s in range(SLOTS):
        to_owners(s)
    for s in range(SLOTS):
        gf[s, my_piece, my_cols] = staged[s, me]

    halves = (pl.ds(0, 512), pl.ds(512, 512))

    def g_own(s):
        arrived(staged.at[s, pl.ds(0, OWNERS - 1)], A2A(s))
        block = gf.at[s, :, my_cols]
        start(block, block, GZ(s), to_z)
        start(block, block, GN(s, 0), to_xp)
        start(block, block, GN(s, 1), to_xm)

    def g_pair(s):
        arrived(gf.at[s, :, lanes(other_block)], GZ(s))
        for turn in range(2):
            block = gf.at[s, halves[turn], lanes(other_block)]
            start(block, block, GP(s, 0, turn), to_xp)
            block = gf.at[s, halves[1 - turn], lanes(other_block)]
            start(block, block, GP(s, 1, turn), to_xm)

    def g_far(s):
        arrived(gf.at[s, :, lanes(zl * 4 + xm)], GN(s, 0))
        block = gf.at[s, halves[0], lanes(zl * 4 + xm)]
        start(block, block, GF(s, 0), to_xp)
        arrived(gf.at[s, :, lanes(zl * 4 + xp)], GN(s, 1))
        block = gf.at[s, halves[1], lanes(zl * 4 + xp)]
        start(block, block, GF(s, 1), to_xm)

    def g_far_pair(s):
        arrived(gf.at[s, halves[0], lanes(zo * 4 + xm)], GP(s, 0, 0))
        block = gf.at[s, halves[0], lanes(zo * 4 + xm)]
        start(block, block, GPF(s, 0), to_xp)
        arrived(gf.at[s, halves[1], lanes(zo * 4 + xp)], GP(s, 1, 0))
        block = gf.at[s, halves[1], lanes(zo * 4 + xp)]
        start(block, block, GPF(s, 1), to_xm)

    def g_far_here(s):
        arrived(gf.at[s, halves[0], lanes(zl * 4 + x2)], GF(s, 0))
        arrived(gf.at[s, halves[1], lanes(zl * 4 + x2)], GF(s, 1))

    def g_far_z(s):
        g_far_here(s)
        block = gf.at[s, :, lanes(zl * 4 + x2)]
        start(block, block, GZ_FAR(s), to_z)

    def g_done(s):
        if s < SLOTS - 1:
            arrived(gf.at[s, halves[0], lanes(zo * 4 + xm)], GP(s, 0, 0))
            arrived(gf.at[s, halves[1], lanes(zo * 4 + xp)], GP(s, 1, 0))
        arrived(gf.at[s, halves[1], lanes(zo * 4 + xm)], GP(s, 0, 1))
        arrived(gf.at[s, halves[0], lanes(zo * 4 + xp)], GP(s, 1, 1))
        if s < SLOTS - 1:
            arrived(gf.at[s, :, lanes(zo * 4 + x2)], GZ_FAR(s))
        else:
            arrived(gf.at[s, halves[0], lanes(zo * 4 + x2)], GPF(s, 0))
            arrived(gf.at[s, halves[1], lanes(zo * 4 + x2)], GPF(s, 1))

    def r_far(s):
        arrived(rf.at[s, quad(xm, 0, 256), :], RN(s, 0))
        block = rf.at[s, quad(xm, 0, LANES), :]
        start(block, block, RF(s, 0), to_xp)
        arrived(rf.at[s, quad(xp, 0, 256), :], RN(s, 1))
        block = rf.at[s, quad(xp, LANES, LANES), :]
        start(block, block, RF(s, 1), to_xm)

    def r_done(s):
        arrived(rf.at[s, quad(x2, 0, LANES), :], RF(s, 0))
        arrived(rf.at[s, quad(x2, LANES, LANES), :], RF(s, 1))
        arrived(lp.at[s, pair_rows, :], LZ(s))

    def grams(s):
        gt[...] = gf[s, :, lanes(d)].T
        grad_rows = gf[s, pl.ds(pl.multiple_of(d * LANES, LANES), LANES), :]

        def columns(n, carry):
            at = pl.ds(pl.multiple_of(n * 256, 256), 256)
            right = jnp.dot(gt[...], gf[s, :, at], preferred_element_type=F32)
            nr[s, :, at] = stat_decay * rs[s, :, at] + (1.0 - stat_decay) * right
            left = lax.dot_general(
                grad_rows, gf[s, at, :], (((1,), (1,)), ((), ())), preferred_element_type=F32
            )
            nl[s, :, at] = stat_decay * ls[s, :, at] + (1.0 - stat_decay) * left
            return carry

        lax.fori_loop(0, 4, columns, 0)

    out_cols = lanes(zl, HALF)

    def left_part(s, half):
        def columns(n, carry):
            at = pl.ds(pl.multiple_of(half * HALF + n * 256, 256), 256)
            part = jnp.dot(lp[s], gf[s, :, at], preferred_element_type=F32)
            tp[:, at] = part.astype(BF16)
            return carry

        lax.fori_loop(0, 2, columns, 0)

    def direction_rows(s):
        def columns(n, carry):
            at = pl.ds(pl.multiple_of(n * 256, 256), 256)
            obuf[:, at] = jnp.dot(tp[...], rf[s, :, at], preferred_element_type=F32)
            return carry

        lax.fori_loop(0, 2, columns, 0)

        def rows(i):
            value = obuf[pl.ds(pl.multiple_of(i * 8, 8), 8), :]
            ostage[s, 2 * i] = value[:4].astype(BF16)
            ostage[s, 2 * i + 1] = value[4:].astype(BF16)

        def give(i, core):
            pltpu.make_async_remote_copy(
                src_ref=ostage.at[s, 2 * i + core],
                dst_ref=ret.at[s * OWNERS + me, :, out_cols],
                send_sem=send.at[RET(s)],
                recv_sem=recv.at[RET(s)],
                device_id={
                    "dp_1": i // 16,
                    "owner_0": (i // 4) % 4,
                    "owner_1": i % 4,
                    "owner_2": core,
                },
                device_id_type=MESH,
            ).start()

        chip = here // 2
        rows((chip + 1) % 32)

        def one(k, carry):
            rows((chip + k + 1) % 32)
            give((chip + k) % 32, 0)
            give((chip + k) % 32, 1)
            return carry

        lax.fori_loop(1, 32, one, 0)
        ret[s * OWNERS + me, :, out_cols] = ostage[s, here]
        give(chip, 1 - co)

    g_own(0)
    for s in range(SLOTS):
        r_far(s)
    g_own(1)
    g_own(2)
    g_pair(0)
    start(l_h.at[2], lp.at[2, pair_rows, :], LZ(2), to_z)
    g_far(0)
    g_pair(1)
    g_far(1)
    g_pair(2)
    g_far(2)
    g_far_z(0)
    g_far_z(1)
    for s in range(SLOTS):
        l_in[s].wait()
    ls_in.wait()
    rs_in.wait()
    g_done(0)
    r_done(0)
    left_part(0, 0)
    left_part(0, 1)
    direction_rows(0)
    g_far_pair(2)
    grams(0)
    g_done(1)
    r_done(1)
    left_part(1, 0)
    left_part(1, 1)
    direction_rows(1)
    grams(1)
    r_done(2)
    g_far_here(2)
    left_part(2, zl)
    g_done(2)
    left_part(2, zo)
    direction_rows(2)
    grams(2)
    for s in range(SLOTS):
        arrived(ostage.at[s, pl.ds(0, 63)], RET(s))
    for copy in sent:
        copy.wait_send()
    for s in range(SLOTS):
        for src, sem in (
            (staged.at[s, pl.ds(0, OWNERS - 1)], A2A(s)),
            (ostage.at[s, pl.ds(0, 63)], RET(s)),
        ):
            pltpu.make_async_remote_copy(
                src_ref=src,
                dst_ref=src,
                send_sem=send.at[sem],
                recv_sem=recv.at[sem],
                device_id=to_xp,
                device_id_type=MESH,
            ).wait_send()


def write_out(owner_s, ret, nl, nr, dir_h, nl_h, nr_h, rows_v, count_s, sems):
    copies = [
        pltpu.make_async_copy(nl, nl_h, sems.at[0]),
        pltpu.make_async_copy(nr, nr_h, sems.at[1]),
    ]
    for copy in copies:
        copy.start()
    d = lax.axis_index(DP)
    me = lax.axis_index(OWNER)
    line = lax.broadcasted_iota(jnp.int32, (4, TILE), 0) + (d * LANES + me * 4)
    lane = lax.broadcasted_iota(jnp.int32, (4, TILE), 1)

    def clear(o, carry):
        count_s[o] = 0
        return carry

    lax.fori_loop(0, OWNERS, clear, 0, unroll=8)

    def write(t, carry):
        rows, cols = extent(t)
        owner = owner_s[t]
        taken = count_s[owner]
        count_s[owner] = taken + OWNERS
        value = ret[taken + owner].astype(F32)
        rows_v[t] = jnp.where((line < rows) & (lane < cols), value, 0.0).astype(BF16)
        return carry

    lax.fori_loop(0, TILES, write, 0, unroll=4)
    copies.append(pltpu.make_async_copy(rows_v, dir_h, sems.at[2]))
    copies[2].start()
    for copy in copies:
        copy.wait()


def body(partial_grads, owner_map, left_stats, right_stats, left_roots, right_roots):
    smem = pl.BlockSpec(memory_space=pltpu.SMEM)
    vmem = pl.BlockSpec(memory_space=pltpu.VMEM)
    hbm = pl.BlockSpec(memory_space=pltpu.HBM)
    returned, new_left, new_right = pl.pallas_call(
        kernel,
        out_shape=(
            pltpu.VMEM((SLOTS * OWNERS, 4, TILE), BF16),
            pltpu.VMEM((SLOTS, LANES, TILE), F32),
            pltpu.VMEM((SLOTS, LANES, TILE), F32),
        ),
        in_specs=[smem, hbm, hbm, hbm, hbm, hbm],
        out_specs=(vmem, vmem, vmem),
        scratch_shapes=[
            pltpu.VMEM((TILES, PIECE, TILE), BF16),
            pltpu.VMEM((2, TILES, PIECE, COLS), BF16),
            pltpu.VMEM((2, TILES, PIECE, COLS), BF16),
            pltpu.VMEM((2, TILES, PIECE, COLS), BF16),
            pltpu.VMEM((2, TILES, PIECE, COLS), BF16),
            pltpu.VMEM((TILES, PIECE, COLS), BF16),
            pltpu.VMEM((TILES, PIECE, COLS), BF16),
            pltpu.VMEM((TILES + 1, PIECE, COLS), BF16),
            pltpu.VMEM((SLOTS, OWNERS, PIECE, COLS), BF16),
            pltpu.VMEM((SLOTS, TILE, TILE), BF16),
            pltpu.VMEM((SLOTS, TILE, HALF), BF16),
            pltpu.VMEM((SLOTS, 256, TILE), BF16),
            pltpu.VMEM((SLOTS, LANES, TILE), F32),
            pltpu.VMEM((SLOTS, LANES, TILE), F32),
            pltpu.VMEM((LANES, TILE), BF16),
            pltpu.VMEM((256, TILE), BF16),
            pltpu.VMEM((256, HALF), F32),
            pltpu.VMEM((SLOTS, 64, 4, HALF), BF16),
            pltpu.VMEM((1, LANES), jnp.int32),
            pltpu.SMEM((1, LANES), jnp.int32),
            pltpu.SemaphoreType.DMA((N_SEMS,)),
            pltpu.SemaphoreType.DMA((N_SEMS,)),
            pltpu.SemaphoreType.DMA((N_LOC,)),
        ],
        compiler_params=pltpu.CompilerParams(
            collective_id=0, has_side_effects=True, vmem_limit_bytes=60 * 1024 * 1024
        ),
    )(
        owner_map,
        partial_grads[0],
        left_roots[0],
        right_roots[0],
        left_stats[0],
        right_stats[0],
    )
    direction, new_left, new_right = pl.pallas_call(
        write_out,
        out_shape=(
            jax.ShapeDtypeStruct((TILES, 4, TILE), BF16),
            jax.ShapeDtypeStruct((SLOTS, LANES, TILE), F32),
            jax.ShapeDtypeStruct((SLOTS, LANES, TILE), F32),
        ),
        in_specs=[smem, vmem, vmem, vmem],
        out_specs=(hbm, hbm, hbm),
        scratch_shapes=[
            pltpu.VMEM((TILES, 4, TILE), BF16),
            pltpu.SMEM((OWNERS,), jnp.int32),
            pltpu.SemaphoreType.DMA((3,)),
        ],
        compiler_params=pltpu.CompilerParams(vmem_limit_bytes=4 * 1024 * 1024),
    )(
        owner_map,
        *(
            pltpu.with_memory_space_constraint(value, pltpu.VMEM)
            for value in (returned, new_left, new_right)
        ),
    )
    return direction, new_left[None], new_right[None]


def solution(mesh):
    torus = Mesh(
        mesh.devices.reshape(4, 2, 4, 4, 2), ("dp_0", "dp_1", "owner_0", "owner_1", "owner_2")
    )
    in_specs = (
        P(DP, None, OWNER, None),
        P(),
        P(OWNER, None, DP, None),
        P(OWNER, None, DP, None),
        P(OWNER, None, DP, None),
        P(OWNER, None, DP, None),
    )
    out_specs = (P(None, DP_OWNER, None), P(OWNER, None, DP, None), P(OWNER, None, DP, None))
    return jax.shard_map(body, mesh=torus, in_specs=in_specs, out_specs=out_specs, check_vma=False)
```

```python
import jax
import jax.numpy as jnp
from jax import lax
from jax.experimental import pallas as pl
from jax.experimental.pallas import tpu as pltpu
from jax.sharding import Mesh
from jax.sharding import PartitionSpec as P

D_MODEL = 2560
D_IN = 10576
D_INNER = 5120
TILE = 1024
TILES = 48
OWNERS = 32
SLOTS = 3
PIECE = 32
LANES = 128
COLS = 128
HALF = 512
BOUNDS = (0, 14, 28, 42, 48)
CHUNKS = len(BOUNDS) - 1
OWNER = ("owner_0", "owner_1", "owner_2")
DP = ("dp_0", "dp_1")
DP_OWNER = ("dp_0", "dp_1", "owner_0", "owner_1", "owner_2")
MESH = pl.DeviceIdType.MESH
F32 = jnp.float32
BF16 = jnp.bfloat16

stat_decay = 0.999


def extent(t):
    in_cols = -(-D_IN // TILE)
    out_cols = -(-D_MODEL // TILE)
    in_count = -(-D_MODEL // TILE) * in_cols
    other = jnp.maximum(t - in_count, 0)
    is_in = t < in_count
    rows = jnp.where(
        is_in,
        jnp.minimum(TILE, D_MODEL - t // in_cols * TILE),
        jnp.minimum(TILE, D_INNER - other // out_cols * TILE),
    )
    cols = jnp.where(
        is_in,
        jnp.minimum(TILE, D_IN - t % in_cols * TILE),
        jnp.minimum(TILE, D_MODEL - other % out_cols * TILE),
    )
    return rows, cols


class Ids:
    def __init__(self):
        self.n = 0

    def __call__(self, *shape):
        size = 1
        for s in shape:
            size *= s
        base = self.n
        self.n += size

        def at(*index):
            flat = 0
            for i, s in zip(index, shape):
                flat = flat * s + i
            return base + flat

        return at


IDS = Ids()
FAR = IDS(CHUNKS, 2)
NEAR = IDS(CHUNKS, 2)
CHAIN = IDS(CHUNKS, 2)
ZZ = IDS(CHUNKS)
RZ = IDS(SLOTS)
RN = IDS(SLOTS, 2)
RF = IDS(SLOTS, 2)
LZ = IDS(SLOTS)
A2A = IDS(SLOTS)
GZ = IDS(SLOTS)
GZ_FAR = IDS(SLOTS)
GN = IDS(SLOTS, 2)
GP = IDS(SLOTS, 2, 2)
GF = IDS(SLOTS, 2)
GPF = IDS(SLOTS, 2)
RET = IDS(SLOTS)
N_SEMS = IDS.n
LOC = Ids()
L_PG = LOC(CHUNKS)
L_R = LOC(SLOTS)
L_L = LOC(SLOTS)
L_LS = LOC(1)
L_RS = LOC(1)
L_SEAT = LOC(1)
N_LOC = LOC.n


def kernel(
    owner_s,
    pg_h,
    l_h,
    r_h,
    ls_h,
    rs_h,
    ret,
    nl,
    nr,
    pg,
    far,
    chs,
    near,
    ch,
    hs,
    zrecv,
    shares,
    staged,
    gf,
    rf,
    lp,
    ls,
    rs,
    gt,
    tp,
    obuf,
    ostage,
    tile_v,
    tile_s,
    send,
    recv,
    local,
    told,
):
    x = lax.axis_index("dp_0")
    zl = lax.axis_index("dp_1")
    y = lax.axis_index("owner_0")
    zh = lax.axis_index("owner_1")
    co = lax.axis_index("owner_2")
    me = (y * 4 + zh) * 2 + co
    d = x * 2 + zl
    xp = (x + 1) % 4
    xm = (x + 3) % 4
    x2 = (x + 2) % 4
    zo = 1 - zl
    here = zl * 32 + me
    to_xp = {"dp_0": xp}
    to_xm = {"dp_0": xm}
    to_z = {"dp_1": zo}

    def owner_device(i):
        return {"owner_0": i // 8, "owner_1": (i // 2) % 4, "owner_2": i % 2}

    def any_device(i):
        return {
            "dp_1": i // 32,
            "owner_0": (i // 8) % 4,
            "owner_1": (i // 2) % 4,
            "owner_2": i % 2,
        }

    sent = []

    def start(src, dst, sem, device):
        copy = pltpu.make_async_remote_copy(
            src_ref=src,
            dst_ref=dst,
            send_sem=send.at[sem],
            recv_sem=recv.at[sem],
            device_id=device,
            device_id_type=MESH,
        )
        copy.start()
        sent.append(copy)

    def arrived(dst, sem):
        pltpu.make_async_remote_copy(
            src_ref=dst,
            dst_ref=dst,
            send_sem=send.at[sem],
            recv_sem=recv.at[sem],
            device_id=to_xp,
            device_id_type=MESH,
        ).wait_recv()

    def lanes(block, width=COLS):
        return pl.ds(pl.multiple_of(block * width, width), width)

    def chunk(k):
        return pl.ds(BOUNDS[k], BOUNDS[k + 1] - BOUNDS[k])

    pg_in = [
        pltpu.make_async_copy(pg_h.at[chunk(k)], pg.at[chunk(k)], local.at[L_PG(k)])
        for k in range(CHUNKS)
    ]
    for copy in pg_in:
        copy.start()
    own_rows = pl.ds(pl.multiple_of(d * LANES, LANES), LANES)
    pair_rows = pl.ds(pl.multiple_of(zl * LANES, LANES), LANES)
    r_in = [
        pltpu.make_async_copy(
            r_h.at[s, :, lanes(zl, HALF)], rf.at[s, own_rows, :], local.at[L_R(s)]
        )
        for s in range(SLOTS)
    ]
    l_in = [
        pltpu.make_async_copy(l_h.at[s], lp.at[s, pair_rows, :], local.at[L_L(s)])
        for s in range(SLOTS)
    ]
    ls_in = pltpu.make_async_copy(ls_h, ls, local.at[L_LS(0)])
    rs_in = pltpu.make_async_copy(rs_h, rs, local.at[L_RS(0)])
    for copy in (*r_in, *l_in, ls_in, rs_in):
        copy.start()

    barrier = pltpu.get_barrier_semaphore()
    to_core = {"owner_2": 1 - co}
    y_sides = ({"owner_0": (y + 1) % 4}, {"owner_0": (y + 3) % 4})
    zh_sides = ({"owner_1": (zh + 1) % 4}, {"owner_1": (zh + 3) % 4})
    neighbours = (to_xp, to_xm, to_z, to_core, *y_sides, *zh_sides)
    for device in neighbours:
        pl.semaphore_signal(barrier, inc=1, device_id=device, device_id_type=MESH)

    seat = lax.broadcasted_iota(jnp.int32, (1, LANES), 1)

    def take(t, carry):
        tile, count = carry
        mine = seat % OWNERS == owner_s[t]
        tile = jnp.where(mine & (count == seat // OWNERS), t, tile)
        return tile, count + mine.astype(jnp.int32)

    tile_v[...], _ = lax.fori_loop(
        0, TILES, take, (jnp.full((1, LANES), TILES, jnp.int32), jnp.zeros((1, LANES), jnp.int32))
    )
    seats_in = pltpu.make_async_copy(tile_v, tile_s, local.at[L_SEAT(0)])
    seats_in.start()
    pl.semaphore_wait(barrier, len(neighbours))

    rounds = (y_sides, zh_sides, zh_sides, (to_core,), (to_z,))

    def tell(n):
        for device in rounds[n]:
            pl.semaphore_signal(told.at[n], inc=1, device_id=device, device_id_type=MESH)

    def heard(n):
        pl.semaphore_wait(told.at[n], len(rounds[n]))

    def send_near(k):
        start(pg.at[chunk(k), :, lanes(xp)], near.at[0, chunk(k)], NEAR(k, 0), to_xp)
        start(pg.at[chunk(k), :, lanes(4 + xm)], near.at[1, chunk(k)], NEAR(k, 1), to_xm)

    for k in range(CHUNKS):
        pg_in[k].wait()
        start(pg.at[chunk(k), :, lanes(x2)], far.at[0, chunk(k)], FAR(k, 0), to_xm)
        start(pg.at[chunk(k), :, lanes(4 + x2)], far.at[1, chunk(k)], FAR(k, 1), to_xp)
    send_near(0)
    tell(0)

    for s in range(SLOTS):
        r_in[s].wait()
        start(r_h.at[s, :, lanes(zo, HALF)], rf.at[s, own_rows, :], RZ(s), to_z)
    for s in range(2):
        start(l_h.at[s], lp.at[s, pair_rows, :], LZ(s), to_z)

    def per_tile(k, step):
        def one(t, carry):
            step(t)
            return carry

        lax.fori_loop(BOUNDS[k], BOUNDS[k + 1], one, 0, unroll=2)

    for k in range(CHUNKS):
        arrived(far.at[0, chunk(k)], FAR(k, 0))
        arrived(far.at[1, chunk(k)], FAR(k, 1))

        def add_chain(t):
            chs[0, t] = (
                far[0, t].astype(F32) + pg[t, :, lanes(xm)].astype(F32)
            ).astype(BF16)
            chs[1, t] = (
                far[1, t].astype(F32) + pg[t, :, lanes(4 + xp)].astype(F32)
            ).astype(BF16)

        per_tile(k, add_chain)
        if k + 1 < CHUNKS:
            send_near(k + 1)
        heard(k)
        tell(k + 1)
        start(chs.at[0, chunk(k)], ch.at[0, chunk(k)], CHAIN(k, 0), to_xm)
        start(chs.at[1, chunk(k)], ch.at[1, chunk(k)], CHAIN(k, 1), to_xp)

    def quad(chip, part, rows):
        return pl.ds(pl.multiple_of(chip * 256 + part, LANES), rows)

    for s in range(SLOTS):
        arrived(rf.at[s, own_rows, :], RZ(s))
        block = rf.at[s, quad(x, 0, 256), :]
        start(block, block, RN(s, 0), to_xp)
        start(block, block, RN(s, 1), to_xm)

    def total(half, t):
        return (
            pg[t, :, lanes(half * 4 + x)].astype(F32)
            + near[half, t].astype(F32)
            + ch[half, t].astype(F32)
        )

    for k in range(CHUNKS):
        for side in range(2):
            arrived(near.at[side, chunk(k)], NEAR(k, side))
            arrived(ch.at[side, chunk(k)], CHAIN(k, side))

        def other_half(t):
            hs[t] = total(zo, t).astype(BF16)

        per_tile(k, other_half)
        start(hs.at[chunk(k)], zrecv.at[chunk(k)], ZZ(k), to_z)

    my_block = zl * 4 + x
    other_block = zo * 4 + x
    row_of = lax.broadcasted_iota(jnp.int32, (PIECE, COLS), 0) + me * PIECE
    col_of = lax.broadcasted_iota(jnp.int32, (PIECE, COLS), 1) + my_block * COLS
    for k in range(CHUNKS):
        arrived(zrecv.at[chunk(k)], ZZ(k))

        def share(t):
            rows, cols = extent(t)
            value = total(zl, t) + zrecv[t].astype(F32)
            shares[t] = jnp.where((row_of < rows) & (col_of < cols), value, 0.0).astype(BF16)

        per_tile(k, share)
    shares[TILES] = jnp.zeros((PIECE, COLS), BF16)

    my_cols = lanes(my_block)
    my_piece = pl.ds(pl.multiple_of(me * PIECE, PIECE), PIECE)
    seats_in.wait()
    for s in range(SLOTS):

        def stage(o, carry):
            staged[s, o] = shares[tile_s[0, s * OWNERS + o]]
            return carry

        lax.fori_loop(0, OWNERS, stage, 0, unroll=4)

    def to_owners(s):
        def one(k, carry):
            o = (me + k) % OWNERS
            pltpu.make_async_remote_copy(
                src_ref=staged.at[s, o],
                dst_ref=gf.at[s, my_piece, my_cols],
                send_sem=send.at[A2A(s)],
                recv_sem=recv.at[A2A(s)],
                device_id=owner_device(o),
                device_id_type=MESH,
            ).start()
            return carry

        lax.fori_loop(1, OWNERS, one, 0)

    heard(4)
    for s in range(SLOTS):
        to_owners(s)
    for s in range(SLOTS):
        gf[s, my_piece, my_cols] = staged[s, me]

    halves = (pl.ds(0, 512), pl.ds(512, 512))

    def g_own(s):
        arrived(staged.at[s, pl.ds(0, OWNERS - 1)], A2A(s))
        block = gf.at[s, :, my_cols]
        start(block, block, GZ(s), to_z)
        start(block, block, GN(s, 0), to_xp)
        start(block, block, GN(s, 1), to_xm)

    def g_pair(s):
        arrived(gf.at[s, :, lanes(other_block)], GZ(s))
        for turn in range(2):
            block = gf.at[s, halves[turn], lanes(other_block)]
            start(block, block, GP(s, 0, turn), to_xp)
            block = gf.at[s, halves[1 - turn], lanes(other_block)]
            start(block, block, GP(s, 1, turn), to_xm)

    def g_far(s):
        arrived(gf.at[s, :, lanes(zl * 4 + xm)], GN(s, 0))
        block = gf.at[s, halves[0], lanes(zl * 4 + xm)]
        start(block, block, GF(s, 0), to_xp)
        arrived(gf.at[s, :, lanes(zl * 4 + xp)], GN(s, 1))
        block = gf.at[s, halves[1], lanes(zl * 4 + xp)]
        start(block, block, GF(s, 1), to_xm)

    def g_far_pair(s):
        arrived(gf.at[s, halves[0], lanes(zo * 4 + xm)], GP(s, 0, 0))
        block = gf.at[s, halves[0], lanes(zo * 4 + xm)]
        start(block, block, GPF(s, 0), to_xp)
        arrived(gf.at[s, halves[1], lanes(zo * 4 + xp)], GP(s, 1, 0))
        block = gf.at[s, halves[1], lanes(zo * 4 + xp)]
        start(block, block, GPF(s, 1), to_xm)

    def g_far_here(s):
        arrived(gf.at[s, halves[0], lanes(zl * 4 + x2)], GF(s, 0))
        arrived(gf.at[s, halves[1], lanes(zl * 4 + x2)], GF(s, 1))

    def g_far_z(s):
        g_far_here(s)
        block = gf.at[s, :, lanes(zl * 4 + x2)]
        start(block, block, GZ_FAR(s), to_z)

    def g_done(s):
        if s < SLOTS - 1:
            arrived(gf.at[s, halves[0], lanes(zo * 4 + xm)], GP(s, 0, 0))
            arrived(gf.at[s, halves[1], lanes(zo * 4 + xp)], GP(s, 1, 0))
        arrived(gf.at[s, halves[1], lanes(zo * 4 + xm)], GP(s, 0, 1))
        arrived(gf.at[s, halves[0], lanes(zo * 4 + xp)], GP(s, 1, 1))
        if s < SLOTS - 1:
            arrived(gf.at[s, :, lanes(zo * 4 + x2)], GZ_FAR(s))
        else:
            arrived(gf.at[s, halves[0], lanes(zo * 4 + x2)], GPF(s, 0))
            arrived(gf.at[s, halves[1], lanes(zo * 4 + x2)], GPF(s, 1))

    def r_far(s):
        arrived(rf.at[s, quad(xm, 0, 256), :], RN(s, 0))
        block = rf.at[s, quad(xm, 0, LANES), :]
        start(block, block, RF(s, 0), to_xp)
        arrived(rf.at[s, quad(xp, 0, 256), :], RN(s, 1))
        block = rf.at[s, quad(xp, LANES, LANES), :]
        start(block, block, RF(s, 1), to_xm)

    def r_done(s):
        arrived(rf.at[s, quad(x2, 0, LANES), :], RF(s, 0))
        arrived(rf.at[s, quad(x2, LANES, LANES), :], RF(s, 1))
        arrived(lp.at[s, pair_rows, :], LZ(s))

    def grams(s):
        gt[...] = gf[s, :, lanes(d)].T
        grad_rows = gf[s, pl.ds(pl.multiple_of(d * LANES, LANES), LANES), :]

        def columns(n, carry):
            at = pl.ds(pl.multiple_of(n * 256, 256), 256)
            right = jnp.dot(gt[...], gf[s, :, at], preferred_element_type=F32)
            nr[s, :, at] = stat_decay * rs[s, :, at] + (1.0 - stat_decay) * right
            left = lax.dot_general(
                grad_rows, gf[s, at, :], (((1,), (1,)), ((), ())), preferred_element_type=F32
            )
            nl[s, :, at] = stat_decay * ls[s, :, at] + (1.0 - stat_decay) * left
            return carry

        lax.fori_loop(0, 4, columns, 0)

    out_cols = lanes(zl, HALF)

    def left_part(s, half):
        def columns(n, carry):
            at = pl.ds(pl.multiple_of(half * HALF + n * 256, 256), 256)
            part = jnp.dot(lp[s], gf[s, :, at], preferred_element_type=F32)
            tp[:, at] = part.astype(BF16)
            return carry

        lax.fori_loop(0, 2, columns, 0)

    def direction_rows(s):
        def columns(n, carry):
            at = pl.ds(pl.multiple_of(n * 256, 256), 256)
            obuf[:, at] = jnp.dot(tp[...], rf[s, :, at], preferred_element_type=F32)
            return carry

        lax.fori_loop(0, 2, columns, 0)

        def rows(i):
            value = obuf[pl.ds(pl.multiple_of(i * 8, 8), 8), :]
            ostage[s, 2 * i] = value[:4].astype(BF16)
            ostage[s, 2 * i + 1] = value[4:].astype(BF16)

        def give(i, core):
            pltpu.make_async_remote_copy(
                src_ref=ostage.at[s, 2 * i + core],
                dst_ref=ret.at[s * OWNERS + me, :, out_cols],
                send_sem=send.at[RET(s)],
                recv_sem=recv.at[RET(s)],
                device_id={
                    "dp_1": i // 16,
                    "owner_0": (i // 4) % 4,
                    "owner_1": i % 4,
                    "owner_2": core,
                },
                device_id_type=MESH,
            ).start()

        chip = here // 2
        rows((chip + 1) % 32)

        def one(k, carry):
            rows((chip + k + 1) % 32)
            give((chip + k) % 32, 0)
            give((chip + k) % 32, 1)
            return carry

        lax.fori_loop(1, 32, one, 0)
        ret[s * OWNERS + me, :, out_cols] = ostage[s, here]
        give(chip, 1 - co)

    g_own(0)
    for s in range(SLOTS):
        r_far(s)
    g_own(1)
    g_own(2)
    g_pair(0)
    start(l_h.at[2], lp.at[2, pair_rows, :], LZ(2), to_z)
    g_far(0)
    g_pair(1)
    g_far(1)
    g_pair(2)
    g_far(2)
    g_far_z(0)
    g_far_z(1)
    for s in range(SLOTS):
        l_in[s].wait()
    ls_in.wait()
    rs_in.wait()
    g_done(0)
    r_done(0)
    left_part(0, 0)
    left_part(0, 1)
    direction_rows(0)
    g_far_pair(2)
    grams(0)
    g_done(1)
    r_done(1)
    left_part(1, 0)
    left_part(1, 1)
    direction_rows(1)
    r_done(2)
    g_far_here(2)
    left_part(2, zl)
    g_done(2)
    left_part(2, zo)
    direction_rows(2)
    grams(1)
    grams(2)
    for s in range(SLOTS):
        arrived(ostage.at[s, pl.ds(0, 63)], RET(s))
    for copy in sent:
        copy.wait_send()
    for s in range(SLOTS):
        for src, sem in (
            (staged.at[s, pl.ds(0, OWNERS - 1)], A2A(s)),
            (ostage.at[s, pl.ds(0, 63)], RET(s)),
        ):
            pltpu.make_async_remote_copy(
                src_ref=src,
                dst_ref=src,
                send_sem=send.at[sem],
                recv_sem=recv.at[sem],
                device_id=to_xp,
                device_id_type=MESH,
            ).wait_send()


def write_out(owner_s, ret, nl, nr, dir_h, nl_h, nr_h, rows_v, count_s, sems):
    copies = [
        pltpu.make_async_copy(nl, nl_h, sems.at[0]),
        pltpu.make_async_copy(nr, nr_h, sems.at[1]),
    ]
    for copy in copies:
        copy.start()
    d = lax.axis_index(DP)
    me = lax.axis_index(OWNER)
    line = lax.broadcasted_iota(jnp.int32, (4, TILE), 0) + (d * LANES + me * 4)
    lane = lax.broadcasted_iota(jnp.int32, (4, TILE), 1)

    def clear(o, carry):
        count_s[o] = 0
        return carry

    lax.fori_loop(0, OWNERS, clear, 0, unroll=8)

    def write(t, carry):
        rows, cols = extent(t)
        owner = owner_s[t]
        taken = count_s[owner]
        count_s[owner] = taken + OWNERS
        value = ret[taken + owner].astype(F32)
        rows_v[t] = jnp.where((line < rows) & (lane < cols), value, 0.0).astype(BF16)
        return carry

    lax.fori_loop(0, TILES, write, 0, unroll=4)
    copies.append(pltpu.make_async_copy(rows_v, dir_h, sems.at[2]))
    copies[2].start()
    for copy in copies:
        copy.wait()


def body(partial_grads, owner_map, left_stats, right_stats, left_roots, right_roots):
    smem = pl.BlockSpec(memory_space=pltpu.SMEM)
    vmem = pl.BlockSpec(memory_space=pltpu.VMEM)
    hbm = pl.BlockSpec(memory_space=pltpu.HBM)
    returned, new_left, new_right = pl.pallas_call(
        kernel,
        out_shape=(
            pltpu.VMEM((SLOTS * OWNERS, 4, TILE), BF16),
            pltpu.VMEM((SLOTS, LANES, TILE), F32),
            pltpu.VMEM((SLOTS, LANES, TILE), F32),
        ),
        in_specs=[smem, hbm, hbm, hbm, hbm, hbm],
        out_specs=(vmem, vmem, vmem),
        scratch_shapes=[
            pltpu.VMEM((TILES, PIECE, TILE), BF16),
            pltpu.VMEM((2, TILES, PIECE, COLS), BF16),
            pltpu.VMEM((2, TILES, PIECE, COLS), BF16),
            pltpu.VMEM((2, TILES, PIECE, COLS), BF16),
            pltpu.VMEM((2, TILES, PIECE, COLS), BF16),
            pltpu.VMEM((TILES, PIECE, COLS), BF16),
            pltpu.VMEM((TILES, PIECE, COLS), BF16),
            pltpu.VMEM((TILES + 1, PIECE, COLS), BF16),
            pltpu.VMEM((SLOTS, OWNERS, PIECE, COLS), BF16),
            pltpu.VMEM((SLOTS, TILE, TILE), BF16),
            pltpu.VMEM((SLOTS, TILE, HALF), BF16),
            pltpu.VMEM((SLOTS, 256, TILE), BF16),
            pltpu.VMEM((SLOTS, LANES, TILE), F32),
            pltpu.VMEM((SLOTS, LANES, TILE), F32),
            pltpu.VMEM((LANES, TILE), BF16),
            pltpu.VMEM((256, TILE), BF16),
            pltpu.VMEM((256, HALF), F32),
            pltpu.VMEM((SLOTS, 64, 4, HALF), BF16),
            pltpu.VMEM((1, LANES), jnp.int32),
            pltpu.SMEM((1, LANES), jnp.int32),
            pltpu.SemaphoreType.DMA((N_SEMS,)),
            pltpu.SemaphoreType.DMA((N_SEMS,)),
            pltpu.SemaphoreType.DMA((N_LOC,)),
            pltpu.SemaphoreType.REGULAR((5,)),
        ],
        compiler_params=pltpu.CompilerParams(
            collective_id=0, has_side_effects=True, vmem_limit_bytes=60 * 1024 * 1024
        ),
    )(
        owner_map,
        partial_grads[0],
        left_roots[0],
        right_roots[0],
        left_stats[0],
        right_stats[0],
    )
    direction, new_left, new_right = pl.pallas_call(
        write_out,
        out_shape=(
            jax.ShapeDtypeStruct((TILES, 4, TILE), BF16),
            jax.ShapeDtypeStruct((SLOTS, LANES, TILE), F32),
            jax.ShapeDtypeStruct((SLOTS, LANES, TILE), F32),
        ),
        in_specs=[smem, vmem, vmem, vmem],
        out_specs=(hbm, hbm, hbm),
        scratch_shapes=[
            pltpu.VMEM((TILES, 4, TILE), BF16),
            pltpu.SMEM((OWNERS,), jnp.int32),
            pltpu.SemaphoreType.DMA((3,)),
        ],
        compiler_params=pltpu.CompilerParams(vmem_limit_bytes=4 * 1024 * 1024),
    )(
        owner_map,
        *(
            pltpu.with_memory_space_constraint(value, pltpu.VMEM)
            for value in (returned, new_left, new_right)
        ),
    )
    return direction, new_left[None], new_right[None]


def solution(mesh):
    torus = Mesh(
        mesh.devices.reshape(4, 2, 4, 4, 2), ("dp_0", "dp_1", "owner_0", "owner_1", "owner_2")
    )
    in_specs = (
        P(DP, None, OWNER, None),
        P(),
        P(OWNER, None, DP, None),
        P(OWNER, None, DP, None),
        P(OWNER, None, DP, None),
        P(OWNER, None, DP, None),
    )
    out_specs = (P(None, DP_OWNER, None), P(OWNER, None, DP, None), P(OWNER, None, DP, None))
    return jax.shard_map(body, mesh=torus, in_specs=in_specs, out_specs=out_specs, check_vma=False)
```

```python
import jax
import jax.numpy as jnp
from jax import lax
from jax.experimental import pallas as pl
from jax.experimental.pallas import tpu as pltpu
from jax.sharding import Mesh
from jax.sharding import PartitionSpec as P

D_MODEL = 2560
D_IN = 10576
D_INNER = 5120
TILE = 1024
TILES = 48
OWNERS = 32
SLOTS = 3
PIECE = 32
LANES = 128
COLS = 128
HALF = 512
BOUNDS = (0, 14, 28, 42, 48)
CHUNKS = len(BOUNDS) - 1
OWNER = ("owner_0", "owner_1", "owner_2")
DP = ("dp_0", "dp_1")
DP_OWNER = ("dp_0", "dp_1", "owner_0", "owner_1", "owner_2")
MESH = pl.DeviceIdType.MESH
F32 = jnp.float32
BF16 = jnp.bfloat16

stat_decay = 0.999


def extent(t):
    in_cols = -(-D_IN // TILE)
    out_cols = -(-D_MODEL // TILE)
    in_count = -(-D_MODEL // TILE) * in_cols
    other = jnp.maximum(t - in_count, 0)
    is_in = t < in_count
    rows = jnp.where(
        is_in,
        jnp.minimum(TILE, D_MODEL - t // in_cols * TILE),
        jnp.minimum(TILE, D_INNER - other // out_cols * TILE),
    )
    cols = jnp.where(
        is_in,
        jnp.minimum(TILE, D_IN - t % in_cols * TILE),
        jnp.minimum(TILE, D_MODEL - other % out_cols * TILE),
    )
    return rows, cols


class Ids:
    def __init__(self):
        self.n = 0

    def __call__(self, *shape):
        size = 1
        for s in shape:
            size *= s
        base = self.n
        self.n += size

        def at(*index):
            flat = 0
            for i, s in zip(index, shape):
                flat = flat * s + i
            return base + flat

        return at


IDS = Ids()
FAR = IDS(CHUNKS, 2)
NEAR = IDS(CHUNKS, 2)
CHAIN = IDS(CHUNKS, 2)
ZZ = IDS(CHUNKS)
RZ = IDS(SLOTS)
RN = IDS(SLOTS, 2)
RF = IDS(SLOTS, 2)
LZ = IDS(SLOTS)
A2A = IDS(SLOTS)
GZ = IDS(SLOTS)
GZ_FAR = IDS(SLOTS)
GN = IDS(SLOTS, 2)
GP = IDS(SLOTS, 2, 2)
GF = IDS(SLOTS, 2)
GPF = IDS(SLOTS, 2)
RET = IDS(SLOTS)
N_SEMS = IDS.n
LOC = Ids()
L_PG = LOC(CHUNKS)
L_R = LOC(SLOTS)
L_L = LOC(SLOTS)
L_LS = LOC(1)
L_RS = LOC(1)
L_SEAT = LOC(1)
N_LOC = LOC.n


def kernel(
    owner_s,
    pg_h,
    l_h,
    r_h,
    ls_h,
    rs_h,
    ret,
    nl,
    nr,
    pg,
    far,
    chs,
    near,
    ch,
    hs,
    zrecv,
    shares,
    staged,
    gf,
    rf,
    lp,
    ls,
    rs,
    gt,
    tp,
    obuf,
    ostage,
    tile_v,
    tile_s,
    send,
    recv,
    local,
    told,
):
    x = lax.axis_index("dp_0")
    zl = lax.axis_index("dp_1")
    y = lax.axis_index("owner_0")
    zh = lax.axis_index("owner_1")
    co = lax.axis_index("owner_2")
    me = (y * 4 + zh) * 2 + co
    d = x * 2 + zl
    xp = (x + 1) % 4
    xm = (x + 3) % 4
    x2 = (x + 2) % 4
    zo = 1 - zl
    here = zl * 32 + me
    to_xp = {"dp_0": xp}
    to_xm = {"dp_0": xm}
    to_z = {"dp_1": zo}

    def owner_device(i):
        return {"owner_0": i // 8, "owner_1": (i // 2) % 4, "owner_2": i % 2}

    def any_device(i):
        return {
            "dp_1": i // 32,
            "owner_0": (i // 8) % 4,
            "owner_1": (i // 2) % 4,
            "owner_2": i % 2,
        }

    sent = []

    def start(src, dst, sem, device):
        copy = pltpu.make_async_remote_copy(
            src_ref=src,
            dst_ref=dst,
            send_sem=send.at[sem],
            recv_sem=recv.at[sem],
            device_id=device,
            device_id_type=MESH,
        )
        copy.start()
        sent.append(copy)

    def arrived(dst, sem):
        pltpu.make_async_remote_copy(
            src_ref=dst,
            dst_ref=dst,
            send_sem=send.at[sem],
            recv_sem=recv.at[sem],
            device_id=to_xp,
            device_id_type=MESH,
        ).wait_recv()

    def lanes(block, width=COLS):
        return pl.ds(pl.multiple_of(block * width, width), width)

    def chunk(k):
        return pl.ds(BOUNDS[k], BOUNDS[k + 1] - BOUNDS[k])

    pg_in = [
        pltpu.make_async_copy(pg_h.at[chunk(k)], pg.at[chunk(k)], local.at[L_PG(k)])
        for k in range(CHUNKS)
    ]
    for copy in pg_in:
        copy.start()
    own_rows = pl.ds(pl.multiple_of(d * LANES, LANES), LANES)
    pair_rows = pl.ds(pl.multiple_of(zl * LANES, LANES), LANES)
    r_in = [
        pltpu.make_async_copy(
            r_h.at[s, :, lanes(zl, HALF)], rf.at[s, own_rows, :], local.at[L_R(s)]
        )
        for s in range(SLOTS)
    ]
    l_in = [
        pltpu.make_async_copy(l_h.at[s], lp.at[s, pair_rows, :], local.at[L_L(s)])
        for s in range(SLOTS)
    ]
    ls_in = pltpu.make_async_copy(ls_h, ls, local.at[L_LS(0)])
    rs_in = pltpu.make_async_copy(rs_h, rs, local.at[L_RS(0)])
    for copy in (*r_in, *l_in, ls_in, rs_in):
        copy.start()

    barrier = pltpu.get_barrier_semaphore()
    to_core = {"owner_2": 1 - co}
    y_sides = ({"owner_0": (y + 1) % 4}, {"owner_0": (y + 3) % 4})
    zh_sides = ({"owner_1": (zh + 1) % 4}, {"owner_1": (zh + 3) % 4})
    neighbours = (to_xp, to_xm, to_z, to_core, *y_sides, *zh_sides)
    for device in neighbours:
        pl.semaphore_signal(barrier, inc=1, device_id=device, device_id_type=MESH)

    seat = lax.broadcasted_iota(jnp.int32, (1, LANES), 1)

    def take(t, carry):
        tile, count = carry
        mine = seat % OWNERS == owner_s[t]
        tile = jnp.where(mine & (count == seat // OWNERS), t, tile)
        return tile, count + mine.astype(jnp.int32)

    tile_v[...], _ = lax.fori_loop(
        0, TILES, take, (jnp.full((1, LANES), TILES, jnp.int32), jnp.zeros((1, LANES), jnp.int32))
    )
    seats_in = pltpu.make_async_copy(tile_v, tile_s, local.at[L_SEAT(0)])
    seats_in.start()
    pl.semaphore_wait(barrier, len(neighbours))

    rounds = (y_sides, zh_sides, zh_sides, (to_core,), (to_z,))

    def tell(n):
        for device in rounds[n]:
            pl.semaphore_signal(told.at[n], inc=1, device_id=device, device_id_type=MESH)

    def heard(n):
        pl.semaphore_wait(told.at[n], len(rounds[n]))

    def send_near(k):
        start(pg.at[chunk(k), :, lanes(xp)], near.at[0, chunk(k)], NEAR(k, 0), to_xp)
        start(pg.at[chunk(k), :, lanes(4 + xm)], near.at[1, chunk(k)], NEAR(k, 1), to_xm)

    for k in range(CHUNKS):
        pg_in[k].wait()
        start(pg.at[chunk(k), :, lanes(x2)], far.at[0, chunk(k)], FAR(k, 0), to_xm)
        start(pg.at[chunk(k), :, lanes(4 + x2)], far.at[1, chunk(k)], FAR(k, 1), to_xp)
    send_near(0)
    tell(0)

    for s in range(SLOTS):
        r_in[s].wait()
        start(r_h.at[s, :, lanes(zo, HALF)], rf.at[s, own_rows, :], RZ(s), to_z)
    for s in range(2):
        start(l_h.at[s], lp.at[s, pair_rows, :], LZ(s), to_z)

    def per_tile(k, step):
        def one(t, carry):
            step(t)
            return carry

        lax.fori_loop(BOUNDS[k], BOUNDS[k + 1], one, 0, unroll=2)

    for k in range(CHUNKS):
        arrived(far.at[0, chunk(k)], FAR(k, 0))
        arrived(far.at[1, chunk(k)], FAR(k, 1))

        def add_chain(t):
            chs[0, t] = (
                far[0, t].astype(F32) + pg[t, :, lanes(xm)].astype(F32)
            ).astype(BF16)
            chs[1, t] = (
                far[1, t].astype(F32) + pg[t, :, lanes(4 + xp)].astype(F32)
            ).astype(BF16)

        per_tile(k, add_chain)
        if k + 1 < CHUNKS:
            send_near(k + 1)
        heard(k)
        tell(k + 1)
        start(chs.at[0, chunk(k)], ch.at[0, chunk(k)], CHAIN(k, 0), to_xm)
        start(chs.at[1, chunk(k)], ch.at[1, chunk(k)], CHAIN(k, 1), to_xp)

    def quad(chip, part, rows):
        return pl.ds(pl.multiple_of(chip * 256 + part, LANES), rows)

    for s in range(SLOTS):
        arrived(rf.at[s, own_rows, :], RZ(s))
        block = rf.at[s, quad(x, 0, 256), :]
        start(block, block, RN(s, 0), to_xp)
        start(block, block, RN(s, 1), to_xm)

    def total(half, t):
        return (
            pg[t, :, lanes(half * 4 + x)].astype(F32)
            + near[half, t].astype(F32)
            + ch[half, t].astype(F32)
        )

    for k in range(CHUNKS):
        for side in range(2):
            arrived(near.at[side, chunk(k)], NEAR(k, side))
            arrived(ch.at[side, chunk(k)], CHAIN(k, side))

        def other_half(t):
            hs[t] = total(zo, t).astype(BF16)

        per_tile(k, other_half)
        start(hs.at[chunk(k)], zrecv.at[chunk(k)], ZZ(k), to_z)

    my_block = zl * 4 + x
    other_block = zo * 4 + x
    row_of = lax.broadcasted_iota(jnp.int32, (PIECE, COLS), 0) + me * PIECE
    col_of = lax.broadcasted_iota(jnp.int32, (PIECE, COLS), 1) + my_block * COLS
    for k in range(CHUNKS):
        arrived(zrecv.at[chunk(k)], ZZ(k))

        def share(t):
            rows, cols = extent(t)
            value = total(zl, t) + zrecv[t].astype(F32)
            shares[t] = jnp.where((row_of < rows) & (col_of < cols), value, 0.0).astype(BF16)

        per_tile(k, share)
    shares[TILES] = jnp.zeros((PIECE, COLS), BF16)

    my_cols = lanes(my_block)
    my_piece = pl.ds(pl.multiple_of(me * PIECE, PIECE), PIECE)
    seats_in.wait()
    for s in range(SLOTS):

        def stage(o, carry):
            staged[s, o] = shares[tile_s[0, s * OWNERS + o]]
            return carry

        lax.fori_loop(0, OWNERS, stage, 0, unroll=4)

    def to_owners(s):
        def one(k, carry):
            o = (me + k) % OWNERS
            pltpu.make_async_remote_copy(
                src_ref=staged.at[s, o],
                dst_ref=gf.at[s, my_piece, my_cols],
                send_sem=send.at[A2A(s)],
                recv_sem=recv.at[A2A(s)],
                device_id=owner_device(o),
                device_id_type=MESH,
            ).start()
            return carry

        lax.fori_loop(1, OWNERS, one, 0)

    heard(4)
    to_owners(0)
    to_owners(1)
    for s in range(SLOTS):
        gf[s, my_piece, my_cols] = staged[s, me]

    halves = (pl.ds(0, 512), pl.ds(512, 512))

    def g_here(s):
        arrived(staged.at[s, pl.ds(0, OWNERS - 1)], A2A(s))
        block = gf.at[s, :, my_cols]
        start(block, block, GZ(s), to_z)

    def g_own(s):
        block = gf.at[s, :, my_cols]
        start(block, block, GN(s, 0), to_xp)
        start(block, block, GN(s, 1), to_xm)

    def g_pair(s):
        arrived(gf.at[s, :, lanes(other_block)], GZ(s))
        for turn in range(2):
            block = gf.at[s, halves[turn], lanes(other_block)]
            start(block, block, GP(s, 0, turn), to_xp)
            block = gf.at[s, halves[1 - turn], lanes(other_block)]
            start(block, block, GP(s, 1, turn), to_xm)

    def g_far(s):
        arrived(gf.at[s, :, lanes(zl * 4 + xm)], GN(s, 0))
        block = gf.at[s, halves[0], lanes(zl * 4 + xm)]
        start(block, block, GF(s, 0), to_xp)
        arrived(gf.at[s, :, lanes(zl * 4 + xp)], GN(s, 1))
        block = gf.at[s, halves[1], lanes(zl * 4 + xp)]
        start(block, block, GF(s, 1), to_xm)

    def g_far_pair(s):
        arrived(gf.at[s, halves[0], lanes(zo * 4 + xm)], GP(s, 0, 0))
        block = gf.at[s, halves[0], lanes(zo * 4 + xm)]
        start(block, block, GPF(s, 0), to_xp)
        arrived(gf.at[s, halves[1], lanes(zo * 4 + xp)], GP(s, 1, 0))
        block = gf.at[s, halves[1], lanes(zo * 4 + xp)]
        start(block, block, GPF(s, 1), to_xm)

    def g_far_here(s):
        arrived(gf.at[s, halves[0], lanes(zl * 4 + x2)], GF(s, 0))
        arrived(gf.at[s, halves[1], lanes(zl * 4 + x2)], GF(s, 1))

    def g_far_z(s):
        g_far_here(s)
        block = gf.at[s, :, lanes(zl * 4 + x2)]
        start(block, block, GZ_FAR(s), to_z)

    def g_done(s):
        if s < SLOTS - 1:
            arrived(gf.at[s, halves[0], lanes(zo * 4 + xm)], GP(s, 0, 0))
            arrived(gf.at[s, halves[1], lanes(zo * 4 + xp)], GP(s, 1, 0))
        arrived(gf.at[s, halves[1], lanes(zo * 4 + xm)], GP(s, 0, 1))
        arrived(gf.at[s, halves[0], lanes(zo * 4 + xp)], GP(s, 1, 1))
        if s < SLOTS - 1:
            arrived(gf.at[s, :, lanes(zo * 4 + x2)], GZ_FAR(s))
        else:
            arrived(gf.at[s, halves[0], lanes(zo * 4 + x2)], GPF(s, 0))
            arrived(gf.at[s, halves[1], lanes(zo * 4 + x2)], GPF(s, 1))

    def r_far(s):
        arrived(rf.at[s, quad(xm, 0, 256), :], RN(s, 0))
        block = rf.at[s, quad(xm, 0, LANES), :]
        start(block, block, RF(s, 0), to_xp)
        arrived(rf.at[s, quad(xp, 0, 256), :], RN(s, 1))
        block = rf.at[s, quad(xp, LANES, LANES), :]
        start(block, block, RF(s, 1), to_xm)

    def r_done(s):
        arrived(rf.at[s, quad(x2, 0, LANES), :], RF(s, 0))
        arrived(rf.at[s, quad(x2, LANES, LANES), :], RF(s, 1))
        arrived(lp.at[s, pair_rows, :], LZ(s))

    def grams(s):
        gt[...] = gf[s, :, lanes(d)].T
        grad_rows = gf[s, pl.ds(pl.multiple_of(d * LANES, LANES), LANES), :]

        def columns(n, carry):
            at = pl.ds(pl.multiple_of(n * 256, 256), 256)
            right = jnp.dot(gt[...], gf[s, :, at], preferred_element_type=F32)
            nr[s, :, at] = stat_decay * rs[s, :, at] + (1.0 - stat_decay) * right
            left = lax.dot_general(
                grad_rows, gf[s, at, :], (((1,), (1,)), ((), ())), preferred_element_type=F32
            )
            nl[s, :, at] = stat_decay * ls[s, :, at] + (1.0 - stat_decay) * left
            return carry

        lax.fori_loop(0, 4, columns, 0)

    out_cols = lanes(zl, HALF)

    def left_part(s, half):
        def columns(n, carry):
            at = pl.ds(pl.multiple_of(half * HALF + n * 256, 256), 256)
            part = jnp.dot(lp[s], gf[s, :, at], preferred_element_type=F32)
            tp[:, at] = part.astype(BF16)
            return carry

        lax.fori_loop(0, 2, columns, 0)

    def direction_rows(s):
        def columns(n, carry):
            at = pl.ds(pl.multiple_of(n * 256, 256), 256)
            obuf[:, at] = jnp.dot(tp[...], rf[s, :, at], preferred_element_type=F32)
            return carry

        lax.fori_loop(0, 2, columns, 0)

        def rows(i):
            value = obuf[pl.ds(pl.multiple_of(i * 8, 8), 8), :]
            ostage[s, 2 * i] = value[:4].astype(BF16)
            ostage[s, 2 * i + 1] = value[4:].astype(BF16)

        def give(i, core):
            pltpu.make_async_remote_copy(
                src_ref=ostage.at[s, 2 * i + core],
                dst_ref=ret.at[s * OWNERS + me, :, out_cols],
                send_sem=send.at[RET(s)],
                recv_sem=recv.at[RET(s)],
                device_id={
                    "dp_1": i // 16,
                    "owner_0": (i // 4) % 4,
                    "owner_1": i % 4,
                    "owner_2": core,
                },
                device_id_type=MESH,
            ).start()

        chip = here // 2
        rows((chip + 1) % 32)

        def one(k, carry):
            rows((chip + k + 1) % 32)
            give((chip + k) % 32, 0)
            give((chip + k) % 32, 1)
            return carry

        lax.fori_loop(1, 32, one, 0)
        ret[s * OWNERS + me, :, out_cols] = ostage[s, here]
        give(chip, 1 - co)

    g_here(0)
    g_own(0)
    to_owners(2)
    r_far(0)
    r_far(1)
    r_far(2)
    g_pair(0)
    g_far(0)
    g_here(1)
    g_own(1)
    g_pair(1)
    g_here(2)
    g_far_z(0)
    start(l_h.at[2], lp.at[2, pair_rows, :], LZ(2), to_z)
    g_far(1)
    g_own(2)
    g_pair(2)
    for s in range(SLOTS):
        l_in[s].wait()
    ls_in.wait()
    rs_in.wait()
    g_done(0)
    r_done(0)
    left_part(0, 0)
    left_part(0, 1)
    direction_rows(0)
    grams(0)
    g_far_z(1)
    g_far(2)
    g_far_pair(2)
    g_done(1)
    r_done(1)
    left_part(1, 0)
    left_part(1, 1)
    direction_rows(1)
    grams(1)
    r_done(2)
    g_far_here(2)
    left_part(2, zl)
    g_done(2)
    left_part(2, zo)
    direction_rows(2)
    grams(2)
    for s in range(SLOTS):
        arrived(ostage.at[s, pl.ds(0, 63)], RET(s))
    for copy in sent:
        copy.wait_send()
    for s in range(SLOTS):
        for src, sem in (
            (staged.at[s, pl.ds(0, OWNERS - 1)], A2A(s)),
            (ostage.at[s, pl.ds(0, 63)], RET(s)),
        ):
            pltpu.make_async_remote_copy(
                src_ref=src,
                dst_ref=src,
                send_sem=send.at[sem],
                recv_sem=recv.at[sem],
                device_id=to_xp,
                device_id_type=MESH,
            ).wait_send()


def write_out(owner_s, ret, nl, nr, dir_h, nl_h, nr_h, rows_v, count_s, sems):
    copies = [
        pltpu.make_async_copy(nl, nl_h, sems.at[0]),
        pltpu.make_async_copy(nr, nr_h, sems.at[1]),
    ]
    for copy in copies:
        copy.start()
    d = lax.axis_index(DP)
    me = lax.axis_index(OWNER)
    line = lax.broadcasted_iota(jnp.int32, (4, TILE), 0) + (d * LANES + me * 4)
    lane = lax.broadcasted_iota(jnp.int32, (4, TILE), 1)

    def clear(o, carry):
        count_s[o] = 0
        return carry

    lax.fori_loop(0, OWNERS, clear, 0, unroll=8)

    def write(t, carry):
        rows, cols = extent(t)
        owner = owner_s[t]
        taken = count_s[owner]
        count_s[owner] = taken + OWNERS
        value = ret[taken + owner].astype(F32)
        rows_v[t] = jnp.where((line < rows) & (lane < cols), value, 0.0).astype(BF16)
        return carry

    lax.fori_loop(0, TILES, write, 0, unroll=4)
    copies.append(pltpu.make_async_copy(rows_v, dir_h, sems.at[2]))
    copies[2].start()
    for copy in copies:
        copy.wait()


def body(partial_grads, owner_map, left_stats, right_stats, left_roots, right_roots):
    smem = pl.BlockSpec(memory_space=pltpu.SMEM)
    vmem = pl.BlockSpec(memory_space=pltpu.VMEM)
    hbm = pl.BlockSpec(memory_space=pltpu.HBM)
    returned, new_left, new_right = pl.pallas_call(
        kernel,
        out_shape=(
            pltpu.VMEM((SLOTS * OWNERS, 4, TILE), BF16),
            pltpu.VMEM((SLOTS, LANES, TILE), F32),
            pltpu.VMEM((SLOTS, LANES, TILE), F32),
        ),
        in_specs=[smem, hbm, hbm, hbm, hbm, hbm],
        out_specs=(vmem, vmem, vmem),
        scratch_shapes=[
            pltpu.VMEM((TILES, PIECE, TILE), BF16),
            pltpu.VMEM((2, TILES, PIECE, COLS), BF16),
            pltpu.VMEM((2, TILES, PIECE, COLS), BF16),
            pltpu.VMEM((2, TILES, PIECE, COLS), BF16),
            pltpu.VMEM((2, TILES, PIECE, COLS), BF16),
            pltpu.VMEM((TILES, PIECE, COLS), BF16),
            pltpu.VMEM((TILES, PIECE, COLS), BF16),
            pltpu.VMEM((TILES + 1, PIECE, COLS), BF16),
            pltpu.VMEM((SLOTS, OWNERS, PIECE, COLS), BF16),
            pltpu.VMEM((SLOTS, TILE, TILE), BF16),
            pltpu.VMEM((SLOTS, TILE, HALF), BF16),
            pltpu.VMEM((SLOTS, 256, TILE), BF16),
            pltpu.VMEM((SLOTS, LANES, TILE), F32),
            pltpu.VMEM((SLOTS, LANES, TILE), F32),
            pltpu.VMEM((LANES, TILE), BF16),
            pltpu.VMEM((256, TILE), BF16),
            pltpu.VMEM((256, HALF), F32),
            pltpu.VMEM((SLOTS, 64, 4, HALF), BF16),
            pltpu.VMEM((1, LANES), jnp.int32),
            pltpu.SMEM((1, LANES), jnp.int32),
            pltpu.SemaphoreType.DMA((N_SEMS,)),
            pltpu.SemaphoreType.DMA((N_SEMS,)),
            pltpu.SemaphoreType.DMA((N_LOC,)),
            pltpu.SemaphoreType.REGULAR((5,)),
        ],
        compiler_params=pltpu.CompilerParams(
            collective_id=0, has_side_effects=True, vmem_limit_bytes=60 * 1024 * 1024
        ),
    )(
        owner_map,
        partial_grads[0],
        left_roots[0],
        right_roots[0],
        left_stats[0],
        right_stats[0],
    )
    direction, new_left, new_right = pl.pallas_call(
        write_out,
        out_shape=(
            jax.ShapeDtypeStruct((TILES, 4, TILE), BF16),
            jax.ShapeDtypeStruct((SLOTS, LANES, TILE), F32),
            jax.ShapeDtypeStruct((SLOTS, LANES, TILE), F32),
        ),
        in_specs=[smem, vmem, vmem, vmem],
        out_specs=(hbm, hbm, hbm),
        scratch_shapes=[
            pltpu.VMEM((TILES, 4, TILE), BF16),
            pltpu.SMEM((OWNERS,), jnp.int32),
            pltpu.SemaphoreType.DMA((3,)),
        ],
        compiler_params=pltpu.CompilerParams(vmem_limit_bytes=4 * 1024 * 1024),
    )(
        owner_map,
        *(
            pltpu.with_memory_space_constraint(value, pltpu.VMEM)
            for value in (returned, new_left, new_right)
        ),
    )
    return direction, new_left[None], new_right[None]


def solution(mesh):
    torus = Mesh(
        mesh.devices.reshape(4, 2, 4, 4, 2), ("dp_0", "dp_1", "owner_0", "owner_1", "owner_2")
    )
    in_specs = (
        P(DP, None, OWNER, None),
        P(),
        P(OWNER, None, DP, None),
        P(OWNER, None, DP, None),
        P(OWNER, None, DP, None),
        P(OWNER, None, DP, None),
    )
    out_specs = (P(None, DP_OWNER, None), P(OWNER, None, DP, None), P(OWNER, None, DP, None))
    return jax.shard_map(body, mesh=torus, in_specs=in_specs, out_specs=out_specs, check_vma=False)
```

```python
import functools

import jax
import jax.numpy as jnp
from jax import lax
from jax.experimental import pallas as pl
from jax.experimental.pallas import tpu as pltpu
from jax.sharding import Mesh
from jax.sharding import PartitionSpec as P

D_MODEL = 2560
D_IN = 10576
D_INNER = 5120
TILE = 1024
TILES = 48
OWNERS = 32
SLOTS = 3
PIECE = 32
LANES = 128
COLS = 128
HALF = 512
BOUNDS = (0, 14, 28, 42, 48)
CHUNKS = len(BOUNDS) - 1
OWNER = ("owner_0", "owner_1", "owner_2")
DP = ("dp_0", "dp_1")
DP_OWNER = ("dp_0", "dp_1", "owner_0", "owner_1", "owner_2")
MESH = pl.DeviceIdType.MESH
F32 = jnp.float32
BF16 = jnp.bfloat16

stat_decay = 0.999


def extent(t):
    in_cols = -(-D_IN // TILE)
    out_cols = -(-D_MODEL // TILE)
    in_count = -(-D_MODEL // TILE) * in_cols
    other = jnp.maximum(t - in_count, 0)
    is_in = t < in_count
    rows = jnp.where(
        is_in,
        jnp.minimum(TILE, D_MODEL - t // in_cols * TILE),
        jnp.minimum(TILE, D_INNER - other // out_cols * TILE),
    )
    cols = jnp.where(
        is_in,
        jnp.minimum(TILE, D_IN - t % in_cols * TILE),
        jnp.minimum(TILE, D_MODEL - other % out_cols * TILE),
    )
    return rows, cols


class Ids:
    def __init__(self):
        self.n = 0

    def __call__(self, *shape):
        size = 1
        for s in shape:
            size *= s
        base = self.n
        self.n += size

        def at(*index):
            flat = 0
            for i, s in zip(index, shape):
                flat = flat * s + i
            return base + flat

        return at


IDS = Ids()
FAR = IDS(CHUNKS, 2)
NEAR = IDS(CHUNKS, 2)
CHAIN = IDS(CHUNKS, 2)
ZZ = IDS(CHUNKS)
RZ = IDS(SLOTS)
RN = IDS(SLOTS, 2)
RF = IDS(SLOTS, 2)
LZ = IDS(SLOTS)
A2A = IDS(SLOTS)
GZ = IDS(SLOTS)
GZ_FAR = IDS(SLOTS)
GN = IDS(SLOTS, 2)
GP = IDS(SLOTS, 2, 2)
GF = IDS(SLOTS, 2)
GPF = IDS(SLOTS, 2)
RET = IDS(SLOTS)
LC = IDS(1)
RC = IDS(1)
RX = IDS(1)
CC = IDS(2)
N_SEMS = IDS.n
LOC = Ids()
L_PG = LOC(CHUNKS)
L_R = LOC(SLOTS)
L_L = LOC(SLOTS)
L_LS = LOC(1)
L_RS = LOC(1)
L_SEAT = LOC(1)
N_LOC = LOC.n


def kernel(
    shared,
    owner_s,
    pg_h,
    l_h,
    r_h,
    ls_h,
    rs_h,
    ret,
    nl,
    nr,
    pg,
    far,
    chs,
    near,
    ch,
    hs,
    zrecv,
    shares,
    staged,
    gf,
    rf,
    lp,
    ls,
    rs,
    gt,
    tp,
    obuf,
    ostage,
    lx,
    rx,
    r2,
    rf2,
    tile_v,
    tile_s,
    send,
    recv,
    local,
    told,
):
    x = lax.axis_index("dp_0")
    zl = lax.axis_index("dp_1")
    y = lax.axis_index("owner_0")
    zh = lax.axis_index("owner_1")
    co = lax.axis_index("owner_2")
    me = (y * 4 + zh) * 2 + co
    d = x * 2 + zl
    xp = (x + 1) % 4
    xm = (x + 3) % 4
    x2 = (x + 2) % 4
    zo = 1 - zl
    here = zl * 32 + me
    to_xp = {"dp_0": xp}
    to_xm = {"dp_0": xm}
    to_z = {"dp_1": zo}
    to_core = {"owner_2": 1 - co}
    my_chip = me // 2
    own = SLOTS - 1 if shared else SLOTS
    last = SLOTS - 1
    far_by_x = (2,)

    def owner_device(i):
        return {"owner_0": i // 8, "owner_1": (i // 2) % 4, "owner_2": i % 2}

    def any_device(i):
        return {
            "dp_1": i // 32,
            "owner_0": (i // 8) % 4,
            "owner_1": (i // 2) % 4,
            "owner_2": i % 2,
        }

    sent = []

    def start(src, dst, sem, device):
        copy = pltpu.make_async_remote_copy(
            src_ref=src,
            dst_ref=dst,
            send_sem=send.at[sem],
            recv_sem=recv.at[sem],
            device_id=device,
            device_id_type=MESH,
        )
        copy.start()
        sent.append(copy)

    def arrived(dst, sem):
        pltpu.make_async_remote_copy(
            src_ref=dst,
            dst_ref=dst,
            send_sem=send.at[sem],
            recv_sem=recv.at[sem],
            device_id=to_xp,
            device_id_type=MESH,
        ).wait_recv()

    def lanes(block, width=COLS):
        return pl.ds(pl.multiple_of(block * width, width), width)

    def chunk(k):
        return pl.ds(BOUNDS[k], BOUNDS[k + 1] - BOUNDS[k])

    pg_in = [
        pltpu.make_async_copy(pg_h.at[chunk(k)], pg.at[chunk(k)], local.at[L_PG(k)])
        for k in range(CHUNKS)
    ]
    for copy in pg_in:
        copy.start()
    own_rows = pl.ds(pl.multiple_of(d * LANES, LANES), LANES)
    pair_rows = pl.ds(pl.multiple_of(zl * LANES, LANES), LANES)
    r_in = [
        pltpu.make_async_copy(
            r_h.at[s, :, lanes(zl, HALF)], rf.at[s, own_rows, :], local.at[L_R(s)]
        )
        for s in range(own)
    ]
    l_in = [
        pltpu.make_async_copy(l_h.at[s], lp.at[s, pair_rows, :], local.at[L_L(s)])
        for s in range(own)
    ]
    core_rows = pl.ds(pl.multiple_of(co * 64, 64), 64)
    if shared:
        r_in.append(
            pltpu.make_async_copy(r_h.at[last, core_rows, :], rx.at[0], local.at[L_R(last)])
        )
        l_in.append(pltpu.make_async_copy(l_h.at[last], lx.at[0], local.at[L_L(last)]))
    ls_in = pltpu.make_async_copy(ls_h, ls, local.at[L_LS(0)])
    rs_in = pltpu.make_async_copy(rs_h, rs, local.at[L_RS(0)])
    for copy in (*r_in, *l_in, ls_in, rs_in):
        copy.start()

    barrier = pltpu.get_barrier_semaphore()
    y_sides = ({"owner_0": (y + 1) % 4}, {"owner_0": (y + 3) % 4})
    zh_sides = ({"owner_1": (zh + 1) % 4}, {"owner_1": (zh + 3) % 4})
    neighbours = (to_xp, to_xm, to_z, to_core, *y_sides, *zh_sides)
    for device in neighbours:
        pl.semaphore_signal(barrier, inc=1, device_id=device, device_id_type=MESH)

    seat = lax.broadcasted_iota(jnp.int32, (1, LANES), 1)

    def take(t, carry):
        tile, count = carry
        mine = seat % OWNERS == owner_s[t]
        tile = jnp.where(mine & (count == seat // OWNERS), t, tile)
        return tile, count + mine.astype(jnp.int32)

    tile_v[...], _ = lax.fori_loop(
        0, TILES, take, (jnp.full((1, LANES), TILES, jnp.int32), jnp.zeros((1, LANES), jnp.int32))
    )
    seats_in = pltpu.make_async_copy(tile_v, tile_s, local.at[L_SEAT(0)])
    seats_in.start()
    pl.semaphore_wait(barrier, len(neighbours))

    rounds = (y_sides, zh_sides, zh_sides, (to_core,), (to_z,))

    def tell(n):
        for device in rounds[n]:
            pl.semaphore_signal(told.at[n], inc=1, device_id=device, device_id_type=MESH)

    def heard(n):
        pl.semaphore_wait(told.at[n], len(rounds[n]))

    def send_near(k):
        start(pg.at[chunk(k), :, lanes(xp)], near.at[0, chunk(k)], NEAR(k, 0), to_xp)
        start(pg.at[chunk(k), :, lanes(4 + xm)], near.at[1, chunk(k)], NEAR(k, 1), to_xm)

    for k in range(CHUNKS):
        pg_in[k].wait()
        start(pg.at[chunk(k), :, lanes(x2)], far.at[0, chunk(k)], FAR(k, 0), to_xm)
        start(pg.at[chunk(k), :, lanes(4 + x2)], far.at[1, chunk(k)], FAR(k, 1), to_xp)
    send_near(0)
    tell(0)

    if shared:
        start(l_h.at[last], lx.at[1], LC(0), to_core)
        other_core_rows = pl.ds(pl.multiple_of(64 - co * 64, 64), 64)
        start(r_h.at[last, other_core_rows, :], rx.at[1], RC(0), to_core)
    for s in range(own):
        r_in[s].wait()
        start(r_h.at[s, :, lanes(zo, HALF)], rf.at[s, own_rows, :], RZ(s), to_z)
    if shared:
        seats_in.wait()
        r_in[last].wait()
        l_in[last].wait()
        arrived(lx.at[1], LC(0))
        arrived(rx.at[1], RC(0))
        second = (tile_s[0, 2 * OWNERS + 2 * my_chip + 1] < TILES).astype(jnp.int32)
        source = (second + co) % 2
        r2[...] = rx[source]

        @pl.when(zl == co)
        def _():
            lp[last, :LANES] = lx[source]

        rf2[d, co] = r2[:, lanes(zl, HALF)]
        start(r2.at[:, lanes(zo, HALF)], rf2.at[d, co], RZ(last), to_z)
    for s in range(2):
        start(l_h.at[s], lp.at[s, pair_rows, :], LZ(s), to_z)

    def per_tile(k, step):
        def one(t, carry):
            step(t)
            return carry

        lax.fori_loop(BOUNDS[k], BOUNDS[k + 1], one, 0, unroll=2)

    for k in range(CHUNKS):
        arrived(far.at[0, chunk(k)], FAR(k, 0))
        arrived(far.at[1, chunk(k)], FAR(k, 1))

        def add_chain(t):
            chs[0, t] = (
                far[0, t].astype(F32) + pg[t, :, lanes(xm)].astype(F32)
            ).astype(BF16)
            chs[1, t] = (
                far[1, t].astype(F32) + pg[t, :, lanes(4 + xp)].astype(F32)
            ).astype(BF16)

        per_tile(k, add_chain)
        if k + 1 < CHUNKS:
            send_near(k + 1)
        heard(k)
        tell(k + 1)
        start(chs.at[0, chunk(k)], ch.at[0, chunk(k)], CHAIN(k, 0), to_xm)
        start(chs.at[1, chunk(k)], ch.at[1, chunk(k)], CHAIN(k, 1), to_xp)

    def quad(chip, part, rows):
        return pl.ds(pl.multiple_of(chip * 256 + part, LANES), rows)

    def r_block(s, chip):
        if shared and s == last:
            return rf2.at[pl.ds(chip * 2, 2), co]
        return rf.at[s, quad(chip, 0, 256), :]

    def r_rows(s, chip, plane):
        if shared and s == last:
            return rf2.at[chip * 2 + plane, co]
        return rf.at[s, quad(chip, plane * LANES, LANES), :]

    for s in range(SLOTS):
        arrived(r_rows(s, x, zo), RZ(s))
        block = r_block(s, x)
        start(block, block, RN(s, 0), to_xp)
        start(block, block, RN(s, 1), to_xm)

    def total(half, t):
        return (
            pg[t, :, lanes(half * 4 + x)].astype(F32)
            + near[half, t].astype(F32)
            + ch[half, t].astype(F32)
        )

    for k in range(CHUNKS):
        for side in range(2):
            arrived(near.at[side, chunk(k)], NEAR(k, side))
            arrived(ch.at[side, chunk(k)], CHAIN(k, side))

        def other_half(t):
            hs[t] = total(zo, t).astype(BF16)

        per_tile(k, other_half)
        start(hs.at[chunk(k)], zrecv.at[chunk(k)], ZZ(k), to_z)

    my_block = zl * 4 + x
    other_block = zo * 4 + x
    row_of = lax.broadcasted_iota(jnp.int32, (PIECE, COLS), 0) + me * PIECE
    col_of = lax.broadcasted_iota(jnp.int32, (PIECE, COLS), 1) + my_block * COLS
    for k in range(CHUNKS):
        arrived(zrecv.at[chunk(k)], ZZ(k))

        def share(t):
            rows, cols = extent(t)
            value = total(zl, t) + zrecv[t].astype(F32)
            shares[t] = jnp.where((row_of < rows) & (col_of < cols), value, 0.0).astype(BF16)

        per_tile(k, share)
    shares[TILES] = jnp.zeros((PIECE, COLS), BF16)

    my_cols = lanes(my_block)
    my_piece = pl.ds(pl.multiple_of(me * PIECE, PIECE), PIECE)
    if not shared:
        seats_in.wait()
    for s in range(own):

        def stage(o, carry):
            staged[s, o] = shares[tile_s[0, s * OWNERS + o]]
            return carry

        lax.fori_loop(0, OWNERS, stage, 0, unroll=4)

    if shared:

        def stage_last(k, carry):
            at = 2 * OWNERS + 2 * k
            staged[last, k] = shares[jnp.minimum(tile_s[0, at], tile_s[0, at + 1])]
            return carry

        lax.fori_loop(0, 16, stage_last, 0, unroll=4)

    side = y // 2

    def to_chip(k):
        pltpu.make_async_remote_copy(
            src_ref=staged.at[last, k],
            dst_ref=gf.at[last, my_piece, my_cols],
            send_sem=send.at[A2A(last)],
            recv_sem=recv.at[A2A(last)],
            device_id={"owner_0": k // 4, "owner_1": k % 4, "owner_2": side},
            device_id_type=MESH,
        ).start()

    def to_chips():
        def one(k, carry):
            to_chip((my_chip + k) % 16)
            return carry

        lax.fori_loop(1, 16, one, 0)

        @pl.when(side == co)
        def _():
            gf[last, my_piece, my_cols] = staged[last, my_chip]

        @pl.when(side != co)
        def _():
            to_chip(my_chip)

    def to_owners(s):
        def one(k, carry):
            o = (me + k) % OWNERS
            pltpu.make_async_remote_copy(
                src_ref=staged.at[s, o],
                dst_ref=gf.at[s, my_piece, my_cols],
                send_sem=send.at[A2A(s)],
                recv_sem=recv.at[A2A(s)],
                device_id=owner_device(o),
                device_id_type=MESH,
            ).start()
            return carry

        lax.fori_loop(1, OWNERS, one, 0)

    heard(4)
    to_owners(0)
    to_owners(1)
    for s in range(own):
        gf[s, my_piece, my_cols] = staged[s, me]

    def span(s, part=0, parts=1):
        first, rows = (co * 512, 512 // parts) if shared and s == last else (0, 1024 // parts)
        return pl.ds(pl.multiple_of(first + part * rows, 256), rows)

    def halves(s, part):
        return span(s, part, 2)

    def g_here(s):
        if shared and s == last:

            @pl.when(side == co)
            def _():
                arrived(staged.at[s, pl.ds(0, 15)], A2A(s))

            @pl.when(side != co)
            def _():
                arrived(staged.at[s, pl.ds(0, 16)], A2A(s))

        else:
            arrived(staged.at[s, pl.ds(0, OWNERS - 1)], A2A(s))
        block = gf.at[s, span(s), my_cols]
        start(block, block, GZ(s), to_z)

    def g_own(s):
        block = gf.at[s, span(s), my_cols]
        start(block, block, GN(s, 0), to_xp)
        start(block, block, GN(s, 1), to_xm)

    def g_pair(s):
        arrived(gf.at[s, span(s), lanes(other_block)], GZ(s))
        for turn in range(2):
            block = gf.at[s, halves(s, turn), lanes(other_block)]
            start(block, block, GP(s, 0, turn), to_xp)
            block = gf.at[s, halves(s, 1 - turn), lanes(other_block)]
            start(block, block, GP(s, 1, turn), to_xm)

    def g_far(s):
        arrived(gf.at[s, span(s), lanes(zl * 4 + xm)], GN(s, 0))
        block = gf.at[s, halves(s, 0), lanes(zl * 4 + xm)]
        start(block, block, GF(s, 0), to_xp)
        arrived(gf.at[s, span(s), lanes(zl * 4 + xp)], GN(s, 1))
        block = gf.at[s, halves(s, 1), lanes(zl * 4 + xp)]
        start(block, block, GF(s, 1), to_xm)

    def g_far_pair(s):
        arrived(gf.at[s, halves(s, 0), lanes(zo * 4 + xm)], GP(s, 0, 0))
        block = gf.at[s, halves(s, 0), lanes(zo * 4 + xm)]
        start(block, block, GPF(s, 0), to_xp)
        arrived(gf.at[s, halves(s, 1), lanes(zo * 4 + xp)], GP(s, 1, 0))
        block = gf.at[s, halves(s, 1), lanes(zo * 4 + xp)]
        start(block, block, GPF(s, 1), to_xm)

    def g_far_here(s):
        arrived(gf.at[s, halves(s, 0), lanes(zl * 4 + x2)], GF(s, 0))
        arrived(gf.at[s, halves(s, 1), lanes(zl * 4 + x2)], GF(s, 1))

    def g_far_z(s):
        g_far_here(s)
        block = gf.at[s, span(s), lanes(zl * 4 + x2)]
        start(block, block, GZ_FAR(s), to_z)

    def g_done(s):
        if s not in far_by_x:
            arrived(gf.at[s, halves(s, 0), lanes(zo * 4 + xm)], GP(s, 0, 0))
            arrived(gf.at[s, halves(s, 1), lanes(zo * 4 + xp)], GP(s, 1, 0))
        arrived(gf.at[s, halves(s, 1), lanes(zo * 4 + xm)], GP(s, 0, 1))
        arrived(gf.at[s, halves(s, 0), lanes(zo * 4 + xp)], GP(s, 1, 1))
        if s not in far_by_x:
            arrived(gf.at[s, span(s), lanes(zo * 4 + x2)], GZ_FAR(s))
        else:
            arrived(gf.at[s, halves(s, 0), lanes(zo * 4 + x2)], GPF(s, 0))
            arrived(gf.at[s, halves(s, 1), lanes(zo * 4 + x2)], GPF(s, 1))

    def cross(plane, part):
        block = gf.at[last, span(last), lanes(plane, HALF)]
        start(block, block, CC(part), to_core)

    def crossed(plane, part):
        rows = pl.ds(pl.multiple_of(512 - co * 512, 512), 512)
        arrived(gf.at[last, rows, lanes(plane, HALF)], CC(part))

    def r_far(s):
        arrived(r_block(s, xm), RN(s, 0))
        block = r_rows(s, xm, 0)
        start(block, block, RF(s, 0), to_xp)
        arrived(r_block(s, xp), RN(s, 1))
        block = r_rows(s, xp, 1)
        start(block, block, RF(s, 1), to_xm)

    def r_done(s):
        arrived(r_rows(s, x2, 0), RF(s, 0))
        arrived(r_rows(s, x2, 1), RF(s, 1))

    def l_done(s):
        if shared and s == last:

            @pl.when(zl != co)
            def _():
                arrived(lp.at[last, pl.ds(0, LANES), :], LZ(last))

        else:
            arrived(lp.at[s, pair_rows, :], LZ(s))

    def l_last():
        if shared:

            @pl.when(zl == co)
            def _():
                block = lp.at[last, pl.ds(0, LANES), :]
                start(block, block, LZ(last), to_z)
                sent.pop()

        else:
            start(l_h.at[last], lp.at[last, pair_rows, :], LZ(last), to_z)

    def r_cross():
        start(rf2.at[:, co], rf2.at[:, co], RX(0), to_core)

    def grams(s):
        gt[...] = gf[s, :, lanes(d)].T
        grad_rows = gf[s, pl.ds(pl.multiple_of(d * LANES, LANES), LANES), :]

        weight = 1.0 - stat_decay
        if shared and s == last:
            weight = jnp.where(tile_s[0, 2 * OWNERS + me] < TILES, F32(weight), F32(0.0))

        def columns(n, carry):
            at = pl.ds(pl.multiple_of(n * 256, 256), 256)
            right = jnp.dot(gt[...], gf[s, :, at], preferred_element_type=F32)
            nr[s, :, at] = stat_decay * rs[s, :, at] + weight * right
            left = lax.dot_general(
                grad_rows, gf[s, at, :], (((1,), (1,)), ((), ())), preferred_element_type=F32
            )
            nl[s, :, at] = stat_decay * ls[s, :, at] + weight * left
            return carry

        lax.fori_loop(0, 4, columns, 0)

    out_cols = lanes(zl, HALF)

    def left_part(s, half):
        def columns(n, carry):
            at = pl.ds(pl.multiple_of(half * HALF + n * 256, 256), 256)
            if shared and s == last:
                part = jnp.dot(lp[s, :LANES], gf[s, :, at], preferred_element_type=F32)
                tp[:LANES, at] = part.astype(BF16)
            else:
                part = jnp.dot(lp[s], gf[s, :, at], preferred_element_type=F32)
                tp[:, at] = part.astype(BF16)
            return carry

        lax.fori_loop(0, 2, columns, 0)

    def direction_rows(s):
        half = shared and s == last
        chips = 16 if half else 32
        chip = my_chip if half else here // 2
        at_owner = 2 * OWNERS + my_chip if half else s * OWNERS + me

        def columns(n, carry):
            at = pl.ds(pl.multiple_of(n * 256, 256), 256)
            if half:
                right = rf2[:, :, :, at].reshape(TILE, 256)
                obuf[:LANES, at] = jnp.dot(tp[:LANES], right, preferred_element_type=F32)
            else:
                obuf[:, at] = jnp.dot(tp[...], rf[s, :, at], preferred_element_type=F32)
            return carry

        lax.fori_loop(0, 2, columns, 0)

        def rows(i):
            value = obuf[pl.ds(pl.multiple_of(i * 8, 8), 8), :]
            ostage[s, 2 * i] = value[:4].astype(BF16)
            ostage[s, 2 * i + 1] = value[4:].astype(BF16)

        def give(i, core):
            pltpu.make_async_remote_copy(
                src_ref=ostage.at[s, 2 * i + core],
                dst_ref=ret.at[at_owner, :, out_cols],
                send_sem=send.at[RET(s)],
                recv_sem=recv.at[RET(s)],
                device_id={
                    "dp_1": co if half else i // 16,
                    "owner_0": (i // 4) % 4,
                    "owner_1": i % 4,
                    "owner_2": core,
                },
                device_id_type=MESH,
            ).start()

        rows((chip + 1) % chips)

        def one(k, carry):
            rows((chip + k + 1) % chips)
            give((chip + k) % chips, 0)
            give((chip + k) % chips, 1)
            return carry

        lax.fori_loop(1, chips, one, 0)
        if half:

            @pl.when(zl == co)
            def _():
                ret[at_owner, :, out_cols] = ostage[s, me]
                give(chip, 1 - co)

            @pl.when(zl != co)
            def _():
                give(chip, 0)
                give(chip, 1)

        else:
            ret[at_owner, :, out_cols] = ostage[s, here]
            give(chip, 1 - co)

    g_here(0)
    g_own(0)
    if shared:
        to_chips()
    else:
        to_owners(2)
    r_far(0)
    r_far(1)
    r_far(2)
    g_pair(0)
    g_far(0)
    g_here(1)
    g_own(1)
    g_pair(1)
    g_here(2)
    g_far_z(0)
    l_last()
    g_far(1)
    if 1 in far_by_x:
        g_far_pair(1)
    g_own(2)
    g_pair(2)
    r_done(2)
    if shared:
        r_cross()
    for s in range(own):
        l_in[s].wait()
    ls_in.wait()
    rs_in.wait()
    g_done(0)
    r_done(0)
    l_done(0)
    left_part(0, 0)
    left_part(0, 1)
    direction_rows(0)
    grams(0)
    if 1 in far_by_x:
        g_far_here(1)
    else:
        g_far_z(1)
    g_far(2)
    g_far_pair(2)
    g_done(1)
    r_done(1)
    l_done(1)
    if shared:
        g_far_here(2)
        cross(zl, 0)
    left_part(1, 0)
    left_part(1, 1)
    direction_rows(1)
    l_done(2)
    if shared:
        g_done(2)
        cross(zo, 1)
        crossed(zl, 0)
        left_part(2, zl)
        crossed(zo, 1)
        arrived(rf2.at[:, 1 - co], RX(0))
    else:
        g_far_here(2)
        left_part(2, zl)
        g_done(2)
    left_part(2, zo)
    direction_rows(2)
    grams(1)
    grams(2)
    def ends(sem, few, many, first, wait):
        @pl.when(first)
        def _():
            wait(few, sem)

        @pl.when(jnp.logical_not(first))
        def _():
            wait(many, sem)

    for s in range(own):
        arrived(ostage.at[s, pl.ds(0, 63)], RET(s))
    few, many = ostage.at[last, pl.ds(0, 31)], ostage.at[last, pl.ds(0, 32)]
    if shared:
        ends(RET(last), few, many, zl == co, arrived)
    for copy in sent:
        copy.wait_send()

    def left(src, sem):
        pltpu.make_async_remote_copy(
            src_ref=src,
            dst_ref=src,
            send_sem=send.at[sem],
            recv_sem=recv.at[sem],
            device_id=to_xp,
            device_id_type=MESH,
        ).wait_send()

    for s in range(own):
        left(staged.at[s, pl.ds(0, OWNERS - 1)], A2A(s))
        left(ostage.at[s, pl.ds(0, 63)], RET(s))
    if shared:
        ends(RET(last), few, many, zl == co, left)
        few, many = staged.at[last, pl.ds(0, 15)], staged.at[last, pl.ds(0, 16)]
        ends(A2A(last), few, many, side == co, left)

        @pl.when(zl == co)
        def _():
            left(lp.at[last, pl.ds(0, LANES), :], LZ(last))


def write_out(shared, owner_s, ret, nl, nr, dir_h, nl_h, nr_h, rows_v, count_s, sems):
    copies = [
        pltpu.make_async_copy(nl, nl_h, sems.at[0]),
        pltpu.make_async_copy(nr, nr_h, sems.at[1]),
    ]
    for copy in copies:
        copy.start()
    d = lax.axis_index(DP)
    me = lax.axis_index(OWNER)
    line = lax.broadcasted_iota(jnp.int32, (4, TILE), 0) + (d * LANES + me * 4)
    lane = lax.broadcasted_iota(jnp.int32, (4, TILE), 1)

    def clear(o, carry):
        count_s[o] = 0
        return carry

    lax.fori_loop(0, OWNERS, clear, 0, unroll=8)

    def write(t, carry):
        rows, cols = extent(t)
        owner = owner_s[t]
        taken = count_s[owner]
        count_s[owner] = taken + OWNERS
        place = taken + owner
        if shared:
            place = jnp.where(taken < 2 * OWNERS, place, 2 * OWNERS + owner // 2)
        value = ret[place].astype(F32)
        rows_v[t] = jnp.where((line < rows) & (lane < cols), value, 0.0).astype(BF16)
        return carry

    lax.fori_loop(0, TILES, write, 0, unroll=4)
    copies.append(pltpu.make_async_copy(rows_v, dir_h, sems.at[2]))
    copies[2].start()
    for copy in copies:
        copy.wait()


def step(shared, owner_map, *arrays):
    smem = pl.BlockSpec(memory_space=pltpu.SMEM)
    vmem = pl.BlockSpec(memory_space=pltpu.VMEM)
    hbm = pl.BlockSpec(memory_space=pltpu.HBM)
    returned, new_left, new_right = pl.pallas_call(
        functools.partial(kernel, shared),
        out_shape=(
            pltpu.VMEM((SLOTS * OWNERS, 4, TILE), BF16),
            pltpu.VMEM((SLOTS, LANES, TILE), F32),
            pltpu.VMEM((SLOTS, LANES, TILE), F32),
        ),
        in_specs=[smem, hbm, hbm, hbm, hbm, hbm],
        out_specs=(vmem, vmem, vmem),
        scratch_shapes=[
            pltpu.VMEM((TILES, PIECE, TILE), BF16),
            pltpu.VMEM((2, TILES, PIECE, COLS), BF16),
            pltpu.VMEM((2, TILES, PIECE, COLS), BF16),
            pltpu.VMEM((2, TILES, PIECE, COLS), BF16),
            pltpu.VMEM((2, TILES, PIECE, COLS), BF16),
            pltpu.VMEM((TILES, PIECE, COLS), BF16),
            pltpu.VMEM((TILES, PIECE, COLS), BF16),
            pltpu.VMEM((TILES + 1, PIECE, COLS), BF16),
            pltpu.VMEM((SLOTS, OWNERS, PIECE, COLS), BF16),
            pltpu.VMEM((SLOTS, TILE, TILE), BF16),
            pltpu.VMEM((SLOTS, TILE, HALF), BF16),
            pltpu.VMEM((SLOTS, 256, TILE), BF16),
            pltpu.VMEM((SLOTS, LANES, TILE), F32),
            pltpu.VMEM((SLOTS, LANES, TILE), F32),
            pltpu.VMEM((LANES, TILE), BF16),
            pltpu.VMEM((256, TILE), BF16),
            pltpu.VMEM((256, HALF), F32),
            pltpu.VMEM((SLOTS, 64, 4, HALF), BF16),
            pltpu.VMEM((2, LANES, TILE), BF16),
            pltpu.VMEM((2, 64, TILE), BF16),
            pltpu.VMEM((64, TILE), BF16),
            pltpu.VMEM((8, 2, 64, HALF), BF16),
            pltpu.VMEM((1, LANES), jnp.int32),
            pltpu.SMEM((1, LANES), jnp.int32),
            pltpu.SemaphoreType.DMA((N_SEMS,)),
            pltpu.SemaphoreType.DMA((N_SEMS,)),
            pltpu.SemaphoreType.DMA((N_LOC,)),
            pltpu.SemaphoreType.REGULAR((5,)),
        ],
        compiler_params=pltpu.CompilerParams(
            collective_id=int(shared), has_side_effects=True, vmem_limit_bytes=60 * 1024 * 1024
        ),
    )(owner_map, *arrays)
    return pl.pallas_call(
        functools.partial(write_out, shared),
        out_shape=(
            jax.ShapeDtypeStruct((TILES, 4, TILE), BF16),
            jax.ShapeDtypeStruct((SLOTS, LANES, TILE), F32),
            jax.ShapeDtypeStruct((SLOTS, LANES, TILE), F32),
        ),
        in_specs=[smem, vmem, vmem, vmem],
        out_specs=(hbm, hbm, hbm),
        scratch_shapes=[
            pltpu.VMEM((TILES, 4, TILE), BF16),
            pltpu.SMEM((OWNERS,), jnp.int32),
            pltpu.SemaphoreType.DMA((3,)),
        ],
        compiler_params=pltpu.CompilerParams(vmem_limit_bytes=4 * 1024 * 1024),
    )(
        owner_map,
        *(
            pltpu.with_memory_space_constraint(value, pltpu.VMEM)
            for value in (returned, new_left, new_right)
        ),
    )


def body(partial_grads, owner_map, left_stats, right_stats, left_roots, right_roots):
    chips = jnp.arange(OWNERS // 2, dtype=jnp.int32)
    first = 2 * chips[:, None]
    on_chip = (owner_map[None, :] >= first) & (owner_map[None, :] < first + 2)
    held = jnp.sum(on_chip.astype(jnp.int32), axis=1)
    direction, new_left, new_right = lax.cond(
        jnp.max(held) < 2 * SLOTS,
        functools.partial(step, True),
        functools.partial(step, False),
        owner_map,
        partial_grads[0],
        left_roots[0],
        right_roots[0],
        left_stats[0],
        right_stats[0],
    )
    return direction, new_left[None], new_right[None]


def solution(mesh):
    torus = Mesh(
        mesh.devices.reshape(4, 2, 4, 4, 2), ("dp_0", "dp_1", "owner_0", "owner_1", "owner_2")
    )
    in_specs = (
        P(DP, None, OWNER, None),
        P(),
        P(OWNER, None, DP, None),
        P(OWNER, None, DP, None),
        P(OWNER, None, DP, None),
        P(OWNER, None, DP, None),
    )
    out_specs = (P(None, DP_OWNER, None), P(OWNER, None, DP, None), P(OWNER, None, DP, None))
    return jax.shard_map(body, mesh=torus, in_specs=in_specs, out_specs=out_specs, check_vma=False)
```

```python
import functools

import jax
import jax.numpy as jnp
from jax import lax
from jax.experimental import pallas as pl
from jax.experimental.pallas import tpu as pltpu
from jax.sharding import Mesh
from jax.sharding import PartitionSpec as P

D_MODEL = 2560
D_IN = 10576
D_INNER = 5120
TILE = 1024
TILES = 48
OWNERS = 32
SLOTS = 3
PIECE = 32
LANES = 128
COLS = 128
HALF = 512
RUNS = (
    (33, 48, ((33, 2), (36, 2), (39, 2), (42, 2), (45, 2))),
    (0, 11, ((0, 10),)),
    (11, 22, ((11, 10),)),
    (22, 28, ((22, 6),)),
    (28, 33, ((28, 4),)),
)
CHUNKS = len(RUNS)
OWNER = ("owner_0", "owner_1", "owner_2")
DP = ("dp_0", "dp_1")
DP_OWNER = ("dp_0", "dp_1", "owner_0", "owner_1", "owner_2")
MESH = pl.DeviceIdType.MESH
F32 = jnp.float32
BF16 = jnp.bfloat16

stat_decay = 0.999


def extent(t):
    in_cols = -(-D_IN // TILE)
    out_cols = -(-D_MODEL // TILE)
    in_count = -(-D_MODEL // TILE) * in_cols
    other = jnp.maximum(t - in_count, 0)
    is_in = t < in_count
    rows = jnp.where(
        is_in,
        jnp.minimum(TILE, D_MODEL - t // in_cols * TILE),
        jnp.minimum(TILE, D_INNER - other // out_cols * TILE),
    )
    cols = jnp.where(
        is_in,
        jnp.minimum(TILE, D_IN - t % in_cols * TILE),
        jnp.minimum(TILE, D_MODEL - other % out_cols * TILE),
    )
    return rows, cols


class Ids:
    def __init__(self):
        self.n = 0

    def __call__(self, *shape):
        size = 1
        for s in shape:
            size *= s
        base = self.n
        self.n += size

        def at(*index):
            flat = 0
            for i, s in zip(index, shape):
                flat = flat * s + i
            return base + flat

        return at


IDS = Ids()
FAR = IDS(CHUNKS, 2)
NEAR = IDS(CHUNKS, 2)
CHAIN = IDS(CHUNKS, 2)
ZZ = IDS(CHUNKS)
RZ = IDS(SLOTS)
RN = IDS(SLOTS, 2)
RF = IDS(SLOTS, 2)
LZ = IDS(SLOTS)
A2A = IDS(SLOTS)
GZ = IDS(SLOTS)
GZ_FAR = IDS(SLOTS)
GN = IDS(SLOTS, 2)
GP = IDS(SLOTS, 2, 2)
GF = IDS(SLOTS, 2)
GPF = IDS(SLOTS, 2)
RET = IDS(SLOTS)
LC = IDS(1)
RC = IDS(1)
RX = IDS(1)
CC = IDS(2)
N_SEMS = IDS.n
LOC = Ids()
L_PG = LOC(CHUNKS)
L_R = LOC(SLOTS)
L_L = LOC(SLOTS)
L_LS = LOC(1)
L_RS = LOC(1)
L_SEAT = LOC(1)
N_LOC = LOC.n


def kernel(
    shared,
    owner_s,
    pg_h,
    l_h,
    r_h,
    ls_h,
    rs_h,
    ret,
    nl,
    nr,
    pg,
    far,
    chs,
    near,
    ch,
    hs,
    zrecv,
    shares,
    staged,
    gf,
    rf,
    lp,
    ls,
    rs,
    gt,
    tp,
    obuf,
    ostage,
    lx,
    rx,
    r2,
    rf2,
    tile_v,
    tile_s,
    send,
    recv,
    local,
    told,
):
    x = lax.axis_index("dp_0")
    zl = lax.axis_index("dp_1")
    y = lax.axis_index("owner_0")
    zh = lax.axis_index("owner_1")
    co = lax.axis_index("owner_2")
    me = (y * 4 + zh) * 2 + co
    d = x * 2 + zl
    xp = (x + 1) % 4
    xm = (x + 3) % 4
    x2 = (x + 2) % 4
    zo = 1 - zl
    here = zl * 32 + me
    to_xp = {"dp_0": xp}
    to_xm = {"dp_0": xm}
    to_z = {"dp_1": zo}
    to_core = {"owner_2": 1 - co}
    my_chip = me // 2
    own = SLOTS - 1 if shared else SLOTS
    last = SLOTS - 1
    far_by_x = (1, 2) if shared else (2,)

    def owner_device(i):
        return {"owner_0": i // 8, "owner_1": (i // 2) % 4, "owner_2": i % 2}

    def any_device(i):
        return {
            "dp_1": i // 32,
            "owner_0": (i // 8) % 4,
            "owner_1": (i // 2) % 4,
            "owner_2": i % 2,
        }

    sent = []

    def start(src, dst, sem, device):
        copy = pltpu.make_async_remote_copy(
            src_ref=src,
            dst_ref=dst,
            send_sem=send.at[sem],
            recv_sem=recv.at[sem],
            device_id=device,
            device_id_type=MESH,
        )
        copy.start()
        sent.append(copy)

    def arrived(dst, sem):
        pltpu.make_async_remote_copy(
            src_ref=dst,
            dst_ref=dst,
            send_sem=send.at[sem],
            recv_sem=recv.at[sem],
            device_id=to_xp,
            device_id_type=MESH,
        ).wait_recv()

    def start_upper(k, src, dst, sem, device):
        for first, count in RUNS[k][2]:
            start(src(pl.ds(first, count)), dst(pl.ds(first, count)), sem, device)
            sent.pop()
        sent.append(copy_of(upper(k, far), sem))

    def upper(k, buffer):
        return buffer.at[1, pl.ds(RUNS[k][0], sum(count for _, count in RUNS[k][2]))]

    def copy_of(ref, sem):
        return pltpu.make_async_remote_copy(
            src_ref=ref,
            dst_ref=ref,
            send_sem=send.at[sem],
            recv_sem=recv.at[sem],
            device_id=to_xp,
            device_id_type=MESH,
        )

    def lanes(block, width=COLS):
        return pl.ds(pl.multiple_of(block * width, width), width)

    def chunk(k):
        return pl.ds(RUNS[k][0], RUNS[k][1] - RUNS[k][0])

    pg_in = [
        pltpu.make_async_copy(pg_h.at[chunk(k)], pg.at[chunk(k)], local.at[L_PG(k)])
        for k in range(CHUNKS)
    ]
    for copy in pg_in:
        copy.start()
    own_rows = pl.ds(pl.multiple_of(d * LANES, LANES), LANES)
    pair_rows = pl.ds(pl.multiple_of(zl * LANES, LANES), LANES)
    r_in = [
        pltpu.make_async_copy(
            r_h.at[s, :, lanes(zl, HALF)], rf.at[s, own_rows, :], local.at[L_R(s)]
        )
        for s in range(own)
    ]
    l_in = [
        pltpu.make_async_copy(l_h.at[s], lp.at[s, pair_rows, :], local.at[L_L(s)])
        for s in range(own)
    ]
    core_rows = pl.ds(pl.multiple_of(co * 64, 64), 64)
    if shared:
        r_in.append(
            pltpu.make_async_copy(r_h.at[last, core_rows, :], rx.at[0], local.at[L_R(last)])
        )
        l_in.append(pltpu.make_async_copy(l_h.at[last], lx.at[0], local.at[L_L(last)]))
    ls_in = pltpu.make_async_copy(ls_h, ls, local.at[L_LS(0)])
    rs_in = pltpu.make_async_copy(rs_h, rs, local.at[L_RS(0)])
    for copy in (*r_in, *l_in, ls_in, rs_in):
        copy.start()

    barrier = pltpu.get_barrier_semaphore()
    y_sides = ({"owner_0": (y + 1) % 4}, {"owner_0": (y + 3) % 4})
    zh_sides = ({"owner_1": (zh + 1) % 4}, {"owner_1": (zh + 3) % 4})
    neighbours = (to_xp, to_xm, to_z, to_core, *y_sides, *zh_sides)
    for device in neighbours:
        pl.semaphore_signal(barrier, inc=1, device_id=device, device_id_type=MESH)

    seat = lax.broadcasted_iota(jnp.int32, (1, LANES), 1)

    def take(t, carry):
        tile, count = carry
        mine = seat % OWNERS == owner_s[t]
        tile = jnp.where(mine & (count == seat // OWNERS), t, tile)
        return tile, count + mine.astype(jnp.int32)

    tile_v[...], _ = lax.fori_loop(
        0, TILES, take, (jnp.full((1, LANES), TILES, jnp.int32), jnp.zeros((1, LANES), jnp.int32))
    )
    seats_in = pltpu.make_async_copy(tile_v, tile_s, local.at[L_SEAT(0)])
    seats_in.start()
    pl.semaphore_wait(barrier, len(neighbours))

    rounds = (y_sides, zh_sides, zh_sides, (to_core,), (to_z,))

    def tell(n):
        for device in rounds[n]:
            pl.semaphore_signal(told.at[n], inc=1, device_id=device, device_id_type=MESH)

    def heard(n):
        pl.semaphore_wait(told.at[n], len(rounds[n]))

    def send_near(k):
        start(pg.at[chunk(k), :, lanes(xp)], near.at[0, chunk(k)], NEAR(k, 0), to_xp)
        start_upper(
            k,
            lambda at: pg.at[at, :, lanes(4 + xm)],
            lambda at: near.at[1, at],
            NEAR(k, 1),
            to_xm,
        )

    for k in range(CHUNKS):
        pg_in[k].wait()
        start(pg.at[chunk(k), :, lanes(x2)], far.at[0, chunk(k)], FAR(k, 0), to_xm)
        start_upper(
            k,
            lambda at: pg.at[at, :, lanes(4 + x2)],
            lambda at: far.at[1, at],
            FAR(k, 1),
            to_xp,
        )
    send_near(0)
    tell(0)

    if shared:
        start(l_h.at[last], lx.at[1], LC(0), to_core)
        other_core_rows = pl.ds(pl.multiple_of(64 - co * 64, 64), 64)
        start(r_h.at[last, other_core_rows, :], rx.at[1], RC(0), to_core)
    for s in range(own):
        r_in[s].wait()
        start(r_h.at[s, :, lanes(zo, HALF)], rf.at[s, own_rows, :], RZ(s), to_z)
    if shared:
        seats_in.wait()
        r_in[last].wait()
        l_in[last].wait()
        arrived(lx.at[1], LC(0))
        arrived(rx.at[1], RC(0))
        second = (tile_s[0, 2 * OWNERS + 2 * my_chip + 1] < TILES).astype(jnp.int32)
        source = (second + co) % 2
        r2[...] = rx[source]

        @pl.when(zl == co)
        def _():
            lp[last, :LANES] = lx[source]

        rf2[d, co] = r2[:, lanes(zl, HALF)]
        start(r2.at[:, lanes(zo, HALF)], rf2.at[d, co], RZ(last), to_z)
    for s in range(2):
        start(l_h.at[s], lp.at[s, pair_rows, :], LZ(s), to_z)

    def per_tile(k, step):
        def one(t, carry):
            step(t)
            return carry

        lax.fori_loop(RUNS[k][0], RUNS[k][1], one, 0, unroll=2)

    for k in range(CHUNKS):
        arrived(far.at[0, chunk(k)], FAR(k, 0))
        arrived(upper(k, far), FAR(k, 1))

        def add_chain(t):
            chs[0, t] = (
                far[0, t].astype(F32) + pg[t, :, lanes(xm)].astype(F32)
            ).astype(BF16)
            chs[1, t] = (
                far[1, t].astype(F32) + pg[t, :, lanes(4 + xp)].astype(F32)
            ).astype(BF16)

        per_tile(k, add_chain)
        if k + 1 < CHUNKS:
            send_near(k + 1)
        if k < 4:
            heard(k)
            tell(k + 1)
        start(chs.at[0, chunk(k)], ch.at[0, chunk(k)], CHAIN(k, 0), to_xm)
        start_upper(k, lambda at: chs.at[1, at], lambda at: ch.at[1, at], CHAIN(k, 1), to_xp)

    def quad(chip, part, rows):
        return pl.ds(pl.multiple_of(chip * 256 + part, LANES), rows)

    def r_block(s, chip):
        if shared and s == last:
            return rf2.at[pl.ds(chip * 2, 2), co]
        return rf.at[s, quad(chip, 0, 256), :]

    def r_rows(s, chip, plane):
        if shared and s == last:
            return rf2.at[chip * 2 + plane, co]
        return rf.at[s, quad(chip, plane * LANES, LANES), :]

    for s in range(SLOTS):
        arrived(r_rows(s, x, zo), RZ(s))
        block = r_block(s, x)
        start(block, block, RN(s, 0), to_xp)
        start(block, block, RN(s, 1), to_xm)

    def total(half, t):
        return (
            pg[t, :, lanes(half * 4 + x)].astype(F32)
            + near[half, t].astype(F32)
            + ch[half, t].astype(F32)
        )

    for k in range(CHUNKS):
        arrived(near.at[0, chunk(k)], NEAR(k, 0))
        arrived(ch.at[0, chunk(k)], CHAIN(k, 0))
        arrived(upper(k, near), NEAR(k, 1))
        arrived(upper(k, ch), CHAIN(k, 1))

        def other_half(t):
            hs[t] = total(zo, t).astype(BF16)

        per_tile(k, other_half)
        start(hs.at[chunk(k)], zrecv.at[chunk(k)], ZZ(k), to_z)

    my_block = zl * 4 + x
    other_block = zo * 4 + x
    row_of = lax.broadcasted_iota(jnp.int32, (PIECE, COLS), 0) + me * PIECE
    col_of = lax.broadcasted_iota(jnp.int32, (PIECE, COLS), 1) + my_block * COLS
    for k in range(CHUNKS):
        arrived(zrecv.at[chunk(k)], ZZ(k))

        def share(t):
            rows, cols = extent(t)
            value = total(zl, t) + zrecv[t].astype(F32)
            shares[t] = jnp.where((row_of < rows) & (col_of < cols), value, 0.0).astype(BF16)

        per_tile(k, share)
    shares[TILES] = jnp.zeros((PIECE, COLS), BF16)

    my_cols = lanes(my_block)
    my_piece = pl.ds(pl.multiple_of(me * PIECE, PIECE), PIECE)
    if not shared:
        seats_in.wait()
    for s in range(own):

        def stage(o, carry):
            staged[s, o] = shares[tile_s[0, s * OWNERS + o]]
            return carry

        lax.fori_loop(0, OWNERS, stage, 0, unroll=4)

    if shared:

        def stage_last(k, carry):
            at = 2 * OWNERS + 2 * k
            staged[last, k] = shares[jnp.minimum(tile_s[0, at], tile_s[0, at + 1])]
            return carry

        lax.fori_loop(0, 16, stage_last, 0, unroll=4)

    side = y // 2

    def to_chip(k):
        pltpu.make_async_remote_copy(
            src_ref=staged.at[last, k],
            dst_ref=gf.at[last, my_piece, my_cols],
            send_sem=send.at[A2A(last)],
            recv_sem=recv.at[A2A(last)],
            device_id={"owner_0": k // 4, "owner_1": k % 4, "owner_2": side},
            device_id_type=MESH,
        ).start()

    def to_chips():
        def one(k, carry):
            to_chip((my_chip + k) % 16)
            return carry

        lax.fori_loop(1, 16, one, 0)

        @pl.when(side == co)
        def _():
            gf[last, my_piece, my_cols] = staged[last, my_chip]

        @pl.when(side != co)
        def _():
            to_chip(my_chip)

    def to_owners(s):
        def one(k, carry):
            o = (me + k) % OWNERS
            pltpu.make_async_remote_copy(
                src_ref=staged.at[s, o],
                dst_ref=gf.at[s, my_piece, my_cols],
                send_sem=send.at[A2A(s)],
                recv_sem=recv.at[A2A(s)],
                device_id=owner_device(o),
                device_id_type=MESH,
            ).start()
            return carry

        lax.fori_loop(1, OWNERS, one, 0)

    heard(4)
    to_owners(0)
    to_owners(1)
    for s in range(own):
        gf[s, my_piece, my_cols] = staged[s, me]

    def span(s, part=0, parts=1):
        first, rows = (co * 512, 512 // parts) if shared and s == last else (0, 1024 // parts)
        return pl.ds(pl.multiple_of(first + part * rows, 256), rows)

    def halves(s, part):
        return span(s, part, 2)

    def g_here(s):
        if shared and s == last:

            @pl.when(side == co)
            def _():
                arrived(staged.at[s, pl.ds(0, 15)], A2A(s))

            @pl.when(side != co)
            def _():
                arrived(staged.at[s, pl.ds(0, 16)], A2A(s))

        else:
            arrived(staged.at[s, pl.ds(0, OWNERS - 1)], A2A(s))
        block = gf.at[s, span(s), my_cols]
        start(block, block, GZ(s), to_z)

    def g_own(s):
        block = gf.at[s, span(s), my_cols]
        start(block, block, GN(s, 0), to_xp)
        start(block, block, GN(s, 1), to_xm)

    def g_pair(s):
        arrived(gf.at[s, span(s), lanes(other_block)], GZ(s))
        for turn in range(2):
            block = gf.at[s, halves(s, turn), lanes(other_block)]
            start(block, block, GP(s, 0, turn), to_xp)
            block = gf.at[s, halves(s, 1 - turn), lanes(other_block)]
            start(block, block, GP(s, 1, turn), to_xm)

    def g_far(s):
        arrived(gf.at[s, span(s), lanes(zl * 4 + xm)], GN(s, 0))
        block = gf.at[s, halves(s, 0), lanes(zl * 4 + xm)]
        start(block, block, GF(s, 0), to_xp)
        arrived(gf.at[s, span(s), lanes(zl * 4 + xp)], GN(s, 1))
        block = gf.at[s, halves(s, 1), lanes(zl * 4 + xp)]
        start(block, block, GF(s, 1), to_xm)

    def g_far_pair(s):
        arrived(gf.at[s, halves(s, 0), lanes(zo * 4 + xm)], GP(s, 0, 0))
        block = gf.at[s, halves(s, 0), lanes(zo * 4 + xm)]
        start(block, block, GPF(s, 0), to_xp)
        arrived(gf.at[s, halves(s, 1), lanes(zo * 4 + xp)], GP(s, 1, 0))
        block = gf.at[s, halves(s, 1), lanes(zo * 4 + xp)]
        start(block, block, GPF(s, 1), to_xm)

    def g_far_here(s):
        arrived(gf.at[s, halves(s, 0), lanes(zl * 4 + x2)], GF(s, 0))
        arrived(gf.at[s, halves(s, 1), lanes(zl * 4 + x2)], GF(s, 1))

    def g_far_z(s):
        g_far_here(s)
        block = gf.at[s, span(s), lanes(zl * 4 + x2)]
        start(block, block, GZ_FAR(s), to_z)

    def g_done(s):
        if s not in far_by_x:
            arrived(gf.at[s, halves(s, 0), lanes(zo * 4 + xm)], GP(s, 0, 0))
            arrived(gf.at[s, halves(s, 1), lanes(zo * 4 + xp)], GP(s, 1, 0))
        arrived(gf.at[s, halves(s, 1), lanes(zo * 4 + xm)], GP(s, 0, 1))
        arrived(gf.at[s, halves(s, 0), lanes(zo * 4 + xp)], GP(s, 1, 1))
        if s not in far_by_x:
            arrived(gf.at[s, span(s), lanes(zo * 4 + x2)], GZ_FAR(s))
        else:
            arrived(gf.at[s, halves(s, 0), lanes(zo * 4 + x2)], GPF(s, 0))
            arrived(gf.at[s, halves(s, 1), lanes(zo * 4 + x2)], GPF(s, 1))

    def cross(plane, part):
        block = gf.at[last, span(last), lanes(plane, HALF)]
        start(block, block, CC(part), to_core)

    def crossed(plane, part):
        rows = pl.ds(pl.multiple_of(512 - co * 512, 512), 512)
        arrived(gf.at[last, rows, lanes(plane, HALF)], CC(part))

    def r_far(s):
        arrived(r_block(s, xm), RN(s, 0))
        block = r_rows(s, xm, 0)
        start(block, block, RF(s, 0), to_xp)
        arrived(r_block(s, xp), RN(s, 1))
        block = r_rows(s, xp, 1)
        start(block, block, RF(s, 1), to_xm)

    def r_done(s):
        arrived(r_rows(s, x2, 0), RF(s, 0))
        arrived(r_rows(s, x2, 1), RF(s, 1))

    def l_done(s):
        if shared and s == last:

            @pl.when(zl != co)
            def _():
                arrived(lp.at[last, pl.ds(0, LANES), :], LZ(last))

        else:
            arrived(lp.at[s, pair_rows, :], LZ(s))

    def l_last():
        if shared:

            @pl.when(zl == co)
            def _():
                block = lp.at[last, pl.ds(0, LANES), :]
                start(block, block, LZ(last), to_z)
                sent.pop()

        else:
            start(l_h.at[last], lp.at[last, pair_rows, :], LZ(last), to_z)

    def r_cross():
        start(rf2.at[:, co], rf2.at[:, co], RX(0), to_core)

    def grams(s):
        gt[...] = gf[s, :, lanes(d)].T
        grad_rows = gf[s, pl.ds(pl.multiple_of(d * LANES, LANES), LANES), :]

        weight = 1.0 - stat_decay
        if shared and s == last:
            weight = jnp.where(tile_s[0, 2 * OWNERS + me] < TILES, F32(weight), F32(0.0))

        def columns(n, carry):
            at = pl.ds(pl.multiple_of(n * 256, 256), 256)
            right = jnp.dot(gt[...], gf[s, :, at], preferred_element_type=F32)
            nr[s, :, at] = stat_decay * rs[s, :, at] + weight * right
            left = lax.dot_general(
                grad_rows, gf[s, at, :], (((1,), (1,)), ((), ())), preferred_element_type=F32
            )
            nl[s, :, at] = stat_decay * ls[s, :, at] + weight * left
            return carry

        lax.fori_loop(0, 4, columns, 0)

    out_cols = lanes(zl, HALF)

    def left_part(s, half):
        def columns(n, carry):
            at = pl.ds(pl.multiple_of(half * HALF + n * 256, 256), 256)
            if shared and s == last:
                part = jnp.dot(lp[s, :LANES], gf[s, :, at], preferred_element_type=F32)
                tp[:LANES, at] = part.astype(BF16)
            else:
                part = jnp.dot(lp[s], gf[s, :, at], preferred_element_type=F32)
                tp[:, at] = part.astype(BF16)
            return carry

        lax.fori_loop(0, 2, columns, 0)

    def direction_rows(s):
        half = shared and s == last
        chips = 16 if half else 32
        chip = my_chip if half else here // 2
        at_owner = 2 * OWNERS + my_chip if half else s * OWNERS + me

        def columns(n, carry):
            at = pl.ds(pl.multiple_of(n * 256, 256), 256)
            if half:
                right = rf2[:, :, :, at].reshape(TILE, 256)
                obuf[:LANES, at] = jnp.dot(tp[:LANES], right, preferred_element_type=F32)
            else:
                obuf[:, at] = jnp.dot(tp[...], rf[s, :, at], preferred_element_type=F32)
            return carry

        lax.fori_loop(0, 2, columns, 0)

        def rows(i):
            value = obuf[pl.ds(pl.multiple_of(i * 8, 8), 8), :]
            ostage[s, 2 * i] = value[:4].astype(BF16)
            ostage[s, 2 * i + 1] = value[4:].astype(BF16)

        def give(i, core):
            pltpu.make_async_remote_copy(
                src_ref=ostage.at[s, 2 * i + core],
                dst_ref=ret.at[at_owner, :, out_cols],
                send_sem=send.at[RET(s)],
                recv_sem=recv.at[RET(s)],
                device_id={
                    "dp_1": co if half else i // 16,
                    "owner_0": (i // 4) % 4,
                    "owner_1": i % 4,
                    "owner_2": core,
                },
                device_id_type=MESH,
            ).start()

        rows((chip + 1) % chips)

        def one(k, carry):
            rows((chip + k + 1) % chips)
            give((chip + k) % chips, 0)
            give((chip + k) % chips, 1)
            return carry

        lax.fori_loop(1, chips, one, 0)
        if half:

            @pl.when(zl == co)
            def _():
                ret[at_owner, :, out_cols] = ostage[s, me]
                give(chip, 1 - co)

            @pl.when(zl != co)
            def _():
                give(chip, 0)
                give(chip, 1)

        else:
            ret[at_owner, :, out_cols] = ostage[s, here]
            give(chip, 1 - co)

    g_here(0)
    g_own(0)
    if shared:
        to_chips()
    else:
        to_owners(2)
    r_far(0)
    r_far(1)
    r_far(2)
    g_pair(0)
    g_far(0)
    g_here(1)
    g_own(1)
    g_pair(1)
    g_here(2)
    g_far_z(0)
    l_last()
    g_far(1)
    if 1 in far_by_x:
        g_far_pair(1)
    g_own(2)
    g_pair(2)
    r_done(2)
    if shared:
        r_cross()
    for s in range(own):
        l_in[s].wait()
    ls_in.wait()
    rs_in.wait()
    g_done(0)
    r_done(0)
    l_done(0)
    left_part(0, 0)
    left_part(0, 1)
    direction_rows(0)
    grams(0)
    if 1 in far_by_x:
        g_far_here(1)
    else:
        g_far_z(1)
        g_far(2)
        g_far_pair(2)
    g_done(1)
    r_done(1)
    l_done(1)
    left_part(1, 0)
    left_part(1, 1)
    direction_rows(1)
    if 1 in far_by_x:
        g_far(2)
        g_far_pair(2)
    if shared:
        g_far_here(2)
        cross(zl, 0)
    l_done(2)
    if shared:
        g_done(2)
        cross(zo, 1)
        crossed(zl, 0)
        left_part(2, zl)
        crossed(zo, 1)
        arrived(rf2.at[:, 1 - co], RX(0))
    else:
        g_far_here(2)
        left_part(2, zl)
        g_done(2)
    left_part(2, zo)
    direction_rows(2)
    grams(1)
    grams(2)
    def ends(sem, few, many, first, wait):
        @pl.when(first)
        def _():
            wait(few, sem)

        @pl.when(jnp.logical_not(first))
        def _():
            wait(many, sem)

    for s in range(own):
        arrived(ostage.at[s, pl.ds(0, 63)], RET(s))
    few, many = ostage.at[last, pl.ds(0, 31)], ostage.at[last, pl.ds(0, 32)]
    if shared:
        ends(RET(last), few, many, zl == co, arrived)
    for copy in sent:
        copy.wait_send()

    def left(src, sem):
        pltpu.make_async_remote_copy(
            src_ref=src,
            dst_ref=src,
            send_sem=send.at[sem],
            recv_sem=recv.at[sem],
            device_id=to_xp,
            device_id_type=MESH,
        ).wait_send()

    for s in range(own):
        left(staged.at[s, pl.ds(0, OWNERS - 1)], A2A(s))
        left(ostage.at[s, pl.ds(0, 63)], RET(s))
    if shared:
        ends(RET(last), few, many, zl == co, left)
        few, many = staged.at[last, pl.ds(0, 15)], staged.at[last, pl.ds(0, 16)]
        ends(A2A(last), few, many, side == co, left)

        @pl.when(zl == co)
        def _():
            left(lp.at[last, pl.ds(0, LANES), :], LZ(last))


def write_out(shared, owner_s, ret, nl, nr, dir_h, nl_h, nr_h, rows_v, count_s, sems):
    copies = [
        pltpu.make_async_copy(nl, nl_h, sems.at[0]),
        pltpu.make_async_copy(nr, nr_h, sems.at[1]),
    ]
    for copy in copies:
        copy.start()
    d = lax.axis_index(DP)
    me = lax.axis_index(OWNER)
    line = lax.broadcasted_iota(jnp.int32, (4, TILE), 0) + (d * LANES + me * 4)
    lane = lax.broadcasted_iota(jnp.int32, (4, TILE), 1)

    def clear(o, carry):
        count_s[o] = 0
        return carry

    lax.fori_loop(0, OWNERS, clear, 0, unroll=8)

    def write(t, carry):
        rows, cols = extent(t)
        owner = owner_s[t]
        taken = count_s[owner]
        count_s[owner] = taken + OWNERS
        place = taken + owner
        if shared:
            place = jnp.where(taken < 2 * OWNERS, place, 2 * OWNERS + owner // 2)
        value = ret[place].astype(F32)
        rows_v[t] = jnp.where((line < rows) & (lane < cols), value, 0.0).astype(BF16)
        return carry

    lax.fori_loop(0, TILES, write, 0, unroll=4)
    copies.append(pltpu.make_async_copy(rows_v, dir_h, sems.at[2]))
    copies[2].start()
    for copy in copies:
        copy.wait()


def step(shared, owner_map, *arrays):
    smem = pl.BlockSpec(memory_space=pltpu.SMEM)
    vmem = pl.BlockSpec(memory_space=pltpu.VMEM)
    hbm = pl.BlockSpec(memory_space=pltpu.HBM)
    returned, new_left, new_right = pl.pallas_call(
        functools.partial(kernel, shared),
        out_shape=(
            pltpu.VMEM((SLOTS * OWNERS, 4, TILE), BF16),
            pltpu.VMEM((SLOTS, LANES, TILE), F32),
            pltpu.VMEM((SLOTS, LANES, TILE), F32),
        ),
        in_specs=[smem, hbm, hbm, hbm, hbm, hbm],
        out_specs=(vmem, vmem, vmem),
        scratch_shapes=[
            pltpu.VMEM((TILES, PIECE, TILE), BF16),
            pltpu.VMEM((2, TILES, PIECE, COLS), BF16),
            pltpu.VMEM((2, TILES, PIECE, COLS), BF16),
            pltpu.VMEM((2, TILES, PIECE, COLS), BF16),
            pltpu.VMEM((2, TILES, PIECE, COLS), BF16),
            pltpu.VMEM((TILES, PIECE, COLS), BF16),
            pltpu.VMEM((TILES, PIECE, COLS), BF16),
            pltpu.VMEM((TILES + 1, PIECE, COLS), BF16),
            pltpu.VMEM((SLOTS, OWNERS, PIECE, COLS), BF16),
            pltpu.VMEM((SLOTS, TILE, TILE), BF16),
            pltpu.VMEM((SLOTS, TILE, HALF), BF16),
            pltpu.VMEM((SLOTS, 256, TILE), BF16),
            pltpu.VMEM((SLOTS, LANES, TILE), F32),
            pltpu.VMEM((SLOTS, LANES, TILE), F32),
            pltpu.VMEM((LANES, TILE), BF16),
            pltpu.VMEM((256, TILE), BF16),
            pltpu.VMEM((256, HALF), F32),
            pltpu.VMEM((SLOTS, 64, 4, HALF), BF16),
            pltpu.VMEM((2, LANES, TILE), BF16),
            pltpu.VMEM((2, 64, TILE), BF16),
            pltpu.VMEM((64, TILE), BF16),
            pltpu.VMEM((8, 2, 64, HALF), BF16),
            pltpu.VMEM((1, LANES), jnp.int32),
            pltpu.SMEM((1, LANES), jnp.int32),
            pltpu.SemaphoreType.DMA((N_SEMS,)),
            pltpu.SemaphoreType.DMA((N_SEMS,)),
            pltpu.SemaphoreType.DMA((N_LOC,)),
            pltpu.SemaphoreType.REGULAR((5,)),
        ],
        compiler_params=pltpu.CompilerParams(
            collective_id=int(shared), has_side_effects=True, vmem_limit_bytes=60 * 1024 * 1024
        ),
    )(owner_map, *arrays)
    return pl.pallas_call(
        functools.partial(write_out, shared),
        out_shape=(
            jax.ShapeDtypeStruct((TILES, 4, TILE), BF16),
            jax.ShapeDtypeStruct((SLOTS, LANES, TILE), F32),
            jax.ShapeDtypeStruct((SLOTS, LANES, TILE), F32),
        ),
        in_specs=[smem, vmem, vmem, vmem],
        out_specs=(hbm, hbm, hbm),
        scratch_shapes=[
            pltpu.VMEM((TILES, 4, TILE), BF16),
            pltpu.SMEM((OWNERS,), jnp.int32),
            pltpu.SemaphoreType.DMA((3,)),
        ],
        compiler_params=pltpu.CompilerParams(vmem_limit_bytes=4 * 1024 * 1024),
    )(
        owner_map,
        *(
            pltpu.with_memory_space_constraint(value, pltpu.VMEM)
            for value in (returned, new_left, new_right)
        ),
    )


def body(partial_grads, owner_map, left_stats, right_stats, left_roots, right_roots):
    chips = jnp.arange(OWNERS // 2, dtype=jnp.int32)
    first = 2 * chips[:, None]
    on_chip = (owner_map[None, :] >= first) & (owner_map[None, :] < first + 2)
    held = jnp.sum(on_chip.astype(jnp.int32), axis=1)
    direction, new_left, new_right = lax.cond(
        jnp.max(held) < 2 * SLOTS,
        functools.partial(step, True),
        functools.partial(step, False),
        owner_map,
        partial_grads[0],
        left_roots[0],
        right_roots[0],
        left_stats[0],
        right_stats[0],
    )
    return direction, new_left[None], new_right[None]


def solution(mesh):
    torus = Mesh(
        mesh.devices.reshape(4, 2, 4, 4, 2), ("dp_0", "dp_1", "owner_0", "owner_1", "owner_2")
    )
    in_specs = (
        P(DP, None, OWNER, None),
        P(),
        P(OWNER, None, DP, None),
        P(OWNER, None, DP, None),
        P(OWNER, None, DP, None),
        P(OWNER, None, DP, None),
    )
    out_specs = (P(None, DP_OWNER, None), P(OWNER, None, DP, None), P(OWNER, None, DP, None))
    return jax.shard_map(body, mesh=torus, in_specs=in_specs, out_specs=out_specs, check_vma=False)
```

```python
import functools

import jax
import jax.numpy as jnp
from jax import lax
from jax.experimental import pallas as pl
from jax.experimental.pallas import tpu as pltpu
from jax.sharding import Mesh
from jax.sharding import PartitionSpec as P

D_MODEL = 2560
D_IN = 10576
D_INNER = 5120
TILE = 1024
TILES = 48
OWNERS = 32
SLOTS = 3
PIECE = 32
LANES = 128
COLS = 128
HALF = 512
RUNS = (
    (33, 48, ((33, 2), (36, 2), (39, 2), (42, 2), (45, 2))),
    (0, 11, ((0, 10),)),
    (11, 22, ((11, 10),)),
    (22, 28, ((22, 6),)),
    (28, 33, ((28, 4),)),
)
CHUNKS = len(RUNS)
OWNER = ("owner_0", "owner_1", "owner_2")
DP = ("dp_0", "dp_1")
DP_OWNER = ("dp_0", "dp_1", "owner_0", "owner_1", "owner_2")
MESH = pl.DeviceIdType.MESH
F32 = jnp.float32
BF16 = jnp.bfloat16

stat_decay = 0.999


def extent(t):
    in_cols = -(-D_IN // TILE)
    out_cols = -(-D_MODEL // TILE)
    in_count = -(-D_MODEL // TILE) * in_cols
    other = jnp.maximum(t - in_count, 0)
    is_in = t < in_count
    rows = jnp.where(
        is_in,
        jnp.minimum(TILE, D_MODEL - t // in_cols * TILE),
        jnp.minimum(TILE, D_INNER - other // out_cols * TILE),
    )
    cols = jnp.where(
        is_in,
        jnp.minimum(TILE, D_IN - t % in_cols * TILE),
        jnp.minimum(TILE, D_MODEL - other % out_cols * TILE),
    )
    return rows, cols


class Ids:
    def __init__(self):
        self.n = 0

    def __call__(self, *shape):
        size = 1
        for s in shape:
            size *= s
        base = self.n
        self.n += size

        def at(*index):
            flat = 0
            for i, s in zip(index, shape):
                flat = flat * s + i
            return base + flat

        return at


IDS = Ids()
FAR = IDS(CHUNKS, 2)
NEAR = IDS(CHUNKS, 2)
CHAIN = IDS(CHUNKS, 2)
ZZ = IDS(CHUNKS)
RZ = IDS(SLOTS)
RN = IDS(SLOTS, 2)
RF = IDS(SLOTS, 2)
LZ = IDS(SLOTS)
A2A = IDS(SLOTS)
GZ = IDS(SLOTS)
GZ_FAR = IDS(SLOTS)
GN = IDS(SLOTS, 2)
GP = IDS(SLOTS, 2, 2)
GF = IDS(SLOTS, 2)
GPF = IDS(SLOTS, 2)
RET = IDS(SLOTS)
LC = IDS(1)
RC = IDS(1)
RX = IDS(1)
CC = IDS(2)
N_SEMS = IDS.n
LOC = Ids()
L_PG = LOC(CHUNKS)
L_R = LOC(SLOTS)
L_L = LOC(SLOTS)
L_LS = LOC(1)
L_RS = LOC(1)
L_SEAT = LOC(1)
N_LOC = LOC.n


def kernel(
    shared,
    owner_s,
    pg_h,
    l_h,
    r_h,
    ls_h,
    rs_h,
    ret,
    nl,
    nr,
    pg,
    far,
    chs,
    near,
    ch,
    hs,
    zrecv,
    shares,
    staged,
    gf,
    rf,
    lp,
    ls,
    rs,
    gt,
    tp,
    obuf,
    ostage,
    lx,
    rx,
    r2,
    rf2,
    tile_v,
    tile_s,
    send,
    recv,
    local,
    told,
):
    x = lax.axis_index("dp_0")
    zl = lax.axis_index("dp_1")
    y = lax.axis_index("owner_0")
    zh = lax.axis_index("owner_1")
    co = lax.axis_index("owner_2")
    me = (y * 4 + zh) * 2 + co
    d = x * 2 + zl
    xp = (x + 1) % 4
    xm = (x + 3) % 4
    x2 = (x + 2) % 4
    zo = 1 - zl
    here = zl * 32 + me
    to_xp = {"dp_0": xp}
    to_xm = {"dp_0": xm}
    to_z = {"dp_1": zo}
    to_core = {"owner_2": 1 - co}
    my_chip = me // 2
    own = SLOTS - 1 if shared else SLOTS
    last = SLOTS - 1
    far_by_x = (1, 2) if shared else (2,)

    def owner_device(i):
        return {"owner_0": i // 8, "owner_1": (i // 2) % 4, "owner_2": i % 2}

    def any_device(i):
        return {
            "dp_1": i // 32,
            "owner_0": (i // 8) % 4,
            "owner_1": (i // 2) % 4,
            "owner_2": i % 2,
        }

    sent = []

    def start(src, dst, sem, device):
        copy = pltpu.make_async_remote_copy(
            src_ref=src,
            dst_ref=dst,
            send_sem=send.at[sem],
            recv_sem=recv.at[sem],
            device_id=device,
            device_id_type=MESH,
        )
        copy.start()
        sent.append(copy)

    def arrived(dst, sem):
        pltpu.make_async_remote_copy(
            src_ref=dst,
            dst_ref=dst,
            send_sem=send.at[sem],
            recv_sem=recv.at[sem],
            device_id=to_xp,
            device_id_type=MESH,
        ).wait_recv()

    def start_upper(k, src, dst, sem, device):
        for first, count in RUNS[k][2]:
            start(src(pl.ds(first, count)), dst(pl.ds(first, count)), sem, device)
            sent.pop()
        sent.append(copy_of(upper(k, far), sem))

    def upper(k, buffer):
        return buffer.at[1, pl.ds(RUNS[k][0], sum(count for _, count in RUNS[k][2]))]

    def copy_of(ref, sem):
        return pltpu.make_async_remote_copy(
            src_ref=ref,
            dst_ref=ref,
            send_sem=send.at[sem],
            recv_sem=recv.at[sem],
            device_id=to_xp,
            device_id_type=MESH,
        )

    def lanes(block, width=COLS):
        return pl.ds(pl.multiple_of(block * width, width), width)

    def chunk(k):
        return pl.ds(RUNS[k][0], RUNS[k][1] - RUNS[k][0])

    pg_in = [
        pltpu.make_async_copy(pg_h.at[chunk(k)], pg.at[chunk(k)], local.at[L_PG(k)])
        for k in range(CHUNKS)
    ]
    for copy in pg_in:
        copy.start()
    own_rows = pl.ds(pl.multiple_of(d * LANES, LANES), LANES)
    pair_rows = pl.ds(pl.multiple_of(zl * LANES, LANES), LANES)
    r_in = [
        pltpu.make_async_copy(
            r_h.at[s, :, lanes(zl, HALF)], rf.at[s, own_rows, :], local.at[L_R(s)]
        )
        for s in range(own)
    ]
    l_in = [
        pltpu.make_async_copy(l_h.at[s], lp.at[s, pair_rows, :], local.at[L_L(s)])
        for s in range(own)
    ]
    core_rows = pl.ds(pl.multiple_of(co * 64, 64), 64)
    if shared:
        r_in.append(
            pltpu.make_async_copy(r_h.at[last, core_rows, :], rx.at[0], local.at[L_R(last)])
        )
        l_in.append(pltpu.make_async_copy(l_h.at[last], lx.at[0], local.at[L_L(last)]))
    ls_in = pltpu.make_async_copy(ls_h, ls, local.at[L_LS(0)])
    rs_in = pltpu.make_async_copy(rs_h, rs, local.at[L_RS(0)])
    for copy in (*r_in, *l_in, ls_in, rs_in):
        copy.start()

    barrier = pltpu.get_barrier_semaphore()
    y_sides = ({"owner_0": (y + 1) % 4}, {"owner_0": (y + 3) % 4})
    zh_sides = ({"owner_1": (zh + 1) % 4}, {"owner_1": (zh + 3) % 4})
    neighbours = (to_xp, to_xm, to_z, to_core, *y_sides, *zh_sides)
    for device in neighbours:
        pl.semaphore_signal(barrier, inc=1, device_id=device, device_id_type=MESH)

    seat = lax.broadcasted_iota(jnp.int32, (1, LANES), 1)

    def take(t, carry):
        tile, count = carry
        mine = seat % OWNERS == owner_s[t]
        tile = jnp.where(mine & (count == seat // OWNERS), t, tile)
        return tile, count + mine.astype(jnp.int32)

    tile_v[...], _ = lax.fori_loop(
        0, TILES, take, (jnp.full((1, LANES), TILES, jnp.int32), jnp.zeros((1, LANES), jnp.int32))
    )
    seats_in = pltpu.make_async_copy(tile_v, tile_s, local.at[L_SEAT(0)])
    seats_in.start()
    pl.semaphore_wait(barrier, len(neighbours))

    rounds = (y_sides, zh_sides, zh_sides, (to_core,), (to_z,))

    def tell(n):
        for device in rounds[n]:
            pl.semaphore_signal(told.at[n], inc=1, device_id=device, device_id_type=MESH)

    def heard(n):
        pl.semaphore_wait(told.at[n], len(rounds[n]))

    def send_near(k):
        start(pg.at[chunk(k), :, lanes(xp)], near.at[0, chunk(k)], NEAR(k, 0), to_xp)
        start_upper(
            k,
            lambda at: pg.at[at, :, lanes(4 + xm)],
            lambda at: near.at[1, at],
            NEAR(k, 1),
            to_xm,
        )

    for k in range(CHUNKS):
        pg_in[k].wait()
        start(pg.at[chunk(k), :, lanes(x2)], far.at[0, chunk(k)], FAR(k, 0), to_xm)
        start_upper(
            k,
            lambda at: pg.at[at, :, lanes(4 + x2)],
            lambda at: far.at[1, at],
            FAR(k, 1),
            to_xp,
        )
    send_near(0)
    tell(0)

    if shared:
        start(l_h.at[last], lx.at[1], LC(0), to_core)
        other_core_rows = pl.ds(pl.multiple_of(64 - co * 64, 64), 64)
        start(r_h.at[last, other_core_rows, :], rx.at[1], RC(0), to_core)
    for s in range(own):
        r_in[s].wait()
        start(r_h.at[s, :, lanes(zo, HALF)], rf.at[s, own_rows, :], RZ(s), to_z)
    if shared:
        seats_in.wait()
        r_in[last].wait()
        l_in[last].wait()
        arrived(lx.at[1], LC(0))
        arrived(rx.at[1], RC(0))
        second = (tile_s[0, 2 * OWNERS + 2 * my_chip + 1] < TILES).astype(jnp.int32)
        source = (second + co) % 2
        r2[...] = rx[source]

        @pl.when(zl == co)
        def _():
            lp[last, :LANES] = lx[source]

        rf2[d, co] = r2[:, lanes(zl, HALF)]
        start(r2.at[:, lanes(zo, HALF)], rf2.at[d, co], RZ(last), to_z)
    for s in range(2):
        start(l_h.at[s], lp.at[s, pair_rows, :], LZ(s), to_z)

    def per_tile(k, step):
        def one(t, carry):
            step(t)
            return carry

        lax.fori_loop(RUNS[k][0], RUNS[k][1], one, 0, unroll=2)

    for k in range(CHUNKS):
        arrived(far.at[0, chunk(k)], FAR(k, 0))
        arrived(upper(k, far), FAR(k, 1))

        def add_chain(t):
            chs[0, t] = (
                far[0, t].astype(F32) + pg[t, :, lanes(xm)].astype(F32)
            ).astype(BF16)
            chs[1, t] = (
                far[1, t].astype(F32) + pg[t, :, lanes(4 + xp)].astype(F32)
            ).astype(BF16)

        per_tile(k, add_chain)
        if k + 1 < CHUNKS:
            send_near(k + 1)
        if k < 4:
            heard(k)
            tell(k + 1)
        start(chs.at[0, chunk(k)], ch.at[0, chunk(k)], CHAIN(k, 0), to_xm)
        start_upper(k, lambda at: chs.at[1, at], lambda at: ch.at[1, at], CHAIN(k, 1), to_xp)

    def quad(chip, part, rows):
        return pl.ds(pl.multiple_of(chip * 256 + part, LANES), rows)

    def r_block(s, chip):
        if shared and s == last:
            return rf2.at[pl.ds(chip * 2, 2), co]
        return rf.at[s, quad(chip, 0, 256), :]

    def r_rows(s, chip, plane):
        if shared and s == last:
            return rf2.at[chip * 2 + plane, co]
        return rf.at[s, quad(chip, plane * LANES, LANES), :]

    for s in range(SLOTS):
        arrived(r_rows(s, x, zo), RZ(s))
        block = r_block(s, x)
        start(block, block, RN(s, 0), to_xp)
        start(block, block, RN(s, 1), to_xm)

    def total(half, t):
        return (
            pg[t, :, lanes(half * 4 + x)].astype(F32)
            + near[half, t].astype(F32)
            + ch[half, t].astype(F32)
        )

    for k in range(CHUNKS):
        arrived(near.at[0, chunk(k)], NEAR(k, 0))
        arrived(ch.at[0, chunk(k)], CHAIN(k, 0))
        arrived(upper(k, near), NEAR(k, 1))
        arrived(upper(k, ch), CHAIN(k, 1))

        def other_half(t):
            hs[t] = total(zo, t).astype(BF16)

        per_tile(k, other_half)
        start(hs.at[chunk(k)], zrecv.at[chunk(k)], ZZ(k), to_z)

    my_block = zl * 4 + x
    other_block = zo * 4 + x
    row_of = lax.broadcasted_iota(jnp.int32, (PIECE, COLS), 0) + me * PIECE
    col_of = lax.broadcasted_iota(jnp.int32, (PIECE, COLS), 1) + my_block * COLS
    for k in range(CHUNKS):
        arrived(zrecv.at[chunk(k)], ZZ(k))

        def share(t):
            rows, cols = extent(t)
            value = total(zl, t) + zrecv[t].astype(F32)
            shares[t] = jnp.where((row_of < rows) & (col_of < cols), value, 0.0).astype(BF16)

        per_tile(k, share)
    shares[TILES] = jnp.zeros((PIECE, COLS), BF16)

    my_cols = lanes(my_block)
    my_piece = pl.ds(pl.multiple_of(me * PIECE, PIECE), PIECE)
    if not shared:
        seats_in.wait()
    for s in range(own):

        def stage(o, carry):
            staged[s, o] = shares[tile_s[0, s * OWNERS + o]]
            return carry

        lax.fori_loop(0, OWNERS, stage, 0, unroll=4)

    if shared:

        def stage_last(k, carry):
            at = 2 * OWNERS + 2 * k
            staged[last, k] = shares[jnp.minimum(tile_s[0, at], tile_s[0, at + 1])]
            return carry

        lax.fori_loop(0, 16, stage_last, 0, unroll=4)

    side = y // 2

    def to_chip(k):
        pltpu.make_async_remote_copy(
            src_ref=staged.at[last, k],
            dst_ref=gf.at[last, my_piece, my_cols],
            send_sem=send.at[A2A(last)],
            recv_sem=recv.at[A2A(last)],
            device_id={"owner_0": k // 4, "owner_1": k % 4, "owner_2": side},
            device_id_type=MESH,
        ).start()

    def to_chips():
        def one(k, carry):
            to_chip((my_chip + k) % 16)
            return carry

        lax.fori_loop(1, 16, one, 0)

        @pl.when(side == co)
        def _():
            gf[last, my_piece, my_cols] = staged[last, my_chip]

        @pl.when(side != co)
        def _():
            to_chip(my_chip)

    def to_owners(s):
        def one(k, carry):
            o = (me + k) % OWNERS
            pltpu.make_async_remote_copy(
                src_ref=staged.at[s, o],
                dst_ref=gf.at[s, my_piece, my_cols],
                send_sem=send.at[A2A(s)],
                recv_sem=recv.at[A2A(s)],
                device_id=owner_device(o),
                device_id_type=MESH,
            ).start()
            return carry

        lax.fori_loop(1, OWNERS, one, 0)

    heard(4)
    to_owners(0)
    to_owners(1)
    for s in range(own):
        gf[s, my_piece, my_cols] = staged[s, me]

    def span(s, part=0, parts=1):
        first, rows = (co * 512, 512 // parts) if shared and s == last else (0, 1024 // parts)
        return pl.ds(pl.multiple_of(first + part * rows, 256), rows)

    def halves(s, part):
        return span(s, part, 2)

    def g_here(s):
        if shared and s == last:

            @pl.when(side == co)
            def _():
                arrived(staged.at[s, pl.ds(0, 15)], A2A(s))

            @pl.when(side != co)
            def _():
                arrived(staged.at[s, pl.ds(0, 16)], A2A(s))

        else:
            arrived(staged.at[s, pl.ds(0, OWNERS - 1)], A2A(s))
        block = gf.at[s, span(s), my_cols]
        start(block, block, GZ(s), to_z)

    def g_own(s):
        block = gf.at[s, span(s), my_cols]
        start(block, block, GN(s, 0), to_xp)
        start(block, block, GN(s, 1), to_xm)

    def g_pair(s):
        arrived(gf.at[s, span(s), lanes(other_block)], GZ(s))
        for turn in range(2):
            block = gf.at[s, halves(s, turn), lanes(other_block)]
            start(block, block, GP(s, 0, turn), to_xp)
            block = gf.at[s, halves(s, 1 - turn), lanes(other_block)]
            start(block, block, GP(s, 1, turn), to_xm)

    def g_far(s):
        arrived(gf.at[s, span(s), lanes(zl * 4 + xm)], GN(s, 0))
        block = gf.at[s, halves(s, 0), lanes(zl * 4 + xm)]
        start(block, block, GF(s, 0), to_xp)
        arrived(gf.at[s, span(s), lanes(zl * 4 + xp)], GN(s, 1))
        block = gf.at[s, halves(s, 1), lanes(zl * 4 + xp)]
        start(block, block, GF(s, 1), to_xm)

    def g_far_pair(s):
        arrived(gf.at[s, halves(s, 0), lanes(zo * 4 + xm)], GP(s, 0, 0))
        block = gf.at[s, halves(s, 0), lanes(zo * 4 + xm)]
        start(block, block, GPF(s, 0), to_xp)
        arrived(gf.at[s, halves(s, 1), lanes(zo * 4 + xp)], GP(s, 1, 0))
        block = gf.at[s, halves(s, 1), lanes(zo * 4 + xp)]
        start(block, block, GPF(s, 1), to_xm)

    def g_far_here(s):
        arrived(gf.at[s, halves(s, 0), lanes(zl * 4 + x2)], GF(s, 0))
        arrived(gf.at[s, halves(s, 1), lanes(zl * 4 + x2)], GF(s, 1))

    def g_far_z(s):
        g_far_here(s)
        block = gf.at[s, span(s), lanes(zl * 4 + x2)]
        start(block, block, GZ_FAR(s), to_z)

    def g_done(s):
        if s not in far_by_x:
            arrived(gf.at[s, halves(s, 0), lanes(zo * 4 + xm)], GP(s, 0, 0))
            arrived(gf.at[s, halves(s, 1), lanes(zo * 4 + xp)], GP(s, 1, 0))
        arrived(gf.at[s, halves(s, 1), lanes(zo * 4 + xm)], GP(s, 0, 1))
        arrived(gf.at[s, halves(s, 0), lanes(zo * 4 + xp)], GP(s, 1, 1))
        if s not in far_by_x:
            arrived(gf.at[s, span(s), lanes(zo * 4 + x2)], GZ_FAR(s))
        else:
            arrived(gf.at[s, halves(s, 0), lanes(zo * 4 + x2)], GPF(s, 0))
            arrived(gf.at[s, halves(s, 1), lanes(zo * 4 + x2)], GPF(s, 1))

    def cross(plane, part):
        block = gf.at[last, span(last), lanes(plane, HALF)]
        start(block, block, CC(part), to_core)

    def crossed(plane, part):
        rows = pl.ds(pl.multiple_of(512 - co * 512, 512), 512)
        arrived(gf.at[last, rows, lanes(plane, HALF)], CC(part))

    def r_far(s):
        arrived(r_block(s, xm), RN(s, 0))
        block = r_rows(s, xm, 0)
        start(block, block, RF(s, 0), to_xp)
        arrived(r_block(s, xp), RN(s, 1))
        block = r_rows(s, xp, 1)
        start(block, block, RF(s, 1), to_xm)

    def r_done(s):
        arrived(r_rows(s, x2, 0), RF(s, 0))
        arrived(r_rows(s, x2, 1), RF(s, 1))

    def l_done(s):
        if shared and s == last:

            @pl.when(zl != co)
            def _():
                arrived(lp.at[last, pl.ds(0, LANES), :], LZ(last))

        else:
            arrived(lp.at[s, pair_rows, :], LZ(s))

    def l_last():
        if shared:

            @pl.when(zl == co)
            def _():
                block = lp.at[last, pl.ds(0, LANES), :]
                start(block, block, LZ(last), to_z)
                sent.pop()

        else:
            start(l_h.at[last], lp.at[last, pair_rows, :], LZ(last), to_z)

    def r_cross():
        start(rf2.at[:, co], rf2.at[:, co], RX(0), to_core)

    def grams(s):
        gt[...] = gf[s, :, lanes(d)].T
        grad_rows = gf[s, pl.ds(pl.multiple_of(d * LANES, LANES), LANES), :]

        weight = 1.0 - stat_decay
        if shared and s == last:
            weight = jnp.where(tile_s[0, 2 * OWNERS + me] < TILES, F32(weight), F32(0.0))

        def columns(n, carry):
            at = pl.ds(pl.multiple_of(n * 256, 256), 256)
            right = jnp.dot(gt[...], gf[s, :, at], preferred_element_type=F32)
            nr[s, :, at] = stat_decay * rs[s, :, at] + weight * right
            left = lax.dot_general(
                grad_rows, gf[s, at, :], (((1,), (1,)), ((), ())), preferred_element_type=F32
            )
            nl[s, :, at] = stat_decay * ls[s, :, at] + weight * left
            return carry

        lax.fori_loop(0, 4, columns, 0)

    out_cols = lanes(zl, HALF)

    def left_part(s, half):
        def columns(n, carry):
            at = pl.ds(pl.multiple_of(half * HALF + n * 256, 256), 256)
            if shared and s == last:
                part = jnp.dot(lp[s, :LANES], gf[s, :, at], preferred_element_type=F32)
                tp[:LANES, at] = part.astype(BF16)
            else:
                part = jnp.dot(lp[s], gf[s, :, at], preferred_element_type=F32)
                tp[:, at] = part.astype(BF16)
            return carry

        lax.fori_loop(0, 2, columns, 0)

    def direction_rows(s):
        half = shared and s == last
        chips = 16 if half else 32
        chip = my_chip if half else here // 2
        at_owner = 2 * OWNERS + my_chip if half else s * OWNERS + me

        def columns(n, carry):
            at = pl.ds(pl.multiple_of(n * 256, 256), 256)
            if half:
                right = rf2[:, :, :, at].reshape(TILE, 256)
                obuf[:LANES, at] = jnp.dot(tp[:LANES], right, preferred_element_type=F32)
            else:
                obuf[:, at] = jnp.dot(tp[...], rf[s, :, at], preferred_element_type=F32)
            return carry

        lax.fori_loop(0, 2, columns, 0)

        def rows(i):
            value = obuf[pl.ds(pl.multiple_of(i * 8, 8), 8), :]
            ostage[s, 2 * i] = value[:4].astype(BF16)
            ostage[s, 2 * i + 1] = value[4:].astype(BF16)

        def give(i, core):
            pltpu.make_async_remote_copy(
                src_ref=ostage.at[s, 2 * i + core],
                dst_ref=ret.at[at_owner, :, out_cols],
                send_sem=send.at[RET(s)],
                recv_sem=recv.at[RET(s)],
                device_id={
                    "dp_1": co if half else i // 16,
                    "owner_0": (i // 4) % 4,
                    "owner_1": i % 4,
                    "owner_2": core,
                },
                device_id_type=MESH,
            ).start()

        rows((chip + 1) % chips)

        def one(k, carry):
            rows((chip + k + 1) % chips)
            give((chip + k) % chips, 0)
            give((chip + k) % chips, 1)
            return carry

        lax.fori_loop(1, chips, one, 0)
        if half:

            @pl.when(zl == co)
            def _():
                ret[at_owner, :, out_cols] = ostage[s, me]
                give(chip, 1 - co)

            @pl.when(zl != co)
            def _():
                give(chip, 0)
                give(chip, 1)

        else:
            ret[at_owner, :, out_cols] = ostage[s, here]
            give(chip, 1 - co)

    r_far(0)
    r_far(1)
    g_here(0)
    g_own(0)
    if shared:
        to_chips()
    else:
        to_owners(2)
    r_far(2)
    g_pair(0)
    g_far(0)
    g_here(1)
    g_own(1)
    g_pair(1)
    g_here(2)
    g_far_z(0)
    l_last()
    g_far(1)
    if 1 in far_by_x:
        g_far_pair(1)
    g_own(2)
    g_pair(2)
    r_done(2)
    if shared:
        r_cross()
    for s in range(own):
        l_in[s].wait()
    ls_in.wait()
    rs_in.wait()
    g_done(0)
    r_done(0)
    l_done(0)
    left_part(0, 0)
    left_part(0, 1)
    direction_rows(0)
    grams(0)
    if 1 in far_by_x:
        g_far_here(1)
    else:
        g_far_z(1)
        g_far(2)
        g_far_pair(2)
    g_done(1)
    r_done(1)
    l_done(1)
    left_part(1, 0)
    left_part(1, 1)
    if 1 in far_by_x:
        g_far(2)
        g_far_pair(2)
    direction_rows(1)
    if shared:
        g_far_here(2)
        cross(zl, 0)
    l_done(2)
    if shared:
        g_done(2)
        cross(zo, 1)
        crossed(zl, 0)
        left_part(2, zl)
        crossed(zo, 1)
        arrived(rf2.at[:, 1 - co], RX(0))
    else:
        g_far_here(2)
        left_part(2, zl)
        g_done(2)
    left_part(2, zo)
    direction_rows(2)
    grams(1)
    grams(2)
    def ends(sem, few, many, first, wait):
        @pl.when(first)
        def _():
            wait(few, sem)

        @pl.when(jnp.logical_not(first))
        def _():
            wait(many, sem)

    for s in range(own):
        arrived(ostage.at[s, pl.ds(0, 63)], RET(s))
    few, many = ostage.at[last, pl.ds(0, 31)], ostage.at[last, pl.ds(0, 32)]
    if shared:
        ends(RET(last), few, many, zl == co, arrived)
    for copy in sent:
        copy.wait_send()

    def left(src, sem):
        pltpu.make_async_remote_copy(
            src_ref=src,
            dst_ref=src,
            send_sem=send.at[sem],
            recv_sem=recv.at[sem],
            device_id=to_xp,
            device_id_type=MESH,
        ).wait_send()

    for s in range(own):
        left(staged.at[s, pl.ds(0, OWNERS - 1)], A2A(s))
        left(ostage.at[s, pl.ds(0, 63)], RET(s))
    if shared:
        ends(RET(last), few, many, zl == co, left)
        few, many = staged.at[last, pl.ds(0, 15)], staged.at[last, pl.ds(0, 16)]
        ends(A2A(last), few, many, side == co, left)

        @pl.when(zl == co)
        def _():
            left(lp.at[last, pl.ds(0, LANES), :], LZ(last))


def write_out(shared, owner_s, ret, nl, nr, dir_h, nl_h, nr_h, rows_v, count_s, sems):
    copies = [
        pltpu.make_async_copy(nl, nl_h, sems.at[0]),
        pltpu.make_async_copy(nr, nr_h, sems.at[1]),
    ]
    for copy in copies:
        copy.start()
    d = lax.axis_index(DP)
    me = lax.axis_index(OWNER)
    line = lax.broadcasted_iota(jnp.int32, (4, TILE), 0) + (d * LANES + me * 4)
    lane = lax.broadcasted_iota(jnp.int32, (4, TILE), 1)

    def clear(o, carry):
        count_s[o] = 0
        return carry

    lax.fori_loop(0, OWNERS, clear, 0, unroll=8)

    def write(t, carry):
        rows, cols = extent(t)
        owner = owner_s[t]
        taken = count_s[owner]
        count_s[owner] = taken + OWNERS
        place = taken + owner
        if shared:
            place = jnp.where(taken < 2 * OWNERS, place, 2 * OWNERS + owner // 2)
        value = ret[place].astype(F32)
        rows_v[t] = jnp.where((line < rows) & (lane < cols), value, 0.0).astype(BF16)
        return carry

    lax.fori_loop(0, TILES, write, 0, unroll=4)
    copies.append(pltpu.make_async_copy(rows_v, dir_h, sems.at[2]))
    copies[2].start()
    for copy in copies:
        copy.wait()


def step(shared, owner_map, *arrays):
    smem = pl.BlockSpec(memory_space=pltpu.SMEM)
    vmem = pl.BlockSpec(memory_space=pltpu.VMEM)
    hbm = pl.BlockSpec(memory_space=pltpu.HBM)
    returned, new_left, new_right = pl.pallas_call(
        functools.partial(kernel, shared),
        out_shape=(
            pltpu.VMEM((SLOTS * OWNERS, 4, TILE), BF16),
            pltpu.VMEM((SLOTS, LANES, TILE), F32),
            pltpu.VMEM((SLOTS, LANES, TILE), F32),
        ),
        in_specs=[smem, hbm, hbm, hbm, hbm, hbm],
        out_specs=(vmem, vmem, vmem),
        scratch_shapes=[
            pltpu.VMEM((TILES, PIECE, TILE), BF16),
            pltpu.VMEM((2, TILES, PIECE, COLS), BF16),
            pltpu.VMEM((2, TILES, PIECE, COLS), BF16),
            pltpu.VMEM((2, TILES, PIECE, COLS), BF16),
            pltpu.VMEM((2, TILES, PIECE, COLS), BF16),
            pltpu.VMEM((TILES, PIECE, COLS), BF16),
            pltpu.VMEM((TILES, PIECE, COLS), BF16),
            pltpu.VMEM((TILES + 1, PIECE, COLS), BF16),
            pltpu.VMEM((SLOTS, OWNERS, PIECE, COLS), BF16),
            pltpu.VMEM((SLOTS, TILE, TILE), BF16),
            pltpu.VMEM((SLOTS, TILE, HALF), BF16),
            pltpu.VMEM((SLOTS, 256, TILE), BF16),
            pltpu.VMEM((SLOTS, LANES, TILE), F32),
            pltpu.VMEM((SLOTS, LANES, TILE), F32),
            pltpu.VMEM((LANES, TILE), BF16),
            pltpu.VMEM((256, TILE), BF16),
            pltpu.VMEM((256, HALF), F32),
            pltpu.VMEM((SLOTS, 64, 4, HALF), BF16),
            pltpu.VMEM((2, LANES, TILE), BF16),
            pltpu.VMEM((2, 64, TILE), BF16),
            pltpu.VMEM((64, TILE), BF16),
            pltpu.VMEM((8, 2, 64, HALF), BF16),
            pltpu.VMEM((1, LANES), jnp.int32),
            pltpu.SMEM((1, LANES), jnp.int32),
            pltpu.SemaphoreType.DMA((N_SEMS,)),
            pltpu.SemaphoreType.DMA((N_SEMS,)),
            pltpu.SemaphoreType.DMA((N_LOC,)),
            pltpu.SemaphoreType.REGULAR((5,)),
        ],
        compiler_params=pltpu.CompilerParams(
            collective_id=int(shared), has_side_effects=True, vmem_limit_bytes=60 * 1024 * 1024
        ),
    )(owner_map, *arrays)
    return pl.pallas_call(
        functools.partial(write_out, shared),
        out_shape=(
            jax.ShapeDtypeStruct((TILES, 4, TILE), BF16),
            jax.ShapeDtypeStruct((SLOTS, LANES, TILE), F32),
            jax.ShapeDtypeStruct((SLOTS, LANES, TILE), F32),
        ),
        in_specs=[smem, vmem, vmem, vmem],
        out_specs=(hbm, hbm, hbm),
        scratch_shapes=[
            pltpu.VMEM((TILES, 4, TILE), BF16),
            pltpu.SMEM((OWNERS,), jnp.int32),
            pltpu.SemaphoreType.DMA((3,)),
        ],
        compiler_params=pltpu.CompilerParams(vmem_limit_bytes=4 * 1024 * 1024),
    )(
        owner_map,
        *(
            pltpu.with_memory_space_constraint(value, pltpu.VMEM)
            for value in (returned, new_left, new_right)
        ),
    )


def body(partial_grads, owner_map, left_stats, right_stats, left_roots, right_roots):
    chips = jnp.arange(OWNERS // 2, dtype=jnp.int32)
    first = 2 * chips[:, None]
    on_chip = (owner_map[None, :] >= first) & (owner_map[None, :] < first + 2)
    held = jnp.sum(on_chip.astype(jnp.int32), axis=1)
    direction, new_left, new_right = lax.cond(
        jnp.max(held) < 2 * SLOTS,
        functools.partial(step, True),
        functools.partial(step, False),
        owner_map,
        partial_grads[0],
        left_roots[0],
        right_roots[0],
        left_stats[0],
        right_stats[0],
    )
    return direction, new_left[None], new_right[None]


def solution(mesh):
    torus = Mesh(
        mesh.devices.reshape(4, 2, 4, 4, 2), ("dp_0", "dp_1", "owner_0", "owner_1", "owner_2")
    )
    in_specs = (
        P(DP, None, OWNER, None),
        P(),
        P(OWNER, None, DP, None),
        P(OWNER, None, DP, None),
        P(OWNER, None, DP, None),
        P(OWNER, None, DP, None),
    )
    out_specs = (P(None, DP_OWNER, None), P(OWNER, None, DP, None), P(OWNER, None, DP, None))
    return jax.shard_map(body, mesh=torus, in_specs=in_specs, out_specs=out_specs, check_vma=False)
```

```python
import functools

import jax
import jax.numpy as jnp
from jax import lax
from jax.experimental import pallas as pl
from jax.experimental.pallas import tpu as pltpu
from jax.sharding import Mesh
from jax.sharding import PartitionSpec as P

D_MODEL = 2560
D_IN = 10576
D_INNER = 5120
TILE = 1024
TILES = 48
OWNERS = 32
SLOTS = 3
PIECE = 32
LANES = 128
COLS = 128
HALF = 512
RUNS = (
    (33, 48, ((33, 2), (36, 2), (39, 2), (42, 2), (45, 2))),
    (0, 11, ((0, 10),)),
    (11, 22, ((11, 10),)),
    (22, 28, ((22, 6),)),
    (28, 33, ((28, 4),)),
)
CHUNKS = len(RUNS)
OWNER = ("owner_0", "owner_1", "owner_2")
DP = ("dp_0", "dp_1")
DP_OWNER = ("dp_0", "dp_1", "owner_0", "owner_1", "owner_2")
MESH = pl.DeviceIdType.MESH
F32 = jnp.float32
BF16 = jnp.bfloat16

stat_decay = 0.999


def extent(t):
    in_cols = -(-D_IN // TILE)
    out_cols = -(-D_MODEL // TILE)
    in_count = -(-D_MODEL // TILE) * in_cols
    other = jnp.maximum(t - in_count, 0)
    is_in = t < in_count
    rows = jnp.where(
        is_in,
        jnp.minimum(TILE, D_MODEL - t // in_cols * TILE),
        jnp.minimum(TILE, D_INNER - other // out_cols * TILE),
    )
    cols = jnp.where(
        is_in,
        jnp.minimum(TILE, D_IN - t % in_cols * TILE),
        jnp.minimum(TILE, D_MODEL - other % out_cols * TILE),
    )
    return rows, cols


class Ids:
    def __init__(self):
        self.n = 0

    def __call__(self, *shape):
        size = 1
        for s in shape:
            size *= s
        base = self.n
        self.n += size

        def at(*index):
            flat = 0
            for i, s in zip(index, shape):
                flat = flat * s + i
            return base + flat

        return at


IDS = Ids()
FAR = IDS(CHUNKS, 2)
NEAR = IDS(CHUNKS, 2)
CHAIN = IDS(CHUNKS, 2)
ZZ = IDS(CHUNKS)
RZ = IDS(SLOTS)
RN = IDS(SLOTS, 2)
RF = IDS(SLOTS, 2)
LZ = IDS(SLOTS)
A2A = IDS(SLOTS)
GZ = IDS(SLOTS)
GZ_FAR = IDS(SLOTS)
GN = IDS(SLOTS, 2)
GP = IDS(SLOTS, 2, 2)
GF = IDS(SLOTS, 2)
GPF = IDS(SLOTS, 2)
RET = IDS(SLOTS)
LC = IDS(1)
RC = IDS(1)
RX = IDS(1)
CC = IDS(2)
N_SEMS = IDS.n
LOC = Ids()
L_PG = LOC(CHUNKS)
L_R = LOC(SLOTS)
L_L = LOC(SLOTS)
L_LS = LOC(1)
L_RS = LOC(1)
L_SEAT = LOC(1)
N_LOC = LOC.n


def kernel(
    shared,
    owner_s,
    pg_h,
    l_h,
    r_h,
    ls_h,
    rs_h,
    ret,
    nl,
    nr,
    pg,
    far,
    chs,
    near,
    ch,
    hs,
    zrecv,
    shares,
    staged,
    gf,
    rf,
    lp,
    ls,
    rs,
    gt,
    tp,
    obuf,
    ostage,
    lx,
    rx,
    r2,
    rf2,
    tile_v,
    tile_s,
    send,
    recv,
    local,
    told,
):
    x = lax.axis_index("dp_0")
    zl = lax.axis_index("dp_1")
    y = lax.axis_index("owner_0")
    zh = lax.axis_index("owner_1")
    co = lax.axis_index("owner_2")
    me = (y * 4 + zh) * 2 + co
    d = x * 2 + zl
    xp = (x + 1) % 4
    xm = (x + 3) % 4
    x2 = (x + 2) % 4
    zo = 1 - zl
    here = zl * 32 + me
    to_xp = {"dp_0": xp}
    to_xm = {"dp_0": xm}
    to_z = {"dp_1": zo}
    to_core = {"owner_2": 1 - co}
    my_chip = me // 2
    own = SLOTS - 1 if shared else SLOTS
    last = SLOTS - 1
    far_by_x = (1, 2) if shared else (2,)

    def owner_device(i):
        return {"owner_0": i // 8, "owner_1": (i // 2) % 4, "owner_2": i % 2}

    def any_device(i):
        return {
            "dp_1": i // 32,
            "owner_0": (i // 8) % 4,
            "owner_1": (i // 2) % 4,
            "owner_2": i % 2,
        }

    sent = []

    def start(src, dst, sem, device):
        copy = pltpu.make_async_remote_copy(
            src_ref=src,
            dst_ref=dst,
            send_sem=send.at[sem],
            recv_sem=recv.at[sem],
            device_id=device,
            device_id_type=MESH,
        )
        copy.start()
        sent.append(copy)

    def arrived(dst, sem):
        pltpu.make_async_remote_copy(
            src_ref=dst,
            dst_ref=dst,
            send_sem=send.at[sem],
            recv_sem=recv.at[sem],
            device_id=to_xp,
            device_id_type=MESH,
        ).wait_recv()

    def start_upper(k, src, dst, sem, device):
        for first, count in RUNS[k][2]:
            start(src(pl.ds(first, count)), dst(pl.ds(first, count)), sem, device)
            sent.pop()
        sent.append(copy_of(upper(k, far), sem))

    def upper(k, buffer):
        return buffer.at[1, pl.ds(RUNS[k][0], sum(count for _, count in RUNS[k][2]))]

    def copy_of(ref, sem):
        return pltpu.make_async_remote_copy(
            src_ref=ref,
            dst_ref=ref,
            send_sem=send.at[sem],
            recv_sem=recv.at[sem],
            device_id=to_xp,
            device_id_type=MESH,
        )

    def lanes(block, width=COLS):
        return pl.ds(pl.multiple_of(block * width, width), width)

    def chunk(k):
        return pl.ds(RUNS[k][0], RUNS[k][1] - RUNS[k][0])

    pg_in = [
        pltpu.make_async_copy(pg_h.at[chunk(k)], pg.at[chunk(k)], local.at[L_PG(k)])
        for k in range(CHUNKS)
    ]
    for copy in pg_in:
        copy.start()
    own_rows = pl.ds(pl.multiple_of(d * LANES, LANES), LANES)
    pair_rows = pl.ds(pl.multiple_of(zl * LANES, LANES), LANES)
    r_in = [
        pltpu.make_async_copy(
            r_h.at[s, :, lanes(zl, HALF)], rf.at[s, own_rows, :], local.at[L_R(s)]
        )
        for s in range(own)
    ]
    l_in = [
        pltpu.make_async_copy(l_h.at[s], lp.at[s, pair_rows, :], local.at[L_L(s)])
        for s in range(own)
    ]
    core_rows = pl.ds(pl.multiple_of(co * 64, 64), 64)
    if shared:
        r_in.append(
            pltpu.make_async_copy(r_h.at[last, core_rows, :], rx.at[0], local.at[L_R(last)])
        )
        l_in.append(pltpu.make_async_copy(l_h.at[last], lx.at[0], local.at[L_L(last)]))
    ls_in = pltpu.make_async_copy(ls_h, ls, local.at[L_LS(0)])
    rs_in = pltpu.make_async_copy(rs_h, rs, local.at[L_RS(0)])
    for copy in (*r_in, *l_in, ls_in, rs_in):
        copy.start()

    barrier = pltpu.get_barrier_semaphore()
    y_sides = ({"owner_0": (y + 1) % 4}, {"owner_0": (y + 3) % 4})
    zh_sides = ({"owner_1": (zh + 1) % 4}, {"owner_1": (zh + 3) % 4})
    neighbours = (to_xp, to_xm, to_z, to_core, *y_sides, *zh_sides)
    for device in neighbours:
        pl.semaphore_signal(barrier, inc=1, device_id=device, device_id_type=MESH)

    seat = lax.broadcasted_iota(jnp.int32, (1, LANES), 1)

    def take(t, carry):
        tile, count = carry
        mine = seat % OWNERS == owner_s[t]
        tile = jnp.where(mine & (count == seat // OWNERS), t, tile)
        return tile, count + mine.astype(jnp.int32)

    tile_v[...], _ = lax.fori_loop(
        0, TILES, take, (jnp.full((1, LANES), TILES, jnp.int32), jnp.zeros((1, LANES), jnp.int32))
    )
    seats_in = pltpu.make_async_copy(tile_v, tile_s, local.at[L_SEAT(0)])
    seats_in.start()
    pl.semaphore_wait(barrier, len(neighbours))

    rounds = (y_sides, zh_sides, zh_sides, (to_core,), (to_z,))

    def tell(n):
        for device in rounds[n]:
            pl.semaphore_signal(told.at[n], inc=1, device_id=device, device_id_type=MESH)

    def heard(n):
        pl.semaphore_wait(told.at[n], len(rounds[n]))

    def send_near(k):
        start(pg.at[chunk(k), :, lanes(xp)], near.at[0, chunk(k)], NEAR(k, 0), to_xp)
        start_upper(
            k,
            lambda at: pg.at[at, :, lanes(4 + xm)],
            lambda at: near.at[1, at],
            NEAR(k, 1),
            to_xm,
        )

    for k in range(CHUNKS):
        pg_in[k].wait()
        start(pg.at[chunk(k), :, lanes(x2)], far.at[0, chunk(k)], FAR(k, 0), to_xm)
        start_upper(
            k,
            lambda at: pg.at[at, :, lanes(4 + x2)],
            lambda at: far.at[1, at],
            FAR(k, 1),
            to_xp,
        )
    send_near(0)
    tell(0)

    if shared:
        start(l_h.at[last], lx.at[1], LC(0), to_core)
        other_core_rows = pl.ds(pl.multiple_of(64 - co * 64, 64), 64)
        start(r_h.at[last, other_core_rows, :], rx.at[1], RC(0), to_core)
    for s in range(own):
        r_in[s].wait()
        start(r_h.at[s, :, lanes(zo, HALF)], rf.at[s, own_rows, :], RZ(s), to_z)
    if shared:
        seats_in.wait()
        r_in[last].wait()
        l_in[last].wait()
        arrived(lx.at[1], LC(0))
        arrived(rx.at[1], RC(0))
        second = (tile_s[0, 2 * OWNERS + 2 * my_chip + 1] < TILES).astype(jnp.int32)
        source = (second + co) % 2
        r2[...] = rx[source]

        @pl.when(zl == co)
        def _():
            lp[last, :LANES] = lx[source]

        rf2[d, co] = r2[:, lanes(zl, HALF)]
        start(r2.at[:, lanes(zo, HALF)], rf2.at[d, co], RZ(last), to_z)
    for s in range(2):
        start(l_h.at[s], lp.at[s, pair_rows, :], LZ(s), to_z)

    def per_tile(k, step):
        def one(t, carry):
            step(t)
            return carry

        lax.fori_loop(RUNS[k][0], RUNS[k][1], one, 0, unroll=2)

    for k in range(CHUNKS):
        arrived(far.at[0, chunk(k)], FAR(k, 0))
        arrived(upper(k, far), FAR(k, 1))

        def add_chain(t):
            chs[0, t] = (
                far[0, t].astype(F32) + pg[t, :, lanes(xm)].astype(F32)
            ).astype(BF16)
            chs[1, t] = (
                far[1, t].astype(F32) + pg[t, :, lanes(4 + xp)].astype(F32)
            ).astype(BF16)

        per_tile(k, add_chain)
        if k + 1 < CHUNKS:
            send_near(k + 1)
        if k < 4:
            heard(k)
            tell(k + 1)
        start(chs.at[0, chunk(k)], ch.at[0, chunk(k)], CHAIN(k, 0), to_xm)
        start_upper(k, lambda at: chs.at[1, at], lambda at: ch.at[1, at], CHAIN(k, 1), to_xp)

    def quad(chip, part, rows):
        return pl.ds(pl.multiple_of(chip * 256 + part, LANES), rows)

    def r_block(s, chip):
        if shared and s == last:
            return rf2.at[pl.ds(chip * 2, 2), co]
        return rf.at[s, quad(chip, 0, 256), :]

    def r_rows(s, chip, plane):
        if shared and s == last:
            return rf2.at[chip * 2 + plane, co]
        return rf.at[s, quad(chip, plane * LANES, LANES), :]

    for s in range(SLOTS):
        arrived(r_rows(s, x, zo), RZ(s))
        block = r_block(s, x)
        start(block, block, RN(s, 0), to_xp)
        start(block, block, RN(s, 1), to_xm)

    def total(half, t):
        return (
            pg[t, :, lanes(half * 4 + x)].astype(F32)
            + near[half, t].astype(F32)
            + ch[half, t].astype(F32)
        )

    for k in range(CHUNKS):
        arrived(near.at[0, chunk(k)], NEAR(k, 0))
        arrived(ch.at[0, chunk(k)], CHAIN(k, 0))
        arrived(upper(k, near), NEAR(k, 1))
        arrived(upper(k, ch), CHAIN(k, 1))

        def other_half(t):
            hs[t] = total(zo, t).astype(BF16)

        per_tile(k, other_half)
        start(hs.at[chunk(k)], zrecv.at[chunk(k)], ZZ(k), to_z)

    my_block = zl * 4 + x
    other_block = zo * 4 + x
    row_of = lax.broadcasted_iota(jnp.int32, (PIECE, COLS), 0) + me * PIECE
    col_of = lax.broadcasted_iota(jnp.int32, (PIECE, COLS), 1) + my_block * COLS
    for k in range(CHUNKS):
        arrived(zrecv.at[chunk(k)], ZZ(k))

        def share(t):
            rows, cols = extent(t)
            value = total(zl, t) + zrecv[t].astype(F32)
            shares[t] = jnp.where((row_of < rows) & (col_of < cols), value, 0.0).astype(BF16)

        per_tile(k, share)
    shares[TILES] = jnp.zeros((PIECE, COLS), BF16)

    my_cols = lanes(my_block)
    my_piece = pl.ds(pl.multiple_of(me * PIECE, PIECE), PIECE)
    if not shared:
        seats_in.wait()
    for s in range(own):

        def stage(o, carry):
            staged[s, o] = shares[tile_s[0, s * OWNERS + o]]
            return carry

        lax.fori_loop(0, OWNERS, stage, 0, unroll=4)

    if shared:

        def stage_last(k, carry):
            at = 2 * OWNERS + 2 * k
            staged[last, k] = shares[jnp.minimum(tile_s[0, at], tile_s[0, at + 1])]
            return carry

        lax.fori_loop(0, 16, stage_last, 0, unroll=4)

    side = y // 2

    def to_chip(k):
        pltpu.make_async_remote_copy(
            src_ref=staged.at[last, k],
            dst_ref=gf.at[last, my_piece, my_cols],
            send_sem=send.at[A2A(last)],
            recv_sem=recv.at[A2A(last)],
            device_id={"owner_0": k // 4, "owner_1": k % 4, "owner_2": side},
            device_id_type=MESH,
        ).start()

    def to_chips():
        def one(k, carry):
            to_chip((my_chip + k) % 16)
            return carry

        lax.fori_loop(1, 16, one, 0)

        @pl.when(side == co)
        def _():
            gf[last, my_piece, my_cols] = staged[last, my_chip]

        @pl.when(side != co)
        def _():
            to_chip(my_chip)

    def to_owners(s):
        def one(k, carry):
            o = (me + k) % OWNERS
            pltpu.make_async_remote_copy(
                src_ref=staged.at[s, o],
                dst_ref=gf.at[s, my_piece, my_cols],
                send_sem=send.at[A2A(s)],
                recv_sem=recv.at[A2A(s)],
                device_id=owner_device(o),
                device_id_type=MESH,
            ).start()
            return carry

        lax.fori_loop(1, OWNERS, one, 0)

    heard(4)
    to_owners(0)
    to_owners(1)
    for s in range(own):
        gf[s, my_piece, my_cols] = staged[s, me]

    def span(s, part=0, parts=1):
        first, rows = (co * 512, 512 // parts) if shared and s == last else (0, 1024 // parts)
        return pl.ds(pl.multiple_of(first + part * rows, 256), rows)

    def halves(s, part):
        return span(s, part, 2)

    def g_here(s):
        if shared and s == last:

            @pl.when(side == co)
            def _():
                arrived(staged.at[s, pl.ds(0, 15)], A2A(s))

            @pl.when(side != co)
            def _():
                arrived(staged.at[s, pl.ds(0, 16)], A2A(s))

        else:
            arrived(staged.at[s, pl.ds(0, OWNERS - 1)], A2A(s))
        block = gf.at[s, span(s), my_cols]
        start(block, block, GZ(s), to_z)

    def g_own(s):
        block = gf.at[s, span(s), my_cols]
        start(block, block, GN(s, 0), to_xp)
        start(block, block, GN(s, 1), to_xm)

    def g_pair(s):
        arrived(gf.at[s, span(s), lanes(other_block)], GZ(s))
        for turn in range(2):
            block = gf.at[s, halves(s, turn), lanes(other_block)]
            start(block, block, GP(s, 0, turn), to_xp)
            block = gf.at[s, halves(s, 1 - turn), lanes(other_block)]
            start(block, block, GP(s, 1, turn), to_xm)

    def g_far(s):
        arrived(gf.at[s, span(s), lanes(zl * 4 + xm)], GN(s, 0))
        block = gf.at[s, halves(s, 0), lanes(zl * 4 + xm)]
        start(block, block, GF(s, 0), to_xp)
        arrived(gf.at[s, span(s), lanes(zl * 4 + xp)], GN(s, 1))
        block = gf.at[s, halves(s, 1), lanes(zl * 4 + xp)]
        start(block, block, GF(s, 1), to_xm)

    def g_far_pair(s):
        arrived(gf.at[s, halves(s, 0), lanes(zo * 4 + xm)], GP(s, 0, 0))
        block = gf.at[s, halves(s, 0), lanes(zo * 4 + xm)]
        start(block, block, GPF(s, 0), to_xp)
        arrived(gf.at[s, halves(s, 1), lanes(zo * 4 + xp)], GP(s, 1, 0))
        block = gf.at[s, halves(s, 1), lanes(zo * 4 + xp)]
        start(block, block, GPF(s, 1), to_xm)

    def g_far_here(s):
        arrived(gf.at[s, halves(s, 0), lanes(zl * 4 + x2)], GF(s, 0))
        arrived(gf.at[s, halves(s, 1), lanes(zl * 4 + x2)], GF(s, 1))

    def g_far_z(s):
        g_far_here(s)
        block = gf.at[s, span(s), lanes(zl * 4 + x2)]
        start(block, block, GZ_FAR(s), to_z)

    def g_done(s):
        if s not in far_by_x:
            arrived(gf.at[s, halves(s, 0), lanes(zo * 4 + xm)], GP(s, 0, 0))
            arrived(gf.at[s, halves(s, 1), lanes(zo * 4 + xp)], GP(s, 1, 0))
        arrived(gf.at[s, halves(s, 1), lanes(zo * 4 + xm)], GP(s, 0, 1))
        arrived(gf.at[s, halves(s, 0), lanes(zo * 4 + xp)], GP(s, 1, 1))
        if s not in far_by_x:
            arrived(gf.at[s, span(s), lanes(zo * 4 + x2)], GZ_FAR(s))
        else:
            arrived(gf.at[s, halves(s, 0), lanes(zo * 4 + x2)], GPF(s, 0))
            arrived(gf.at[s, halves(s, 1), lanes(zo * 4 + x2)], GPF(s, 1))

    def cross(plane, part):
        block = gf.at[last, span(last), lanes(plane, HALF)]
        start(block, block, CC(part), to_core)

    def crossed(plane, part):
        rows = pl.ds(pl.multiple_of(512 - co * 512, 512), 512)
        arrived(gf.at[last, rows, lanes(plane, HALF)], CC(part))

    def r_far(s):
        arrived(r_block(s, xm), RN(s, 0))
        block = r_rows(s, xm, 0)
        start(block, block, RF(s, 0), to_xp)
        arrived(r_block(s, xp), RN(s, 1))
        block = r_rows(s, xp, 1)
        start(block, block, RF(s, 1), to_xm)

    def r_done(s):
        arrived(r_rows(s, x2, 0), RF(s, 0))
        arrived(r_rows(s, x2, 1), RF(s, 1))

    def l_done(s):
        if shared and s == last:

            @pl.when(zl != co)
            def _():
                arrived(lp.at[last, pl.ds(0, LANES), :], LZ(last))

        else:
            arrived(lp.at[s, pair_rows, :], LZ(s))

    def l_last():
        if shared:

            @pl.when(zl == co)
            def _():
                block = lp.at[last, pl.ds(0, LANES), :]
                start(block, block, LZ(last), to_z)
                sent.pop()

        else:
            start(l_h.at[last], lp.at[last, pair_rows, :], LZ(last), to_z)

    def r_cross():
        start(rf2.at[:, co], rf2.at[:, co], RX(0), to_core)

    def grams(s):
        gt[...] = gf[s, :, lanes(d)].T
        grad_rows = gf[s, pl.ds(pl.multiple_of(d * LANES, LANES), LANES), :]

        weight = 1.0 - stat_decay
        if shared and s == last:
            weight = jnp.where(tile_s[0, 2 * OWNERS + me] < TILES, F32(weight), F32(0.0))

        def columns(n, carry):
            at = pl.ds(pl.multiple_of(n * 256, 256), 256)
            right = jnp.dot(gt[...], gf[s, :, at], preferred_element_type=F32)
            nr[s, :, at] = stat_decay * rs[s, :, at] + weight * right
            left = lax.dot_general(
                grad_rows, gf[s, at, :], (((1,), (1,)), ((), ())), preferred_element_type=F32
            )
            nl[s, :, at] = stat_decay * ls[s, :, at] + weight * left
            return carry

        lax.fori_loop(0, 4, columns, 0)

    out_cols = lanes(zl, HALF)

    def left_part(s, half):
        def columns(n, carry):
            at = pl.ds(pl.multiple_of(half * HALF + n * 256, 256), 256)
            if shared and s == last:
                part = jnp.dot(lp[s, :LANES], gf[s, :, at], preferred_element_type=F32)
                tp[:LANES, at] = part.astype(BF16)
            else:
                part = jnp.dot(lp[s], gf[s, :, at], preferred_element_type=F32)
                tp[:, at] = part.astype(BF16)
            return carry

        lax.fori_loop(0, 2, columns, 0)

    def direction_rows(s):
        half = shared and s == last
        chips = 16 if half else 32
        chip = my_chip if half else here // 2
        at_owner = 2 * OWNERS + my_chip if half else s * OWNERS + me

        def columns(n, carry):
            at = pl.ds(pl.multiple_of(n * 256, 256), 256)
            if half:
                right = rf2[:, :, :, at].reshape(TILE, 256)
                obuf[:LANES, at] = jnp.dot(tp[:LANES], right, preferred_element_type=F32)
            else:
                obuf[:, at] = jnp.dot(tp[...], rf[s, :, at], preferred_element_type=F32)
            return carry

        lax.fori_loop(0, 2, columns, 0)

        def rows(i):
            value = obuf[pl.ds(pl.multiple_of(i * 8, 8), 8), :]
            ostage[s, 2 * i] = value[:4].astype(BF16)
            ostage[s, 2 * i + 1] = value[4:].astype(BF16)

        def give(i, core):
            pltpu.make_async_remote_copy(
                src_ref=ostage.at[s, 2 * i + core],
                dst_ref=ret.at[at_owner, :, out_cols],
                send_sem=send.at[RET(s)],
                recv_sem=recv.at[RET(s)],
                device_id={
                    "dp_1": co if half else i // 16,
                    "owner_0": (i // 4) % 4,
                    "owner_1": i % 4,
                    "owner_2": core,
                },
                device_id_type=MESH,
            ).start()

        rows((chip + 1) % chips)

        def one(k, carry):
            rows((chip + k + 1) % chips)
            give((chip + k) % chips, 0)
            give((chip + k) % chips, 1)
            return carry

        lax.fori_loop(1, chips, one, 0)
        if half:

            @pl.when(zl == co)
            def _():
                ret[at_owner, :, out_cols] = ostage[s, me]
                give(chip, 1 - co)

            @pl.when(zl != co)
            def _():
                give(chip, 0)
                give(chip, 1)

        else:
            ret[at_owner, :, out_cols] = ostage[s, here]
            give(chip, 1 - co)

    r_far(0)
    r_far(1)
    g_here(0)
    g_own(0)
    if shared:
        to_chips()
    else:
        to_owners(2)
    r_far(2)
    g_pair(0)
    g_far(0)
    g_here(1)
    g_own(1)
    g_pair(1)
    g_here(2)
    g_far_z(0)
    l_last()
    g_far(1)
    if 1 in far_by_x:
        g_far_pair(1)
    g_own(2)
    g_pair(2)
    r_done(2)
    if shared:
        r_cross()
    for s in range(own):
        l_in[s].wait()
    ls_in.wait()
    rs_in.wait()
    g_done(0)
    r_done(0)
    l_done(0)
    left_part(0, 0)
    left_part(0, 1)
    direction_rows(0)
    grams(0)
    if 1 in far_by_x:
        g_far_here(1)
    else:
        g_far_z(1)
        g_far(2)
        g_far_pair(2)
    g_done(1)
    r_done(1)
    l_done(1)
    left_part(1, 0)
    left_part(1, 1)
    direction_rows(1)
    if 1 in far_by_x:
        g_far(2)
        g_far_pair(2)
    if shared:
        g_far_here(2)
        cross(zl, 0)
    l_done(2)
    if shared:
        g_done(2)
        cross(zo, 1)
        crossed(zl, 0)
        left_part(2, zl)
        crossed(zo, 1)
        arrived(rf2.at[:, 1 - co], RX(0))
    else:
        g_far_here(2)
        left_part(2, zl)
        g_done(2)
    left_part(2, zo)
    direction_rows(2)
    grams(1)
    grams(2)
    def ends(sem, few, many, first, wait):
        @pl.when(first)
        def _():
            wait(few, sem)

        @pl.when(jnp.logical_not(first))
        def _():
            wait(many, sem)

    for s in range(own):
        arrived(ostage.at[s, pl.ds(0, 63)], RET(s))
    few, many = ostage.at[last, pl.ds(0, 31)], ostage.at[last, pl.ds(0, 32)]
    if shared:
        ends(RET(last), few, many, zl == co, arrived)
    for copy in sent:
        copy.wait_send()

    def left(src, sem):
        pltpu.make_async_remote_copy(
            src_ref=src,
            dst_ref=src,
            send_sem=send.at[sem],
            recv_sem=recv.at[sem],
            device_id=to_xp,
            device_id_type=MESH,
        ).wait_send()

    for s in range(own):
        left(staged.at[s, pl.ds(0, OWNERS - 1)], A2A(s))
        left(ostage.at[s, pl.ds(0, 63)], RET(s))
    if shared:
        ends(RET(last), few, many, zl == co, left)
        few, many = staged.at[last, pl.ds(0, 15)], staged.at[last, pl.ds(0, 16)]
        ends(A2A(last), few, many, side == co, left)

        @pl.when(zl == co)
        def _():
            left(lp.at[last, pl.ds(0, LANES), :], LZ(last))


def write_out(shared, owner_s, ret, nl, nr, dir_h, nl_h, nr_h, rows_v, count_s, sems):
    copies = [
        pltpu.make_async_copy(nl, nl_h, sems.at[0]),
        pltpu.make_async_copy(nr, nr_h, sems.at[1]),
    ]
    for copy in copies:
        copy.start()
    d = lax.axis_index(DP)
    me = lax.axis_index(OWNER)
    line = lax.broadcasted_iota(jnp.int32, (4, TILE), 0) + (d * LANES + me * 4)
    lane = lax.broadcasted_iota(jnp.int32, (4, TILE), 1)

    def clear(o, carry):
        count_s[o] = 0
        return carry

    lax.fori_loop(0, OWNERS, clear, 0, unroll=8)

    def write(t, carry):
        rows, cols = extent(t)
        owner = owner_s[t]
        taken = count_s[owner]
        count_s[owner] = taken + OWNERS
        place = taken + owner
        if shared:
            place = jnp.where(taken < 2 * OWNERS, place, 2 * OWNERS + owner // 2)
        value = ret[place].astype(F32)
        rows_v[t] = jnp.where((line < rows) & (lane < cols), value, 0.0).astype(BF16)
        return carry

    lax.fori_loop(0, TILES, write, 0, unroll=4)
    copies.append(pltpu.make_async_copy(rows_v, dir_h, sems.at[2]))
    copies[2].start()
    for copy in copies:
        copy.wait()


def step(shared, owner_map, *arrays):
    smem = pl.BlockSpec(memory_space=pltpu.SMEM)
    vmem = pl.BlockSpec(memory_space=pltpu.VMEM)
    hbm = pl.BlockSpec(memory_space=pltpu.HBM)
    returned, new_left, new_right = pl.pallas_call(
        functools.partial(kernel, shared),
        out_shape=(
            pltpu.VMEM((SLOTS * OWNERS, 4, TILE), BF16),
            pltpu.VMEM((SLOTS, LANES, TILE), F32),
            pltpu.VMEM((SLOTS, LANES, TILE), F32),
        ),
        in_specs=[smem, hbm, hbm, hbm, hbm, hbm],
        out_specs=(vmem, vmem, vmem),
        scratch_shapes=[
            pltpu.VMEM((TILES, PIECE, TILE), BF16),
            pltpu.VMEM((2, TILES, PIECE, COLS), BF16),
            pltpu.VMEM((2, TILES, PIECE, COLS), BF16),
            pltpu.VMEM((2, TILES, PIECE, COLS), BF16),
            pltpu.VMEM((2, TILES, PIECE, COLS), BF16),
            pltpu.VMEM((TILES, PIECE, COLS), BF16),
            pltpu.VMEM((TILES, PIECE, COLS), BF16),
            pltpu.VMEM((TILES + 1, PIECE, COLS), BF16),
            pltpu.VMEM((SLOTS, OWNERS, PIECE, COLS), BF16),
            pltpu.VMEM((SLOTS, TILE, TILE), BF16),
            pltpu.VMEM((SLOTS, TILE, HALF), BF16),
            pltpu.VMEM((SLOTS, 256, TILE), BF16),
            pltpu.VMEM((SLOTS, LANES, TILE), F32),
            pltpu.VMEM((SLOTS, LANES, TILE), F32),
            pltpu.VMEM((LANES, TILE), BF16),
            pltpu.VMEM((256, TILE), BF16),
            pltpu.VMEM((256, HALF), F32),
            pltpu.VMEM((SLOTS, 64, 4, HALF), BF16),
            pltpu.VMEM((2, LANES, TILE), BF16),
            pltpu.VMEM((2, 64, TILE), BF16),
            pltpu.VMEM((64, TILE), BF16),
            pltpu.VMEM((8, 2, 64, HALF), BF16),
            pltpu.VMEM((1, LANES), jnp.int32),
            pltpu.SMEM((1, LANES), jnp.int32),
            pltpu.SemaphoreType.DMA((N_SEMS,)),
            pltpu.SemaphoreType.DMA((N_SEMS,)),
            pltpu.SemaphoreType.DMA((N_LOC,)),
            pltpu.SemaphoreType.REGULAR((5,)),
        ],
        compiler_params=pltpu.CompilerParams(
            collective_id=int(shared), has_side_effects=True, vmem_limit_bytes=60 * 1024 * 1024
        ),
    )(owner_map, *arrays)
    return pl.pallas_call(
        functools.partial(write_out, shared),
        out_shape=(
            jax.ShapeDtypeStruct((TILES, 4, TILE), BF16),
            jax.ShapeDtypeStruct((SLOTS, LANES, TILE), F32),
            jax.ShapeDtypeStruct((SLOTS, LANES, TILE), F32),
        ),
        in_specs=[smem, vmem, vmem, vmem],
        out_specs=(hbm, hbm, hbm),
        scratch_shapes=[
            pltpu.VMEM((TILES, 4, TILE), BF16),
            pltpu.SMEM((OWNERS,), jnp.int32),
            pltpu.SemaphoreType.DMA((3,)),
        ],
        compiler_params=pltpu.CompilerParams(vmem_limit_bytes=4 * 1024 * 1024),
    )(
        owner_map,
        *(
            pltpu.with_memory_space_constraint(value, pltpu.VMEM)
            for value in (returned, new_left, new_right)
        ),
    )


def body(partial_grads, owner_map, left_stats, right_stats, left_roots, right_roots):
    chips = jnp.arange(OWNERS // 2, dtype=jnp.int32)
    first = 2 * chips[:, None]
    on_chip = (owner_map[None, :] >= first) & (owner_map[None, :] < first + 2)
    held = jnp.sum(on_chip.astype(jnp.int32), axis=1)
    direction, new_left, new_right = lax.cond(
        jnp.max(held) < 2 * SLOTS,
        functools.partial(step, True),
        functools.partial(step, False),
        owner_map,
        partial_grads[0],
        left_roots[0],
        right_roots[0],
        left_stats[0],
        right_stats[0],
    )
    return direction, new_left[None], new_right[None]


def solution(mesh):
    torus = Mesh(
        mesh.devices.reshape(4, 2, 4, 4, 2), ("dp_0", "dp_1", "owner_0", "owner_1", "owner_2")
    )
    in_specs = (
        P(DP, None, OWNER, None),
        P(),
        P(OWNER, None, DP, None),
        P(OWNER, None, DP, None),
        P(OWNER, None, DP, None),
        P(OWNER, None, DP, None),
    )
    out_specs = (P(None, DP_OWNER, None), P(OWNER, None, DP, None), P(OWNER, None, DP, None))
    return jax.shard_map(body, mesh=torus, in_specs=in_specs, out_specs=out_specs, check_vma=False)
```
